128 devices in a mesh: gx: 32 (over x, y, core), gy: 4 (over z).
Axes of the slice: x: 4, y: 4, z: 4, core: 2. Of those that a mesh axis runs over, the one named last changes fastest.
Arguments:
- signals: float32 [64, 32, 16, 128], P('gx', 'gy'), may hold values from -6 to 6
- tiles: bfloat16 [64, 32, 4, 128, 128], P('gx', 'gy'), may hold values from 0 to 0.00390625
- tile_dir: int32 [64, 32, 4], P('gx', 'gy'), may hold values from 0 to 8
- tile_mask: int32 [64, 32, 4], P('gx', 'gy'), may hold values 0 or 1
- live_rows: int32 [64, 32], P('gx', 'gy'), may hold values from 32 to 128
- bound_rows: int32 [64, 32], P('gx', 'gy'), may hold values from 1 to 32, as said below
- scale_coeffs: float32 [6, 5], replicated, may hold values from -1 to 1
- spectral_bound: float32 [1], replicated, may hold values from 2.5 to 4
Outputs:
- coefficients: float32 [6, 64, 32, 16, 128], P(None, 'gx', 'gy')
- energy: float32 [6, 16], replicated
The draws below stay inside these ranges and needn't reach their ends.
Inputs may be any that keep to these rules, and one draw needn't show every extreme that they name: `bound_rows`: in every draw, some blocks on every device have exactly 32 boundary rows.
All inputs are finite; a program needn't handle non-finite values. No bound on the sum of `tile_mask` on one device may be relied on, other than what follows from the above.
Results may differ from the reference program's by a relative error of at most 0.0003.
Values may be sent and summed in bfloat16 or wider, within the bound.
No kernel may reach another device: no remote copies, remote signals or barrier semaphores. Data moves between devices by JAX's collectives and lax.ppermute only.
A program may use at most 64 MiB of HBM per device.

```python
import jax
import jax.numpy as jnp
from jax import lax

SIG = 16
SCALES = 6
DEG = 4
SLOTS = 4
TILE = 128
BMAX = 32
BY = 8
NBX = 64
NBY = 32


def draw_bound_rows(key, part):
    drawn = jax.random.randint(key, (NBX, NBY), 1, BMAX + 1, dtype=jnp.int32)
    columns = lax.broadcasted_iota(jnp.int32, (NBX, NBY), 1)
    return jnp.where(columns % BY == 0, jnp.int32(BMAX), drawn)


def with_ends(values, own_key, low, high):
    spot = [jax.random.randint(jax.random.fold_in(own_key, axis), (), 0, length) for axis, length in enumerate(values.shape)]
    main_axis = values.shape.index(max(values.shape))
    next_to = spot[:main_axis] + [(spot[main_axis] + 1) % values.shape[main_axis]] + spot[main_axis + 1:]
    return values.at[tuple(spot)].set(low).at[tuple(next_to)].set(high)


def steps_of(key, shape, cuts, low, high):
    def one(position, shards_of):
        steps = jax.random.uniform(jax.random.fold_in(jax.random.fold_in(key, 6), position), (shards_of,), jnp.float32, low / len(cuts), high / len(cuts))
        return jnp.repeat(jnp.exp(steps), shape[position] // shards_of).reshape((-1,) + (1,) * (len(shape) - position - 1))

    factor_of = one(*cuts[0])
    for cut in cuts[1:]:
        factor_of = factor_of * one(*cut)
    return factor_of


def scatter_about(key, dims, spread, limit, cuts=(), held_as=jnp.bfloat16):
    values = jax.random.normal(key, dims, jnp.float32) * spread
    if len(cuts) > 0:
        values = steps_of(key, dims, cuts, -0.22, 0.18) * values
    return jnp.clip(values, min=-limit, max=limit).astype(held_as)


def setup_inputs(seed: int = 0) -> dict:
    key_list = jax.random.split(jax.random.key(seed), 9)
    return {
        "signals": scatter_about(key_list[0], (NBX, NBY, SIG, TILE), 1.0, 6.0, ((0, 32), (1, 4)), jnp.float32),
        "tiles": jnp.clip(0.00390625 * jax.random.uniform(key_list[1], (NBX, NBY, SLOTS, TILE, TILE), jnp.float32) ** steps_of(key_list[1], (NBX, NBY, SLOTS, TILE, TILE), ((0, 32), (1, 4)), -0.2, 0.2), 0.0, 0.00390625).astype(jnp.bfloat16),
        "tile_dir": with_ends(jax.random.randint(key_list[2], (NBX, NBY, SLOTS), 0, 9), jax.random.fold_in(key_list[2], 1), 0, 8).astype(jnp.int32),
        "tile_mask": with_ends((jax.random.randint(key_list[3], (NBX, NBY, SLOTS), 0, 4) < 3).astype(jnp.int32), jax.random.fold_in(key_list[3], 1), 0, 1),
        "live_rows": with_ends(jax.random.randint(key_list[4], (NBX, NBY), TILE // 4, TILE + 1), jax.random.fold_in(key_list[4], 1), TILE // 4, TILE).astype(jnp.int32),
        "bound_rows": draw_bound_rows(jax.random.fold_in(key_list[8], 71), 0),
        "scale_coeffs": jnp.clip(jax.random.uniform(key_list[6], (SCALES, DEG + 1), jnp.float32, -1.0, 1.0), -1.0, 1.0),
        "spectral_bound": jnp.clip(jax.random.uniform(key_list[7], (1,), jnp.float32, 2.5, 4.0), 2.5, 4.0),
    }


def adjacency(values, tiles, tile_dir, tile_mask, bound_ind):
    own_rows = values.astype(jnp.bfloat16)
    edge_rows = (values * bound_ind[:, :, None, :]).astype(jnp.bfloat16)
    padded = jnp.pad(edge_rows, ((1, 1), (1, 1), (0, 0), (0, 0)))
    extent_x = values.shape[0]
    extent_y = values.shape[1]
    slot_list = []
    for slot_index in range(SLOTS):
        picked = jnp.zeros_like(own_rows)
        for direction in range(9):
            step_x = direction // 3 - 1
            step_y = direction % 3 - 1
            if direction == 4:
                source = own_rows
            else:
                source = padded[1 + step_x:1 + step_x + extent_x, 1 + step_y:1 + step_y + extent_y]
            matches = (tile_dir[:, :, slot_index] == direction)[:, :, None, None]
            picked = jnp.where(matches, source, picked)
        kept_mask = (tile_mask[:, :, slot_index] == 1)[:, :, None, None]
        picked = jnp.where(kept_mask, picked, jnp.zeros_like(picked))
        slot_list.append(picked)
    inputs = jnp.stack(slot_list, axis=2)

    def one_row(bundle):
        tile_row, input_row = bundle
        return jnp.einsum("jsrc,jsgc->jgr", tile_row.astype(jnp.float32), input_row.astype(jnp.float32))

    return lax.map(one_row, (tiles, inputs))


def scaled_laplacian(values, adjacent, degree, factor):
    return factor * (degree * values - adjacent) - values


def reference(signals, tiles, tile_dir, tile_mask, live_rows, bound_rows, scale_coeffs, spectral_bound):
    positions = lax.broadcasted_iota(jnp.int32, (1, 1, TILE), 2)
    live_ind = (positions < live_rows[:, :, None]).astype(jnp.float32)
    bound_ind = (positions < bound_rows[:, :, None]).astype(jnp.float32)
    initial = signals * live_ind[:, :, None, :]
    joined = jnp.concatenate([initial, live_ind[:, :, None, :]], axis=2)
    first_pass = adjacency(joined, tiles, tile_dir, tile_mask, bound_ind) * live_ind[:, :, None, :]
    degree = first_pass[:, :, SIG:, :]
    factor = 2.0 / spectral_bound[0]
    previous = initial
    current = scaled_laplacian(initial, first_pass[:, :, :SIG, :], degree, factor)
    totals = 0.5 * scale_coeffs[:, 0][:, None, None, None, None] * initial[None]
    totals = totals + scale_coeffs[:, 1][:, None, None, None, None] * current[None]
    for degree_index in range(2, DEG + 1):
        adjacent = adjacency(current, tiles, tile_dir, tile_mask, bound_ind) * live_ind[:, :, None, :]
        following = 2.0 * scaled_laplacian(current, adjacent, degree, factor) - previous
        previous = current
        current = following
        totals = totals + scale_coeffs[:, degree_index][:, None, None, None, None] * current[None]
    energy = jnp.sum(totals * totals, axis=(1, 2, 4)) / (NBX * NBY * TILE)
    return totals, energy
```

```python
import jax
import jax.numpy as jnp
from jax import lax
from jax.sharding import Mesh
from jax.sharding import PartitionSpec as P

DEG = 4
GX_GY = ("gx_0", "gx_1", "gx_2", "gy")
GX = ("gx_0", "gx_1", "gx_2")


def neighbour_pairs(devices, first):
    pairs = [(i, i + 1) for i in range(first, devices - 1, 2)]
    return pairs + [(j, i) for i, j in pairs]


def with_halo(array, sides, width):
    for axis, dim in sides:
        devices, length = (lax.axis_size(axis), array.shape[dim])
        is_even = lax.axis_index(axis) % 2 == 0
        last = lax.slice_in_dim(array, length - width, length, axis=dim)
        first = lax.slice_in_dim(array, 0, width, axis=dim)
        from_a = lax.ppermute(jnp.where(is_even, last, first), axis, neighbour_pairs(devices, 0))
        from_b = lax.ppermute(jnp.where(is_even, first, last), axis, neighbour_pairs(devices, 1))
        before = jnp.where(is_even, from_b, from_a)
        after = jnp.where(is_even, from_a, from_b)
        array = jnp.concatenate([before, array, after], axis=dim)
    return array


def sum_over(array, axes, devices):
    row = jnp.pad(array.reshape(1, -1), ((0, 0), (0, -array.size % 128)))
    spread = jnp.broadcast_to(row[None], (devices,) + row.shape)
    gathered = lax.all_to_all(spread, axes, 0, 0)
    return jnp.sum(gathered, axis=0).reshape(-1)[: array.size].reshape(array.shape)


def scaled_laplacian(values, adjacent, degree, factor):
    return factor * (degree * values - adjacent) - values


def shards(
    signals, tiles, tile_dir, tile_mask, live_rows, bound_rows, scale_coeffs, spectral_bound
):
    tile_size = signals.shape[3]
    extent_x = signals.shape[0]
    extent_y = signals.shape[1]
    slot_count = tiles.shape[2]
    block_count = extent_x * extent_y
    positions = lax.broadcasted_iota(jnp.int32, (1, 1, tile_size), 2)
    live_ind = (positions < live_rows[:, :, None]).astype(jnp.float32)
    bound_ind = (positions < bound_rows[:, :, None]).astype(jnp.float32)
    flat_tiles = tiles.reshape(block_count, slot_count, tile_size, tile_size)

    def adjacency(values):
        own_rows = values.astype(jnp.bfloat16)
        edge_rows = (values * bound_ind[:, :, None, :]).astype(jnp.bfloat16)
        padded = with_halo(edge_rows, (("gy", 1), (GX, 0)), 1)
        slot_list = []
        for slot_index in range(slot_count):
            picked = jnp.zeros_like(own_rows)
            for direction in range(9):
                step_x = direction // 3 - 1
                step_y = direction % 3 - 1
                if direction == 4:
                    source = own_rows
                else:
                    source = padded[
                        1 + step_x : 1 + step_x + extent_x, 1 + step_y : 1 + step_y + extent_y
                    ]
                matches = (tile_dir[:, :, slot_index] == direction)[:, :, None, None]
                picked = jnp.where(matches, source, picked)
            kept = (tile_mask[:, :, slot_index] == 1)[:, :, None, None]
            picked = jnp.where(kept, picked, jnp.zeros_like(picked))
            slot_list.append(picked)
        inputs = jnp.stack(slot_list, axis=1 + 1)
        flat_inputs = inputs.reshape(block_count, slot_count, inputs.shape[3], tile_size)
        product = lax.dot_general(
            flat_inputs,
            flat_tiles,
            (((1, 3), (1, 3)), ((0,), (0,))),
            preferred_element_type=jnp.float32,
        )
        product = product.reshape(extent_x, extent_y, inputs.shape[3], tile_size)
        return product * live_ind[:, :, None, :]

    channels = signals.shape[2]
    initial = signals * live_ind[:, :, None, :]
    joined = jnp.concatenate([initial, live_ind[:, :, None, :]], axis=2)
    first_pass = adjacency(joined)
    degree = first_pass[:, :, channels:, :]
    factor = 2.0 / spectral_bound[0]
    previous = initial
    current = scaled_laplacian(initial, first_pass[:, :, :channels, :], degree, factor)
    totals = 0.5 * scale_coeffs[:, 0][:, None, None, None, None] * initial[None]
    totals = totals + scale_coeffs[:, 1][:, None, None, None, None] * current[None]
    for degree_index in range(2, DEG + 1):
        adjacent = adjacency(current)
        following = 2.0 * scaled_laplacian(current, adjacent, degree, factor) - previous
        previous = current
        current = following
        totals = totals + scale_coeffs[:, degree_index][:, None, None, None, None] * current[None]
    devices = lax.axis_size(GX) * lax.axis_size("gy")
    nodes = extent_x * extent_y * tile_size * devices
    local_sums = jnp.sum(totals * totals, axis=(1, 2, 4))
    energy = sum_over(local_sums, GX_GY, devices) / nodes
    return (totals, energy)


def solution(mesh):
    torus = Mesh(mesh.devices.reshape(4, 4, 2, mesh.shape["gy"]), ("gx_0", "gx_1", "gx_2", "gy"))
    placed = (
        P(GX, "gy", None, None),
        P(GX, "gy", None, None, None),
        P(GX, "gy", None),
        P(GX, "gy", None),
        P(GX, "gy"),
        P(GX, "gy"),
        P(),
        P(),
    )
    return jax.shard_map(
        shards,
        mesh=torus,
        in_specs=placed,
        out_specs=(P(None, GX, "gy", None, None), P()),
        check_vma=False,
    )
```

```python
import jax
import jax.numpy as jnp
from jax import lax
from jax.experimental import pallas as pl
from jax.experimental.pallas import tpu as pltpu
from jax.sharding import Mesh
from jax.sharding import PartitionSpec as P

GX_GY = ("gx_0", "gx_1", "gx_2", "gy")
GX = ("gx_0", "gx_1", "gx_2")
F32 = jnp.float32
BF16 = jnp.bfloat16
EDGE = 32
ROWS, COLS = 2, 8
WIDE = COLS + 4
SPOTS = (ROWS + 4) * WIDE
ZERO = 2 * SPOTS
SLOTS = 4
HI, INFO, PACK, LONG = 128, 144, 160, 176
LIVE, BOUND, DIR, BOUND2, BOUND3, BOUND4 = 0, 1, 2, 6, 7, 8
VMEM = pl.BlockSpec(memory_space=pltpu.VMEM)
SMEM = pl.BlockSpec(memory_space=pltpu.SMEM)
ANY = pl.BlockSpec(memory_space=pl.ANY)


def params(mib):
    return pltpu.CompilerParams(vmem_limit_bytes=mib * 1024 * 1024)


def cost(flops):
    return pl.CostEstimate(flops=flops, bytes_accessed=1 << 20, transcendentals=0)


def spot(row, col):
    return (row + 2) * WIDE + (col + 2)


def lanes():
    return lax.broadcasted_iota(jnp.int32, (16, 128), 1)


def below(count):
    return (lanes() < count).astype(F32)


def split(value):
    high = value.astype(BF16)
    return high, value - high.astype(F32)


def info_of(rows):
    index = lax.broadcasted_iota(jnp.int32, (16, 128), 0)
    info = jnp.zeros((16, 128), F32)
    for row, value in rows.items():
        info = jnp.where(index == row, value, info)
    return info.astype(BF16)


def odd_z():
    return lax.axis_index("gy") % 2


def odd_core():
    return lax.axis_index("gx_2")


def merge(parts):
    lane = lanes()
    merged = parts[0]
    for index, part in enumerate(parts[1:], 1):
        merged = jnp.where(lane < EDGE * index, merged, pltpu.roll(part, EDGE * index, 1))
    return jnp.where(lane < EDGE * len(parts), merged, 0.0)


def piece(pack, index):
    moved = pltpu.roll(pack, 128 - EDGE * index, 1) if index else pack
    return jnp.where(lanes() < EDGE, moved, 0.0)


def block_message(out, at, refs, row, col, row2, col2):
    signals, dirs, masks, live, bound = refs
    value = signals[row, col] * below(live[row, col])
    high, low = split(value)
    second = signals[row2, col2] * below(bound[row2, col2])
    rows = {LIVE: below(live[row, col]), BOUND: below(bound[row, col]), BOUND2: below(bound[row2, col2])}
    for slot in range(SLOTS):
        used = jnp.where(masks[row, col, slot] == 1, dirs[row, col, slot], 9)
        rows[DIR + slot] = jnp.full((16, 128), used.astype(F32))
    out[at, HI:INFO] = high
    out[at, INFO:PACK] = info_of(rows)
    out[at, PACK:LONG] = merge([low, second]).astype(BF16)


def pack_z(tiles, signals, dirs, masks, live, bound, out_a, out_b, sem):
    refs = (signals, dirs, masks, live, bound)
    odd = odd_z()
    copies = []
    for which, out in enumerate((out_a, out_b)):
        right = odd == which
        col = jnp.where(right, COLS - 1, 0)
        for slot in range(SLOTS):
            copies.append(
                pltpu.make_async_copy(
                    tiles.at[:, col, slot, 0:EDGE, :], out.at[:, EDGE * slot : EDGE * (slot + 1), :], sem.at[which, slot]
                )
            )
            copies[-1].start()
    for which, out in enumerate((out_a, out_b)):
        right = odd == which
        col, col2 = jnp.where(right, COLS - 1, 0), jnp.where(right, COLS - 2, 1)
        for row in range(ROWS):
            block_message(out, row, refs, row, col, row, col2)
    for copy in copies:
        copy.wait()


def pack_x(tiles, signals, dirs, masks, live, bound, out_s, out_b, sem):
    refs = (signals, dirs, masks, live, bound)
    core = odd_core()
    copies = []
    for which, out in enumerate((out_s, out_b)):
        row = jnp.where(core == which, 1, 0)
        for slot in range(SLOTS):
            copies.append(
                pltpu.make_async_copy(
                    tiles.at[row, :, slot, 0:EDGE, :],
                    out.at[1 : 1 + COLS, EDGE * slot : EDGE * (slot + 1), :],
                    sem.at[which, slot],
                )
            )
            copies[-1].start()
    for which, out in enumerate((out_s, out_b)):
        row = jnp.where(core == which, 1, 0)
        for col in range(COLS):
            block_message(out, 1 + col, refs, row, col, 1 - row, col)
        for at in (0, COLS + 1):
            out[at] = jnp.zeros((LONG, 128), BF16)
    for copy in copies:
        copy.wait()


def corners_1(from_a, from_b, in_s, in_b, out_s, out_b, room, sem):
    del in_s, in_b
    odd, core = odd_z(), odd_core()
    copies = []
    for side, halo in enumerate((from_a, from_b)):
        at = jnp.where(odd == side, COLS + 1, 0)
        for which, out in enumerate((out_s, out_b)):
            row = jnp.where(core == which, 1, 0)
            first, other = halo[row].astype(F32), halo[1 - row].astype(F32)
            info, info2 = first[INFO:PACK], other[INFO:PACK]
            index = lax.broadcasted_iota(jnp.int32, (16, 128), 0)
            for place, source in (
                (BOUND2, info2[BOUND : BOUND + 1]),
                (BOUND3, info[BOUND2 : BOUND2 + 1]),
                (BOUND4, info2[BOUND2 : BOUND2 + 1]),
            ):
                info = jnp.where(index == place, source, info)
            own2 = other[HI:INFO] * info2[BOUND : BOUND + 1]
            pack = merge([first[PACK:LONG], own2, piece(first[PACK:LONG], 1), piece(other[PACK:LONG], 1)])
            room[which, side, 0:INFO] = halo[row, 0:INFO]
            room[which, side, INFO:PACK] = info.astype(BF16)
            room[which, side, PACK:LONG] = pack.astype(BF16)
            copies.append(pltpu.make_async_copy(room.at[which, side], out.at[at], sem.at[which, side]))
    for copy in copies:
        copy.start()
    for copy in copies:
        copy.wait()


def corners_2(bounds_a, bounds_b, from_a, from_b, in_s, in_b, out_s, out_b, room, sem):
    del in_s, in_b
    odd, core = odd_z(), odd_core()
    copies = []
    for side, (halo, bounds) in enumerate(((from_a, bounds_a), (from_b, bounds_b))):
        at = jnp.where(odd == side, COLS + 1, 0)
        for which, out in enumerate((out_s, out_b)):
            row = jnp.where(core == which, 1, 0)
            first, other = halo[row].astype(F32), halo[1 - row].astype(F32)
            info2 = bounds[1 - row, INFO:PACK].astype(F32)
            own2 = other[0:16] * info2[BOUND : BOUND + 1]
            pack = merge([first[16:32], own2, piece(first[16:32], 1), piece(other[16:32], 1)])
            room[which, side, 0:16] = halo[row, 0:16]
            room[which, side, 16:32] = pack.astype(BF16)
            copies.append(pltpu.make_async_copy(room.at[which, side], out.at[at], sem.at[which, side]))
    for copy in copies:
        copy.start()
    for copy in copies:
        copy.wait()


def product(inputs, weights):
    total = None
    for first in range(0, SLOTS, 2):
        term = lax.dot_general(
            jnp.concatenate(inputs[first : first + 2], axis=1),
            jnp.concatenate(weights[first : first + 2], axis=1),
            (((1,), (1,)), ((), ())),
            preferred_element_type=F32,
        )
        total = term if total is None else total + term
    return total


def ghost_blocks(from_a, from_b, from_s, from_x):
    odd, core = odd_z(), odd_core()
    found = []
    for side, halo in enumerate((from_a, from_b)):
        col = jnp.where(odd == side, COLS, -1)
        found += [(halo, row, row, col) for row in range(ROWS)]
    for which, halo in enumerate((from_s, from_x)):
        row = jnp.where(core == which, ROWS, -1)
        found += [(halo, at, row, at - 1) for at in range(COLS + 2)]
    return found


def wide(value):
    return jnp.concatenate([value, jnp.zeros((value.shape[0], 128 - value.shape[1]), value.dtype)], axis=1)


def ghost_product(halo, at, place, room, height):
    info = halo[at, INFO:PACK].astype(F32)
    offsets = [(d // 3 - 1) * WIDE + d % 3 - 1 for d in range(9)]
    inputs = []
    near = [room[place + offsets[d] + (SPOTS if d == 4 else 0)] for d in range(9)]
    for slot in range(SLOTS):
        turn = jnp.broadcast_to(info[DIR + slot : DIR + slot + 1], (16, 128)).astype(BF16)
        halves = []
        for half in range(0, height, 16):
            chosen = jnp.zeros((16, 128), BF16)
            for d in range(9):
                chosen = jnp.where(turn == d, near[d][half : half + 16], chosen)
            halves.append(chosen)
        inputs.append(halves[0] if height == 16 else jnp.concatenate(halves, axis=0))
    weights = [halo[at, EDGE * slot : EDGE * (slot + 1)] for slot in range(SLOTS)]
    return wide(product(inputs, weights))


def own_product(tiles, index, row, col, room):
    inputs = [room[index[row, col, slot]] for slot in range(SLOTS)]
    return product(inputs, [tiles[row, col, slot] for slot in range(SLOTS)])


def place_own(room, row, col, value, bound):
    at = spot(row, col)
    room[SPOTS + at, 0:16] = value.astype(BF16)
    room[at, 0:16] = (value * below(bound[row, col])).astype(BF16)


def message_2(out, at, value, bound, row, col, row2, col2):
    high, low = split(value[row, col])
    second = value[row2, col2] * below(bound[row2, col2])
    out[at, 0:16] = high
    out[at, 16:32] = merge([low, second]).astype(BF16)


def steps_12(
    tiles, signals, index, live, bound, spectral, from_a, from_b, from_s, from_x,
    degree, first_out, second_out, ghost_degree, ghost_first, out_a, out_b, out_s, out_x, room, room2,
):
    factor = 2.0 / jnp.full((16, 128), spectral[0])
    odd, core = odd_z(), odd_core()
    lane = lanes()
    head = lax.broadcasted_iota(jnp.int32, (16, 128), 0) == 0
    room[ZERO] = jnp.zeros((32, 128), BF16)
    room2[ZERO] = jnp.zeros((16, 128), BF16)

    def put_own(at, high, info):
        room[SPOTS + at, 0:16] = high
        room[SPOTS + at, 16:32] = info
        inside = info[BOUND : BOUND + 1].astype(F32)
        room[at, 0:16] = (high.astype(F32) * inside).astype(BF16)
        room[at, 16:32] = (info.astype(F32) * inside).astype(BF16)

    def put_far(at, pack, place, inside):
        room[at, 0:16] = piece(pack, place).astype(BF16)
        room[at, 16:32] = jnp.where(head, inside, 0.0).astype(BF16)

    for row in range(ROWS):
        for col in range(COLS):
            at = spot(row, col)
            alive, inside = below(live[row, col]), below(bound[row, col])
            value = signals[row, col] * alive
            place_own(room, row, col, value, bound)
            room[SPOTS + at, 16:32] = jnp.where(head, alive, 0.0).astype(BF16)
            room[at, 16:32] = jnp.where(head, inside, 0.0).astype(BF16)
    for side, halo in enumerate((from_a, from_b)):
        right = odd == side
        col, far = jnp.where(right, COLS, -1), jnp.where(right, COLS + 1, -2)
        for row in range(ROWS):
            info = halo[row, INFO:PACK]
            put_own(spot(row, col), halo[row, HI:INFO], info)
            pack = halo[row, PACK:LONG].astype(F32)
            put_far(spot(row, far), pack, 1, info[BOUND2 : BOUND2 + 1].astype(F32))
    for which, halo in enumerate((from_s, from_x)):
        down = core == which
        row, far = jnp.where(down, ROWS, -1), jnp.where(down, ROWS + 1, -2)
        for k in range(COLS + 2):
            info = halo[k, INFO:PACK]
            put_own(spot(row, k - 1), halo[k, HI:INFO], info)
            info = info.astype(F32)
            pack = halo[k, PACK:LONG].astype(F32)
            put_far(spot(far, k - 1), pack, 1, info[BOUND2 : BOUND2 + 1])
            if k in (0, COLS + 1):
                col = -2 if k == 0 else COLS + 1
                put_far(spot(row, col), pack, 2, info[BOUND3 : BOUND3 + 1])
                put_far(spot(far, col), pack, 3, info[BOUND4 : BOUND4 + 1])

    for number, (halo, at, row, col) in enumerate(ghost_blocks(from_a, from_b, from_s, from_x)):
        place = spot(row, col)
        sums = ghost_product(halo, at, place, room, 32)
        value = halo[at, HI:INFO].astype(F32) + piece(halo[at, PACK:LONG].astype(F32), 0)
        around = jnp.broadcast_to(sums[16:17], (16, 128))
        result = factor * (around * value - sums[0:16]) - value
        ghost_degree[number] = around
        ghost_first[number] = result
        inside = halo[at, INFO:PACK].astype(F32)[BOUND : BOUND + 1]
        room2[place] = jnp.where(lane < EDGE, result * inside, 0.0).astype(BF16)

    for row in range(ROWS):
        for col in range(COLS):
            sums = own_product(tiles, index, row, col, room)
            alive = below(live[row, col])
            value = signals[row, col] * alive
            around = jnp.broadcast_to(sums[16:17], (16, 128)) * alive
            result = factor * (around * value - sums[0:16] * alive) - value
            degree[row, col] = around
            first_out[row, col] = result
            place_own(room2, row, col, result, bound)

    for row in range(ROWS):
        for col in range(COLS):
            sums = own_product(tiles, index, row, col, room2)
            alive = below(live[row, col])
            value = first_out[row, col]
            result = 2.0 * (factor * (degree[row, col] * value - sums * alive) - value)
            second_out[row, col] = result - signals[row, col] * alive

    for side, out in enumerate((out_a, out_b)):
        right = odd == side
        col, col2 = jnp.where(right, COLS - 1, 0), jnp.where(right, COLS - 2, 1)
        for row in range(ROWS):
            message_2(out, row, second_out, bound, row, col, row, col2)
    for which, out in enumerate((out_s, out_x)):
        row = jnp.where(core == which, 1, 0)
        for col in range(COLS):
            message_2(out, 1 + col, second_out, bound, row, col, 1 - row, col)
        for at in (0, COLS + 1):
            out[at] = jnp.zeros((32, 128), BF16)


def steps_34(
    tiles, signals, index, live, bound, spectral, scales, from_a, from_b, from_s, from_x,
    degree, first, second, ghost_degree, ghost_first, new_a, new_b, new_s, new_x,
    coefficients, partial, room, room2, third,
):
    factor = 2.0 / jnp.full((16, 128), spectral[0])
    odd, core = odd_z(), odd_core()
    lane = lanes()
    room[ZERO] = jnp.zeros((16, 128), BF16)
    room2[ZERO] = jnp.zeros((16, 128), BF16)

    def put_own(at, high, info):
        room[SPOTS + at] = high
        room[at] = (high.astype(F32) * info.astype(F32)[BOUND : BOUND + 1]).astype(BF16)

    def put_far(at, pack, place):
        room[at] = piece(pack, place).astype(BF16)

    for row in range(ROWS):
        for col in range(COLS):
            place_own(room, row, col, second[row, col], bound)
    for side, (halo, old) in enumerate(((new_a, from_a), (new_b, from_b))):
        right = odd == side
        col, far = jnp.where(right, COLS, -1), jnp.where(right, COLS + 1, -2)
        for row in range(ROWS):
            put_own(spot(row, col), halo[row, 0:16], old[row, INFO:PACK])
            put_far(spot(row, far), halo[row, 16:32].astype(F32), 1)
    for which, (halo, old) in enumerate(((new_s, from_s), (new_x, from_x))):
        down = core == which
        row, far = jnp.where(down, ROWS, -1), jnp.where(down, ROWS + 1, -2)
        for k in range(COLS + 2):
            put_own(spot(row, k - 1), halo[k, 0:16], old[k, INFO:PACK])
            pack = halo[k, 16:32].astype(F32)
            put_far(spot(far, k - 1), pack, 1)
            if k in (0, COLS + 1):
                col = -2 if k == 0 else COLS + 1
                put_far(spot(row, col), pack, 2)
                put_far(spot(far, col), pack, 3)

    values = ghost_blocks(new_a, new_b, new_s, new_x)
    for number, (halo, at, row, col) in enumerate(ghost_blocks(from_a, from_b, from_s, from_x)):
        place = spot(row, col)
        sums = ghost_product(halo, at, place, room, 16)
        fresh = values[number][0]
        value = fresh[at, 0:16].astype(F32) + piece(fresh[at, 16:32].astype(F32), 0)
        result = 2.0 * (factor * (ghost_degree[number] * value - sums) - value) - ghost_first[number]
        inside = halo[at, INFO:PACK].astype(F32)[BOUND : BOUND + 1]
        room2[place] = jnp.where(lane < EDGE, result * inside, 0.0).astype(BF16)

    for row in range(ROWS):
        for col in range(COLS):
            sums = own_product(tiles, index, row, col, room)
            alive = below(live[row, col])
            value = second[row, col]
            result = 2.0 * (factor * (degree[row, col] * value - sums * alive) - value) - first[row, col]
            third[row, col] = result
            place_own(room2, row, col, result, bound)

    count = scales.shape[0]
    squares = [jnp.zeros((16, 128), F32) for _ in range(count)]
    for row in range(ROWS):
        for col in range(COLS):
            sums = own_product(tiles, index, row, col, room2)
            alive = below(live[row, col])
            value = third[row, col]
            fourth = 2.0 * (factor * (degree[row, col] * value - sums * alive) - value) - second[row, col]
            terms = (signals[row, col] * alive, first[row, col], second[row, col], value, fourth)
            for scale in range(count):
                total = (0.5 * scales[scale, 0]) * terms[0]
                for order in range(1, len(terms)):
                    total = total + scales[scale, order] * terms[order]
                coefficients[scale, row, col] = total
                squares[scale] = squares[scale] + total * total
    block = jnp.concatenate(squares + [jnp.zeros((128 - 16 * count, 128), F32)], axis=0)
    line = jnp.sum(jnp.transpose(block), axis=0, keepdims=True)
    partial[...] = jnp.broadcast_to(line[None], partial.shape)


def neighbour_pairs(devices, first):
    pairs = [(i, i + 1) for i in range(first, devices - 1, 2)]
    return pairs + [(j, i) for i, j in pairs]


def shape(dims, kind=BF16):
    return jax.ShapeDtypeStruct(dims, kind)


def shards(signals, tiles, tile_dir, tile_mask, live_rows, bound_rows, scale_coeffs, spectral_bound):
    devices_x, devices_z = lax.axis_size(GX), lax.axis_size("gy")
    devices = devices_x * devices_z
    scales, channels = scale_coeffs.shape[0], signals.shape[2]
    nodes = ROWS * COLS * 128 * devices

    def swap_z(a, b):
        return (
            lax.ppermute(a, "gy", neighbour_pairs(devices_z, 0)),
            lax.ppermute(b, "gy", neighbour_pairs(devices_z, 1)),
        )

    def swap_x(s, x):
        far = lax.ppermute(x, GX, neighbour_pairs(devices_x, 1))
        return lax.ppermute(s, "gx_2", [(0, 1), (1, 0)]), far

    base = spot(
        lax.broadcasted_iota(jnp.int32, tile_dir.shape, 0), lax.broadcasted_iota(jnp.int32, tile_dir.shape, 1)
    )
    moved = base + (tile_dir // 3 - 1) * WIDE + tile_dir % 3 - 1
    index = jnp.where(tile_dir == 4, SPOTS + base, moved)
    index = jnp.where(tile_mask == 1, index, ZERO)

    local = (tiles, signals, tile_dir, tile_mask, live_rows, bound_rows)
    local_specs = [ANY, VMEM] + [SMEM] * 4
    message_z, message_x = shape((ROWS, LONG, 128)), shape((COLS + 2, LONG, 128))
    a, b = pl.pallas_call(
        pack_z,
        out_shape=[message_z] * 2,
        in_specs=local_specs,
        out_specs=[VMEM] * 2,
        scratch_shapes=[pltpu.SemaphoreType.DMA((2, SLOTS))],
        compiler_params=params(8),
        cost_estimate=cost(1000),
        name="pack_z",
    )(*local)
    s, x = pl.pallas_call(
        pack_x,
        out_shape=[message_x] * 2,
        in_specs=local_specs,
        out_specs=[VMEM] * 2,
        scratch_shapes=[pltpu.SemaphoreType.DMA((2, SLOTS))],
        compiler_params=params(8),
        cost_estimate=cost(2000000),
        name="pack_x",
    )(*local)
    a, b = swap_z(a, b)
    s, x = pl.pallas_call(
        corners_1,
        out_shape=[message_x] * 2,
        in_specs=[VMEM] * 2 + [ANY] * 2,
        out_specs=[ANY] * 2,
        scratch_shapes=[pltpu.VMEM((2, 2, LONG, 128), BF16), pltpu.SemaphoreType.DMA((2, 2))],
        input_output_aliases={2: 0, 3: 1},
        compiler_params=params(8),
        cost_estimate=cost(1000),
        name="corners_1",
    )(a, b, s, x)
    s, x = swap_x(s, x)

    ghosts = 2 * ROWS + 2 * (COLS + 2)
    field = shape((ROWS, COLS, channels, 128), F32)
    extra = shape((ghosts, channels, 128), F32)
    short_z, short_x = shape((ROWS, 32, 128)), shape((COLS + 2, 32, 128))
    state = pl.pallas_call(
        steps_12,
        out_shape=[field] * 3 + [extra] * 2 + [short_z] * 2 + [short_x] * 2,
        in_specs=[VMEM] * 2 + [SMEM] * 4 + [VMEM] * 4,
        out_specs=[VMEM] * 9,
        scratch_shapes=[pltpu.VMEM((ZERO + 1, 32, 128), BF16), pltpu.VMEM((ZERO + 1, 16, 128), BF16)],
        compiler_params=params(24),
        cost_estimate=cost(1 << 27),
        name="steps_12",
    )(tiles, signals, index, live_rows, bound_rows, spectral_bound, a, b, s, x)
    degree, first, second, ghost_degree, ghost_first, a2, b2, s2, x2 = state
    a2, b2 = swap_z(a2, b2)
    s2, x2 = pl.pallas_call(
        corners_2,
        out_shape=[short_x] * 2,
        in_specs=[VMEM] * 4 + [ANY] * 2,
        out_specs=[ANY] * 2,
        scratch_shapes=[pltpu.VMEM((2, 2, 32, 128), BF16), pltpu.SemaphoreType.DMA((2, 2))],
        input_output_aliases={4: 0, 5: 1},
        compiler_params=params(8),
        cost_estimate=cost(1000),
        name="corners_2",
    )(a, b, a2, b2, s2, x2)
    s2, x2 = swap_x(s2, x2)
    totals, partial = pl.pallas_call(
        steps_34,
        out_shape=[shape((scales, ROWS, COLS, channels, 128), F32), shape((devices, 1, 128), F32)],
        in_specs=[VMEM] * 2 + [SMEM] * 5 + [VMEM] * 13,
        out_specs=[VMEM] * 2,
        scratch_shapes=[
            pltpu.VMEM((ZERO + 1, 16, 128), BF16),
            pltpu.VMEM((ZERO + 1, 16, 128), BF16),
            pltpu.VMEM((ROWS, COLS, channels, 128), F32),
        ],
        compiler_params=params(24),
        cost_estimate=cost(1 << 27),
        name="steps_34",
    )(
        tiles, signals, index, live_rows, bound_rows, spectral_bound, scale_coeffs, a, b, s, x,
        degree, first, second, ghost_degree, ghost_first, a2, b2, s2, x2,
    )
    gathered = lax.all_to_all(partial, GX_GY, 0, 0)
    energy = jnp.sum(gathered, axis=(0, 1))[: scales * channels].reshape(scales, channels) / nodes
    return (totals, energy)


def solution(mesh):
    torus = Mesh(mesh.devices.reshape(4, 4, 2, mesh.shape["gy"]), ("gx_0", "gx_1", "gx_2", "gy"))
    placed = (
        P(GX, "gy", None, None),
        P(GX, "gy", None, None, None),
        P(GX, "gy", None),
        P(GX, "gy", None),
        P(GX, "gy"),
        P(GX, "gy"),
        P(),
        P(),
    )
    return jax.shard_map(
        shards,
        mesh=torus,
        in_specs=placed,
        out_specs=(P(None, GX, "gy", None, None), P()),
        check_vma=False,
    )
```

```python
import jax
import jax.numpy as jnp
from jax import lax
from jax.experimental import pallas as pl
from jax.experimental.pallas import tpu as pltpu
from jax.sharding import Mesh
from jax.sharding import PartitionSpec as P

GX_GY = ("gx_0", "gx_1", "gx_2", "gy")
GX = ("gx_0", "gx_1", "gx_2")
F32 = jnp.float32
BF16 = jnp.bfloat16
EDGE = 32
ROWS, COLS = 2, 8
WIDE = COLS + 4
SPOTS = (ROWS + 4) * WIDE
ZERO = 2 * SPOTS
SLOTS = 4
HI, INFO, PACK, LONG = 128, 144, 160, 176
LIVE, BOUND, DIR, BOUND2, BOUND3, BOUND4 = 0, 1, 2, 6, 7, 8
VMEM = pl.BlockSpec(memory_space=pltpu.VMEM)
SMEM = pl.BlockSpec(memory_space=pltpu.SMEM)
ANY = pl.BlockSpec(memory_space=pl.ANY)
HBM = pl.BlockSpec(memory_space=pltpu.MemorySpace.HBM)


def params(mib):
    return pltpu.CompilerParams(vmem_limit_bytes=mib * 1024 * 1024)


def cost(flops):
    return pl.CostEstimate(flops=flops, bytes_accessed=1 << 20, transcendentals=0)


def lanes():
    return lax.broadcasted_iota(jnp.int32, (16, 128), 1)


def below(count):
    return (lanes() < count).astype(F32)


def split(value):
    high = value.astype(BF16)
    return high, value - high.astype(F32)


def info_of(rows):
    index = lax.broadcasted_iota(jnp.int32, (16, 128), 0)
    info = jnp.zeros((16, 128), F32)
    for row, value in rows.items():
        info = jnp.where(index == row, value, info)
    return info.astype(BF16)


def odd_z():
    return lax.axis_index("gy") % 2


def odd_core():
    return lax.axis_index("gx_2")


def merge(parts):
    lane = lanes()
    merged = parts[0]
    for index, part in enumerate(parts[1:], 1):
        merged = jnp.where(lane < EDGE * index, merged, pltpu.roll(part, EDGE * index, 1))
    return jnp.where(lane < EDGE * len(parts), merged, 0.0)


def piece(pack, index):
    moved = pltpu.roll(pack, 128 - EDGE * index, 1) if index else pack
    return jnp.where(lanes() < EDGE, moved, 0.0)


def block_message(out, at, refs, row, col, row2, col2):
    signals, dirs, masks, live, bound = refs
    value = signals[row, col] * below(live[row, col])
    high, low = split(value)
    second = signals[row2, col2] * below(bound[row2, col2])
    rows = {LIVE: below(live[row, col]), BOUND: below(bound[row, col]), BOUND2: below(bound[row2, col2])}
    for slot in range(SLOTS):
        used = jnp.where(masks[row, slot, col] == 1, dirs[row, slot, col], 9)
        rows[DIR + slot] = jnp.full((16, 128), used.astype(F32))
    out[at, HI:INFO] = high
    out[at, INFO:PACK] = info_of(rows)
    out[at, PACK:LONG] = merge([low, second]).astype(BF16)


def fetch(refs, rooms, sems):
    copies = [pltpu.make_async_copy(ref, room, sems.at[i]) for i, (ref, room) in enumerate(zip(refs, rooms))]
    for copy in copies:
        copy.start()
    return copies


def pack_z(tiles, signals, dirs, masks, live, bound, out_a, out_b, signals_v, dirs_s, masks_s, live_s, bound_s, sem, sem2):
    refs = (signals_v, dirs_s, masks_s, live_s, bound_s)
    copies = fetch((signals, dirs, masks, live, bound), refs, sem2)
    odd = odd_z()
    later = []
    for which, out in enumerate((out_a, out_b)):
        right = odd == which
        col = jnp.where(right, COLS - 1, 0)
        for slot in range(SLOTS):
            later.append(
                pltpu.make_async_copy(
                    tiles.at[:, col, slot, 0:EDGE, :], out.at[:, EDGE * slot : EDGE * (slot + 1), :], sem.at[which, slot]
                )
            )
            later[-1].start()
    for copy in copies:
        copy.wait()
    for which, out in enumerate((out_a, out_b)):
        right = odd == which
        col, col2 = jnp.where(right, COLS - 1, 0), jnp.where(right, COLS - 2, 1)
        for row in range(ROWS):
            block_message(out, row, refs, row, col, row, col2)
    for copy in later:
        copy.wait()


def pack_x(tiles, signals, dirs, masks, live, bound, out_s, out_b, table, signals_v, dirs_s, masks_s, live_s, bound_s, sem, sem2):
    refs = (signals_v, dirs_s, masks_s, live_s, bound_s)
    copies = fetch((signals, dirs, masks, live, bound), refs, sem2)
    core = odd_core()
    later = []
    for which, out in enumerate((out_s, out_b)):
        row = jnp.where(core == which, 1, 0)
        for slot in range(SLOTS):
            later.append(
                pltpu.make_async_copy(
                    tiles.at[row, :, slot, 0:EDGE, :],
                    out.at[1 : 1 + COLS, EDGE * slot : EDGE * (slot + 1), :],
                    sem.at[which, slot],
                )
            )
            later[-1].start()
    for copy in copies:
        copy.wait()
    for which, out in enumerate((out_s, out_b)):
        row = jnp.where(core == which, 1, 0)
        for col in range(COLS):
            block_message(out, 1 + col, refs, row, col, 1 - row, col)
    odd = odd_z()
    down, right = (2 * core - 1) * WIDE, 1 - 2 * odd
    for row in range(ROWS):
        for col in range(COLS):
            base = place(jnp.where(core == row, 3, 2), jnp.where(odd == 1, COLS - 1 - col, col))
            for slot in range(SLOTS):
                side = dirs_s[row, slot, col]
                step = jnp.where(side > 5, 1, jnp.where(side > 2, 0, -1))
                index = base + step * down + (side - 3 * step - 4) * right
                index = jnp.where(side == 4, SPOTS + base, index)
                table[row, slot, col] = jnp.where(masks_s[row, slot, col] == 1, index, ZERO)
            table[row, SLOTS, col] = live_s[row, col]
            table[row, SLOTS + 1, col] = bound_s[row, col]
        for at in (0, COLS + 1):
            out[at] = jnp.zeros((LONG, 128), BF16)
    for copy in later:
        copy.wait()


def corners_1(from_a, from_b, in_s, in_b, out_s, out_b, room, sem):
    del in_s, in_b
    odd, core = odd_z(), odd_core()
    copies = []
    for side, halo in enumerate((from_a, from_b)):
        at = jnp.where(odd == side, COLS + 1, 0)
        for which, out in enumerate((out_s, out_b)):
            row = jnp.where(core == which, 1, 0)
            first, other = halo[row].astype(F32), halo[1 - row].astype(F32)
            info, info2 = first[INFO:PACK], other[INFO:PACK]
            index = lax.broadcasted_iota(jnp.int32, (16, 128), 0)
            for place, source in (
                (BOUND2, info2[BOUND : BOUND + 1]),
                (BOUND3, info[BOUND2 : BOUND2 + 1]),
                (BOUND4, info2[BOUND2 : BOUND2 + 1]),
            ):
                info = jnp.where(index == place, source, info)
            own2 = other[HI:INFO] * info2[BOUND : BOUND + 1]
            pack = merge([first[PACK:LONG], own2, piece(first[PACK:LONG], 1), piece(other[PACK:LONG], 1)])
            room[which, side, 0:INFO] = halo[row, 0:INFO]
            room[which, side, INFO:PACK] = info.astype(BF16)
            room[which, side, PACK:LONG] = pack.astype(BF16)
            copies.append(pltpu.make_async_copy(room.at[which, side], out.at[at], sem.at[which, side]))
    for copy in copies:
        copy.start()
    for copy in copies:
        copy.wait()


def corners_2(bounds_a, bounds_b, from_a, from_b, in_s, in_b, out_s, out_b, room, sem):
    del in_s, in_b
    odd, core = odd_z(), odd_core()
    copies = []
    for side, (halo, bounds) in enumerate(((from_a, bounds_a), (from_b, bounds_b))):
        at = jnp.where(odd == side, COLS + 1, 0)
        for which, out in enumerate((out_s, out_b)):
            row = jnp.where(core == which, 1, 0)
            first, other = halo[row].astype(F32), halo[1 - row].astype(F32)
            info2 = bounds[1 - row, INFO:PACK].astype(F32)
            own2 = other[0:16] * info2[BOUND : BOUND + 1]
            pack = merge([first[16:32], own2, piece(first[16:32], 1), piece(other[16:32], 1)])
            room[which, side, 0:16] = halo[row, 0:16]
            room[which, side, 16:32] = pack.astype(BF16)
            copies.append(pltpu.make_async_copy(room.at[which, side], out.at[at], sem.at[which, side]))
    for copy in copies:
        copy.start()
    for copy in copies:
        copy.wait()


def place(u, v):
    return u * WIDE + v + 2


class Frame:
    def __init__(self):
        self.odd, self.core = odd_z(), odd_core()
        self.up = 2 * self.core - 1
        self.right = 1 - 2 * self.odd

    def row(self, u):
        return 1 - self.core if u == 2 else self.core

    def col(self, v):
        return jnp.where(self.odd == 1, COLS - 1 - v, v)


def product(inputs, weights):
    total = None
    for first in range(0, SLOTS, 2):
        term = lax.dot_general(
            jnp.concatenate(inputs[first : first + 2], axis=1),
            jnp.concatenate(weights[first : first + 2], axis=1),
            (((1,), (1,)), ((), ())),
            preferred_element_type=F32,
        )
        total = term if total is None else total + term
    return total


def ghost_blocks(frame, u, halo_a, halo_b, halo_x):
    row = frame.row(u)
    found = [(halo_a, row, u, COLS), (halo_b, row, u, -1)]
    return found + [(halo_x, frame.col(v) + 1, 1 if u == 2 else 4, v) for v in range(-1, COLS + 1)]


def wide(value):
    return jnp.concatenate([value, jnp.zeros((value.shape[0], 128 - value.shape[1]), value.dtype)], axis=1)


def ghost_product(frame, halo, at, spot_at, room, height):
    info = halo[at, INFO:PACK].astype(F32)
    step = jnp.where(info > 5.5, 1.0, jnp.where(info > 2.5, 0.0, -1.0))
    turned = 3.0 * (frame.up.astype(F32) * step) + frame.right.astype(F32) * (info - 3.0 * step - 4.0) + 4.0
    turned = jnp.where(info > 8.5, 9.0, turned)
    offsets = [(d // 3 - 1) * WIDE + d % 3 - 1 for d in range(9)]
    near = [room[spot_at + offsets[d] + (SPOTS if d == 4 else 0)] for d in range(9)]
    inputs = []
    for slot in range(SLOTS):
        turn = jnp.broadcast_to(turned[DIR + slot : DIR + slot + 1], (16, 128)).astype(BF16)
        halves = []
        for half in range(0, height, 16):
            chosen = jnp.zeros((16, 128), BF16)
            for d in range(9):
                chosen = jnp.where(turn == d, near[d][half : half + 16], chosen)
            halves.append(chosen)
        inputs.append(halves[0] if height == 16 else jnp.concatenate(halves, axis=0))
    weights = [halo[at, EDGE * slot : EDGE * (slot + 1)] for slot in range(SLOTS)]
    return wide(product(inputs, weights))


def own_product(tiles, table, row, col, room):
    inputs = [room[table[row, slot, col]] for slot in range(SLOTS)]
    return jnp.dot(jnp.concatenate(inputs, axis=1), tiles[row, col], preferred_element_type=F32)


def alive_of(table, row, col):
    return below(table[row, SLOTS, col])


def inside_of(table, row, col):
    return below(table[row, SLOTS + 1, col])


def place_own(room, table, row, col, at, value):
    room[SPOTS + at, 0:16] = value.astype(BF16)
    room[at, 0:16] = (value * inside_of(table, row, col)).astype(BF16)


def bound_row(halo, at):
    return halo[at, INFO:PACK].astype(F32)[BOUND : BOUND + 1]


def message_2(out, at, value, table, col, u, v, u2, v2, col2, row2):
    high, low = split(value[u - 2, v])
    second = value[u2 - 2, v2] * inside_of(table, row2, col2)
    out[at, 0:16] = high
    out[at, 16:32] = merge([low, second]).astype(BF16)


def turn_tiles(tiles, out):
    def one(block, carry):
        row, col = block // COLS, block % COLS
        for slot in range(SLOTS):
            out[row, col, 128 * slot : 128 * (slot + 1)] = jnp.transpose(tiles[row, col, slot])
        return carry

    lax.fori_loop(0, ROWS * COLS, one, 0)


def heads():
    return lax.broadcasted_iota(jnp.int32, (16, 128), 0) == 0


def fill_1(room, halo, at, near, far, corner):
    high, info = halo[at, HI:INFO], halo[at, INFO:PACK]
    rows, pack = info.astype(F32), halo[at, PACK:LONG].astype(F32)
    inside = rows[BOUND : BOUND + 1]
    room[SPOTS + near, 0:16] = high
    room[SPOTS + near, 16:32] = info
    room[near, 0:16] = (high.astype(F32) * inside).astype(BF16)
    room[near, 16:32] = (rows * inside).astype(BF16)
    for index, (spot_at, line) in enumerate(zip((far,) + corner, (BOUND2, BOUND3, BOUND4)), 1):
        room[spot_at, 0:16] = piece(pack, index).astype(BF16)
        room[spot_at, 16:32] = jnp.where(heads(), rows[line : line + 1], 0.0).astype(BF16)


def fill_2(room, halo, old, at, near, far, corner):
    high, pack = halo[at, 0:16], halo[at, 16:32].astype(F32)
    room[SPOTS + near] = high
    room[near] = (high.astype(F32) * bound_row(old, at)).astype(BF16)
    for index, spot_at in enumerate((far,) + corner, 1):
        room[spot_at] = piece(pack, index).astype(BF16)


def fill_z(fill, frame, room, halos):
    for halo, near, far in ((halos[0], COLS, COLS + 1), (halos[1], -1, -2)):
        for u in (2, 3):
            fill(room, *halo, frame.row(u), place(u, near), place(u, far), ())


def fill_x(fill, frame, room, halo, near, far):
    for v in range(-1, COLS + 1):
        beyond = {-1: -2, COLS: COLS + 1}.get(v)
        corner = () if beyond is None else (place(near, beyond), place(far, beyond))
        fill(room, *halo, frame.col(v) + 1, place(near, v), place(far, v), corner)


def half_1(frame, u, tiles, signals, table, factor, halos, room, room2, degree, first, ghost_degree, ghost_first):
    lane = lanes()
    for number, (halo, at, gu, gv) in enumerate(ghost_blocks(frame, u, *halos)):
        sums = ghost_product(frame, halo, at, place(gu, gv), room, 32)
        value = halo[at, HI:INFO].astype(F32) + piece(halo[at, PACK:LONG].astype(F32), 0)
        around = jnp.broadcast_to(sums[16:17], (16, 128))
        result = factor * (around * value - sums[0:16]) - value
        ghost_degree[number] = around
        ghost_first[number] = result
        room2[place(gu, gv)] = jnp.where(lane < EDGE, result * bound_row(halo, at), 0.0).astype(BF16)
    row = frame.row(u)
    for v in range(COLS):
        col = frame.col(v)
        sums = own_product(tiles, table, row, col, room)
        alive = alive_of(table, row, col)
        value = signals[row, col] * alive
        around = jnp.broadcast_to(sums[16:17], (16, 128)) * alive
        result = factor * (around * value - sums[0:16] * alive) - value
        degree[v] = around
        first[v] = result
        place_own(room2, table, row, col, place(u, v), result)


def half_3(frame, u, tiles, table, factor, halos, fresh, room, room2, degree, first, second, third, ghost_degree, ghost_first):
    lane = lanes()
    values = ghost_blocks(frame, u, *fresh)
    for number, (halo, at, gu, gv) in enumerate(ghost_blocks(frame, u, *halos)):
        sums = ghost_product(frame, halo, at, place(gu, gv), room, 16)
        new = values[number][0]
        value = new[at, 0:16].astype(F32) + piece(new[at, 16:32].astype(F32), 0)
        result = 2.0 * (factor * (ghost_degree[number] * value - sums) - value) - ghost_first[number]
        room2[place(gu, gv)] = jnp.where(lane < EDGE, result * bound_row(halo, at), 0.0).astype(BF16)
    row = frame.row(u)
    for v in range(COLS):
        col = frame.col(v)
        sums = own_product(tiles, table, row, col, room)
        value = second[u - 2, v]
        result = 2.0 * (factor * (degree[v] * value - sums * alive_of(table, row, col)) - value) - first[v]
        third[v] = result
        place_own(room2, table, row, col, place(u, v), result)


def carry_rooms(room, room_in, room2, room2_in):
    for u in (2, 3):
        for v in range(-2, COLS + 2):
            room[place(u, v)] = room_in[place(u, v)]
            room[SPOTS + place(u, v)] = room_in[SPOTS + place(u, v)]
    for v in range(-1, COLS + 1):
        room2[place(1, v)] = room2_in[place(1, v)]
        room2[place(2, v)] = room2_in[place(2, v)]
        if 0 <= v < COLS:
            room2[SPOTS + place(2, v)] = room2_in[SPOTS + place(2, v)]


def step_1a(
    tiles, signals, table, spectral, from_a, from_b, from_s, room, room2, degree, first, ghost_degree, ghost_first
):
    frame = Frame()
    factor = 2.0 / jnp.full((16, 128), spectral[0])
    room[ZERO] = jnp.zeros((32, 128), BF16)
    for u in (2, 3):
        row = frame.row(u)
        for v in range(COLS):
            col, at = frame.col(v), place(u, v)
            alive = alive_of(table, row, col)
            place_own(room, table, row, col, at, signals[row, col] * alive)
            room[SPOTS + at, 16:32] = jnp.where(heads(), alive, 0.0).astype(BF16)
            room[at, 16:32] = jnp.where(heads(), inside_of(table, row, col), 0.0).astype(BF16)
    fill_z(fill_1, frame, room, ((from_a,), (from_b,)))
    fill_x(fill_1, frame, room, (from_s,), 1, 0)
    halos = (from_a, from_b, from_s)
    half_1(frame, 2, tiles, signals, table, factor, halos, room, room2, degree, first, ghost_degree, ghost_first)


def step_1b(
    tiles, signals, table, spectral, from_a, from_b, from_x, room_in, room2_in, degree_a, first_a,
    degree, first, ghost_degree, ghost_first, second, out_a, out_b, room, room2,
):
    frame = Frame()
    factor = 2.0 / jnp.full((16, 128), spectral[0])
    room[ZERO] = jnp.zeros((32, 128), BF16)
    room2[ZERO] = jnp.zeros((16, 128), BF16)
    carry_rooms(room, room_in, room2, room2_in)
    fill_x(fill_1, frame, room, (from_x,), 4, 5)
    halos = (from_a, from_b, from_x)
    half_1(frame, 3, tiles, signals, table, factor, halos, room, room2, degree, first, ghost_degree, ghost_first)
    for u, degrees, firsts in ((2, degree_a, first_a), (3, degree, first)):
        row = frame.row(u)
        for v in range(COLS):
            col = frame.col(v)
            sums = own_product(tiles, table, row, col, room2)
            alive = alive_of(table, row, col)
            value = firsts[v]
            result = 2.0 * (factor * (degrees[v] * value - sums * alive) - value)
            second[u - 2, v] = result - signals[row, col] * alive
    for out, v, v2 in ((out_a, COLS - 1, COLS - 2), (out_b, 0, 1)):
        for u in (2, 3):
            row = frame.row(u)
            message_2(out, row, second, table, frame.col(v), u, v, u, v2, frame.col(v2), row)


def pack_x2(second, table, out_s, out_x):
    frame = Frame()
    for out, u in ((out_s, 2), (out_x, 3)):
        row = frame.row(u)
        for v in range(COLS):
            col = frame.col(v)
            message_2(out, col + 1, second, table, col, u, v, 5 - u, v, col, 1 - row)
        for at in (0, COLS + 1):
            out[at] = jnp.zeros((32, 128), BF16)


def step_3a(
    tiles, table, spectral, from_a, from_b, from_s, new_a, new_b, new_s,
    degree, first, second, ghost_degree, ghost_first, room, room2, third,
):
    frame = Frame()
    factor = 2.0 / jnp.full((16, 128), spectral[0])
    room[ZERO] = jnp.zeros((16, 128), BF16)
    for u in (2, 3):
        row = frame.row(u)
        for v in range(COLS):
            place_own(room, table, row, frame.col(v), place(u, v), second[u - 2, v])
    fill_z(fill_2, frame, room, ((new_a, from_a), (new_b, from_b)))
    fill_x(fill_2, frame, room, (new_s, from_s), 1, 0)
    half_3(
        frame, 2, tiles, table, factor, (from_a, from_b, from_s), (new_a, new_b, new_s), room, room2,
        degree, first, second, third, ghost_degree, ghost_first,
    )


def step_3b(
    tiles, signals, table, spectral, scales, from_a, from_b, from_x, new_a, new_b, new_x, room_in, room2_in,
    degree_a, degree, first_a, first, second, ghost_degree, ghost_first, third_a,
    coefficients, partial, room, room2, third,
):
    frame = Frame()
    factor = 2.0 / jnp.full((16, 128), spectral[0])
    room[ZERO] = jnp.zeros((16, 128), BF16)
    room2[ZERO] = jnp.zeros((16, 128), BF16)
    carry_rooms(room, room_in, room2, room2_in)
    fill_x(fill_2, frame, room, (new_x, from_x), 4, 5)
    half_3(
        frame, 3, tiles, table, factor, (from_a, from_b, from_x), (new_a, new_b, new_x), room, room2,
        degree, first, second, third, ghost_degree, ghost_first,
    )
    count = scales.shape[0]
    squares = [jnp.zeros((16, 128), F32) for _ in range(count)]
    for u, degrees, firsts, thirds in ((2, degree_a, first_a, third_a), (3, degree, first, third)):
        row = frame.row(u)
        for v in range(COLS):
            col = frame.col(v)
            sums = own_product(tiles, table, row, col, room2)
            alive = alive_of(table, row, col)
            value = thirds[v]
            fourth = 2.0 * (factor * (degrees[v] * value - sums * alive) - value) - second[u - 2, v]
            terms = (signals[row, col] * alive, firsts[v], second[u - 2, v], value, fourth)
            for scale in range(count):
                total = (0.5 * scales[scale, 0]) * terms[0]
                for order in range(1, len(terms)):
                    total = total + scales[scale, order] * terms[order]
                coefficients[scale, row, col] = total
                squares[scale] = squares[scale] + total * total
    block = jnp.concatenate(squares + [jnp.zeros((128 - 16 * count, 128), F32)], axis=0)
    line = jnp.sum(jnp.transpose(block), axis=0, keepdims=True)
    partial[...] = jnp.broadcast_to(line[None], partial.shape)


def in_hbm(*arrays):
    return tuple(pltpu.with_memory_space_constraint(array, pltpu.MemorySpace.HBM) for array in arrays)


def in_vmem(*arrays):
    return tuple(pltpu.with_memory_space_constraint(array, pltpu.MemorySpace.VMEM) for array in arrays)


def neighbour_pairs(devices, first):
    pairs = [(i, i + 1) for i in range(first, devices - 1, 2)]
    return pairs + [(j, i) for i, j in pairs]


def shape(dims, kind=BF16):
    return jax.ShapeDtypeStruct(dims, kind)


def shards(signals, tiles, tile_dir, tile_mask, live_rows, bound_rows, scale_coeffs, spectral_bound):
    devices_x, devices_z = lax.axis_size(GX), lax.axis_size("gy")
    devices = devices_x * devices_z
    scales, channels = scale_coeffs.shape[0], signals.shape[2]
    nodes = ROWS * COLS * 128 * devices

    def swap_z(a, b):
        return (
            lax.ppermute(a, "gy", neighbour_pairs(devices_z, 0)),
            lax.ppermute(b, "gy", neighbour_pairs(devices_z, 1)),
        )

    def swap_x(s, x):
        far = lax.ppermute(x, GX, neighbour_pairs(devices_x, 1))
        return lax.ppermute(s, "gx_2", [(0, 1), (1, 0)]), far

    def call(body, outs, in_specs, out_specs, scratch=(), aliases=None, flops=1000, mib=16):
        return pl.pallas_call(
            body,
            out_shape=outs,
            in_specs=in_specs,
            out_specs=out_specs,
            scratch_shapes=list(scratch),
            input_output_aliases=aliases or {},
            compiler_params=params(mib),
            cost_estimate=cost(flops),
        )

    tile_dir, tile_mask = jnp.swapaxes(tile_dir, 1, 2), jnp.swapaxes(tile_mask, 1, 2)
    local = (tiles, signals, tile_dir, tile_mask, live_rows, bound_rows)
    rooms = [
        pltpu.VMEM(signals.shape, F32),
        pltpu.SMEM(tile_dir.shape, jnp.int32),
        pltpu.SMEM(tile_dir.shape, jnp.int32),
        pltpu.SMEM(live_rows.shape, jnp.int32),
        pltpu.SMEM(live_rows.shape, jnp.int32),
        pltpu.SemaphoreType.DMA((2, SLOTS)),
        pltpu.SemaphoreType.DMA((5,)),
    ]
    message_z, message_x = pltpu.VMEM((ROWS, LONG, 128), BF16), pltpu.VMEM((COLS + 2, LONG, 128), BF16)
    a, b = call(pack_z, [message_z] * 2, [HBM] * 6, [VMEM] * 2, rooms)(*in_hbm(*local))
    table_shape = shape((ROWS, SLOTS + 2, COLS), jnp.int32)
    s, x, table = call(
        pack_x, [message_x] * 2 + [table_shape], [HBM] * 6, [VMEM] * 2 + [SMEM], rooms, flops=1 << 21
    )(*in_hbm(*local))
    a, b = swap_z(a, b)
    corner_room = [pltpu.VMEM((2, 2, LONG, 128), BF16), pltpu.SemaphoreType.DMA((2, 2))]
    s, x = call(
        corners_1, [message_x] * 2, [VMEM] * 2 + [ANY] * 2, [ANY] * 2, corner_room, {2: 0, 3: 1}
    )(a, b, *in_vmem(s, x))
    s, x = swap_x(s, x)

    turned = call(
        turn_tiles, [shape((ROWS, COLS, SLOTS * 128, 128))], [VMEM], [VMEM], flops=1 << 24
    )(tiles)[0]
    half = shape((COLS, channels, 128), F32)
    extra = shape((COLS + 4, channels, 128), F32)
    wide_room, room = shape((ZERO + 1, 32, 128)), shape((ZERO + 1, 16, 128))
    wide_scratch, scratch = pltpu.VMEM((ZERO + 1, 32, 128), BF16), pltpu.VMEM((ZERO + 1, 16, 128), BF16)
    short_z, short_x = pltpu.VMEM((ROWS, 32, 128), BF16), pltpu.VMEM((COLS + 2, 32, 128), BF16)
    room_1, room_2, degree_a, first_a, ghost_degree_a, ghost_first_a = call(
        step_1a, [wide_room, room, half, half, extra, extra], [VMEM] * 2 + [SMEM] * 2 + [VMEM] * 3, [VMEM] * 6, flops=1 << 25
    )(turned, signals, table, spectral_bound, a, b, s)
    degree_b, first_b, ghost_degree_b, ghost_first_b, second, a2, b2 = call(
        step_1b,
        [half, half, extra, extra, shape((ROWS, COLS, channels, 128), F32), short_z, short_z],
        [VMEM] * 2 + [SMEM] * 2 + [VMEM] * 7,
        [VMEM] * 7,
        [wide_scratch, scratch],
        flops=1 << 26,
    )(turned, signals, table, spectral_bound, a, b, x, room_1, room_2, degree_a, first_a)
    s2, x2 = call(pack_x2, [short_x] * 2, [VMEM, SMEM], [VMEM] * 2, flops=1 << 20)(second, table)
    a2, b2 = swap_z(a2, b2)
    corner_room = [pltpu.VMEM((2, 2, 32, 128), BF16), pltpu.SemaphoreType.DMA((2, 2))]
    s2, x2 = call(
        corners_2, [short_x] * 2, [VMEM] * 4 + [ANY] * 2, [ANY] * 2, corner_room, {4: 0, 5: 1}
    )(a, b, a2, b2, *in_vmem(s2, x2))
    s2, x2 = swap_x(s2, x2)
    room_1, room_2, third_a = call(
        step_3a, [room, room, half], [VMEM, SMEM, SMEM] + [VMEM] * 11, [VMEM] * 3, flops=1 << 25
    )(
        turned, table, spectral_bound, a, b, s, a2, b2, s2, degree_a, first_a, second, ghost_degree_a, ghost_first_a
    )
    totals, partial = call(
        step_3b,
        [shape((scales, ROWS, COLS, channels, 128), F32), shape((devices, 1, 128), F32)],
        [VMEM] * 2 + [SMEM] * 3 + [VMEM] * 16,
        [VMEM] * 2,
        [scratch, scratch, pltpu.VMEM((COLS, channels, 128), F32)],
        flops=1 << 26,
    )(
        turned, signals, table, spectral_bound, scale_coeffs, a, b, x, a2, b2, x2, room_1, room_2,
        degree_a, degree_b, first_a, first_b, second, ghost_degree_b, ghost_first_b, third_a,
    )
    gathered = lax.all_to_all(partial, GX_GY, 0, 0)
    energy = jnp.sum(gathered, axis=(0, 1))[: scales * channels].reshape(scales, channels) / nodes
    return (totals, energy)


def solution(mesh):
    torus = Mesh(mesh.devices.reshape(4, 4, 2, mesh.shape["gy"]), ("gx_0", "gx_1", "gx_2", "gy"))
    placed = (
        P(GX, "gy", None, None),
        P(GX, "gy", None, None, None),
        P(GX, "gy", None),
        P(GX, "gy", None),
        P(GX, "gy"),
        P(GX, "gy"),
        P(),
        P(),
    )
    return jax.shard_map(
        shards,
        mesh=torus,
        in_specs=placed,
        out_specs=(P(None, GX, "gy", None, None), P()),
        check_vma=False,
    )
```

```python
import jax
import jax.numpy as jnp
from jax import lax
from jax.experimental import pallas as pl
from jax.experimental.pallas import tpu as pltpu
from jax.sharding import Mesh
from jax.sharding import PartitionSpec as P

GX_GY = ("gx_0", "gx_1", "gx_2", "gy")
GX = ("gx_0", "gx_1", "gx_2")
F32 = jnp.float32
BF16 = jnp.bfloat16
EDGE = 32
ROWS, COLS = 2, 8
WIDE = COLS + 4
SPOTS = (ROWS + 4) * WIDE
ZERO = SPOTS
SLOTS = 4
NEAR, INFO, FAR, LONG = 32, 48, 64, 80
HIGH, LOW, OWN_HIGH, OWN_LOW = 0, 1, 2, 3
DIRS, BOUND, DEGREE, BOUND2, BOUND3, BOUND4 = 0, 1, 2, 3, 4, 5
VMEM = pl.BlockSpec(memory_space=pltpu.VMEM)
SMEM = pl.BlockSpec(memory_space=pltpu.SMEM)
ANY = pl.BlockSpec(memory_space=pl.ANY)
HBM = pl.BlockSpec(memory_space=pltpu.MemorySpace.HBM)


def params(mib):
    return pltpu.CompilerParams(vmem_limit_bytes=mib * 1024 * 1024)


def cost(flops):
    return pl.CostEstimate(flops=flops, bytes_accessed=1 << 20, transcendentals=0)


def lanes():
    return lax.broadcasted_iota(jnp.int32, (16, 128), 1)


def below(count):
    return (lanes() < count).astype(F32)


def split(value):
    high = value.astype(BF16)
    return high, value - high.astype(F32)


def info_of(rows):
    index = lax.broadcasted_iota(jnp.int32, (16, 128), 0)
    info = jnp.zeros((16, 128), F32)
    for row, value in rows.items():
        info = jnp.where(index == row, value, info)
    return info.astype(BF16)


def odd_z():
    return lax.axis_index("gy") % 2


def odd_core():
    return lax.axis_index("gx_2")


def merge(parts):
    lane = lax.broadcasted_iota(jnp.int32, parts[0].shape, 1)
    merged = parts[0]
    for index, part in enumerate(parts[1:], 1):
        merged = jnp.where(lane < EDGE * index, merged, pltpu.roll(part, EDGE * index, 1))
    return merged if len(parts) == 4 else jnp.where(lane < EDGE * len(parts), merged, 0.0)


def piece(pack, index):
    moved = pltpu.roll(pack, 128 - EDGE * index, 1) if index else pack
    return jnp.where(lanes() < EDGE, moved, 0.0)


def repeat(value):
    value = value + pltpu.roll(value, EDGE, 1)
    return value + pltpu.roll(value, 2 * EDGE, 1)


def wide(value):
    return jnp.concatenate([value, jnp.zeros((value.shape[0], 128 - value.shape[1]), value.dtype)], axis=1)


def with_head(value, line):
    return jnp.concatenate([value.astype(BF16), jnp.where(heads(), line, 0.0).astype(BF16)], axis=0)


def heads():
    return lax.broadcasted_iota(jnp.int32, (16, 128), 0) == 0


def block_message(out, at, refs, raw, row, col, row2, col2):
    signals, dirs, masks, live, bound = refs
    alive, inside = below(live[row, col]), below(bound[row, col])
    value = signals[row, col] * alive
    full = with_head(value, alive).astype(F32)
    inputs, sides = [], []
    for slot in range(SLOTS):
        side, used = dirs[row, slot, col], masks[row, slot, col] == 1
        own = jnp.where(side == 4, jnp.where(used, 1.0, 0.0), 0.0)
        inputs.append((full * own).astype(BF16))
        sides.append(jnp.full((16, 128), jnp.where(used, side, 9).astype(F32)))
    product = lax.dot_general(
        jnp.concatenate(inputs, axis=1),
        jnp.concatenate([raw[slot] for slot in range(SLOTS)], axis=1),
        (((1,), (1,)), ((), ())),
        preferred_element_type=F32,
    )
    product = wide(product)
    value = value * inside
    high, low = split(value)
    own_high, own_low = split(product[0:16])
    own_high = own_high.astype(F32)
    degree_high, degree_low = split(product[16:17])
    out[at, 0:NEAR] = merge([raw[slot].astype(F32) for slot in range(SLOTS)]).astype(BF16)
    out[at, NEAR:INFO] = merge([high.astype(F32), low, own_high, own_low]).astype(BF16)
    inside2 = below(bound[row2, col2])
    lane = lanes()
    rows = {
        DIRS: jnp.where(
            lane < EDGE, sides[0], jnp.where(lane < 2 * EDGE, sides[1], jnp.where(lane < 3 * EDGE, sides[2], sides[3]))
        ),
        BOUND: repeat(inside),
        DEGREE: jnp.broadcast_to(degree_high.astype(F32) + pltpu.roll(degree_low, EDGE, 1), (16, 128)),
        BOUND2: repeat(inside2),
    }
    out[at, INFO:FAR] = info_of(rows)
    out[at, FAR:LONG] = (signals[row2, col2] * inside2).astype(BF16)


def fetch(refs, rooms, sems):
    copies = [pltpu.make_async_copy(ref, room, sems.at[i]) for i, (ref, room) in enumerate(zip(refs, rooms))]
    for copy in copies:
        copy.start()
    return copies


def pack_z(tiles, signals, dirs, masks, live, bound, out_a, out_b, raw, signals_v, dirs_s, masks_s, live_s, bound_s, sem, sem2):
    refs = (signals_v, dirs_s, masks_s, live_s, bound_s)
    copies = fetch((signals, dirs, masks, live, bound), refs, sem2)
    odd = odd_z()
    for which in range(2):
        col = jnp.where(odd == which, COLS - 1, 0)
        copies.append(pltpu.make_async_copy(tiles.at[:, col, :, 0:EDGE, :], raw.at[which], sem.at[which]))
        copies[-1].start()
    for copy in copies:
        copy.wait()
    for which, out in enumerate((out_a, out_b)):
        right = odd == which
        col, col2 = jnp.where(right, COLS - 1, 0), jnp.where(right, COLS - 2, 1)
        for row in range(ROWS):
            block_message(out, row, refs, raw[which, row], row, col, row, col2)


def pack_x(tiles, signals, dirs, masks, live, bound, out_s, out_b, raw, signals_v, dirs_s, masks_s, live_s, bound_s, sem, sem2):
    refs = (signals_v, dirs_s, masks_s, live_s, bound_s)
    copies = fetch((signals, dirs, masks, live, bound), refs, sem2)
    core = odd_core()
    for which in range(2):
        row = jnp.where(core == which, 1, 0)
        copies.append(pltpu.make_async_copy(tiles.at[row, :, :, 0:EDGE, :], raw.at[which], sem.at[which]))
        copies[-1].start()
    for copy in copies:
        copy.wait()
    for which, out in enumerate((out_s, out_b)):
        row = jnp.where(core == which, 1, 0)
        for col in range(COLS):
            block_message(out, 1 + col, refs, raw[which, col], row, col, 1 - row, col)


def place_corners(from_a, from_b, out_s, out_b, room, sem, far, info_at):
    odd, core = odd_z(), odd_core()
    copies = []
    for side, halo in enumerate((from_a, from_b)):
        at = jnp.where(odd == side, COLS + 1, 0)
        for which, out in enumerate((out_s, out_b)):
            row = jnp.where(core == which, 1, 0)
            near = far - 16 if info_at is None else info_at - 16
            first, other = halo[row, far : far + 16].astype(F32), halo[1 - row, far : far + 16].astype(F32)
            pack = merge([halo[1 - row, near : near + 16].astype(F32), first, other])
            room[which, side, 0:far] = halo[row, 0:far]
            room[which, side, far : far + 16] = pack.astype(BF16)
            if info_at is not None:
                info = halo[row, info_at : info_at + 16].astype(F32)
                info2 = halo[1 - row, info_at : info_at + 16].astype(F32)
                index = lax.broadcasted_iota(jnp.int32, (16, 128), 0)
                for place_at, source in (
                    (BOUND2, info2[BOUND : BOUND + 1]),
                    (BOUND3, info[BOUND2 : BOUND2 + 1]),
                    (BOUND4, info2[BOUND2 : BOUND2 + 1]),
                ):
                    info = jnp.where(index == place_at, source, info)
                room[which, side, info_at : info_at + 16] = info.astype(BF16)
            copies.append(pltpu.make_async_copy(room.at[which, side], out.at[at], sem.at[which, side]))
    for copy in copies:
        copy.start()
    for copy in copies:
        copy.wait()


def corners_1(from_a, from_b, in_s, in_b, out_s, out_b, room, sem):
    del in_s, in_b
    place_corners(from_a, from_b, out_s, out_b, room, sem, FAR, INFO)


def corners_2(from_a, from_b, in_s, in_b, out_s, out_b, room, sem):
    del in_s, in_b
    place_corners(from_a, from_b, out_s, out_b, room, sem, 16, None)


def place(u, v):
    return u * WIDE + v + 2


class Frame:
    def __init__(self):
        self.odd, self.core = odd_z(), odd_core()
        self.up = 2 * self.core - 1
        self.right = 1 - 2 * self.odd

    def row(self, u):
        return 1 - self.core if u == 2 else self.core

    def col(self, v):
        return jnp.where(self.odd == 1, COLS - 1 - v, v)


def ghost_blocks(frame, u, halo_a, halo_b, halo_x):
    row = frame.row(u)
    found = [(halo_a, row, u, COLS), (halo_b, row, u, -1)]
    return found + [(halo_x, frame.col(v) + 1, 1 if u == 2 else 4, v) for v in range(-1, COLS + 1)]


def ghost_product(frame, halo, at, spot_at, room, height):
    info = halo[at, INFO:FAR].astype(F32)
    step = jnp.where(info > 5.5, 1.0, jnp.where(info > 2.5, 0.0, -1.0))
    turned = 3.0 * (frame.up.astype(F32) * step) + frame.right.astype(F32) * (info - 3.0 * step - 4.0) + 4.0
    turned = jnp.where(info > 8.5, 9.0, turned)
    turn = jnp.broadcast_to(turned[DIRS : DIRS + 1], (16, 128)).astype(BF16)
    halves = [jnp.zeros((16, 128), BF16) for _ in range(height // 16)]
    for d in (0, 1, 2, 3, 5, 6, 7, 8):
        near = room[spot_at + (d // 3 - 1) * WIDE + d % 3 - 1]
        chosen = turn == d
        halves = [jnp.where(chosen, near[16 * h : 16 * h + 16], half) for h, half in enumerate(halves)]
    inputs = halves[0] if height == 16 else jnp.concatenate(halves, axis=0)
    product = lax.dot_general(inputs, halo[at, 0:NEAR], (((1,), (1,)), ((), ())), preferred_element_type=F32)
    return wide(product)


def slot_lanes():
    return (lanes() // EDGE).astype(F32).astype(BF16)


def near_input(table, row, col, room, height):
    group = slot_lanes()
    blocks = [room[table[row, slot, col]] for slot in range(SLOTS)]
    halves = []
    for half in range(0, height, 16):
        chosen = blocks[0][half : half + 16]
        for slot in range(1, SLOTS):
            chosen = jnp.where(group == slot, blocks[slot][half : half + 16], chosen)
        halves.append(chosen)
    return halves[0] if height == 16 else jnp.concatenate(halves, axis=0)


def own_product(weights, table, row, col, room, own):
    near = near_input(table, row, col, room, own.shape[0])
    return jnp.dot(jnp.concatenate([own, own, near], axis=1), weights[row, col], preferred_element_type=F32)


def alive_of(table, row, col):
    return below(table[row, SLOTS, col])


def inside_of(table, row, col):
    return below(table[row, SLOTS + 1, col])


def place_edge(room, at, value):
    room[at, 0:16] = repeat(value).astype(BF16)


def bound_row(halo, at):
    return halo[at, INFO:FAR].astype(F32)[BOUND : BOUND + 1]


def message_2(out, at, second, weights, table, u, v, u2, v2, frame):
    row, col = frame.row(u), frame.col(v)
    value = second[u - 2, v]
    own = value.astype(BF16)
    product = jnp.dot(jnp.concatenate([own, own], axis=1), weights[row, col, 0:256], preferred_element_type=F32)
    high, low = split(value * inside_of(table, row, col))
    own_high, own_low = split(product)
    out[at, 0:16] = merge([high.astype(F32), low, own_high.astype(F32), own_low]).astype(BF16)
    out[at, 16:32] = (second[u2 - 2, v2] * inside_of(table, frame.row(u2), frame.col(v2))).astype(BF16)
    return product


def turn_tiles(
    tiles, dirs, masks, live, bound, scales, out, table, scales_out, dirs_s, masks_s, live_s, bound_s, sem
):
    refs = (dirs_s, masks_s, live_s, bound_s, scales_out)
    for copy in fetch((dirs, masks, live, bound, scales), refs, sem):
        copy.wait()

    def one(block, carry):
        row, col = block // COLS, block % COLS
        total = jnp.zeros((128, 128), F32)
        for slot in range(SLOTS):
            own = jnp.where(dirs_s[row, slot, col] == 4, jnp.where(masks_s[row, slot, col] == 1, 1.0, 0.0), 0.0)
            tile = tiles[row, col, slot]
            total = total + tile.astype(F32) * own
            out[row, col, 256 + EDGE * slot : 256 + EDGE * (slot + 1)] = jnp.transpose(tile)[0:EDGE]
        high = total.astype(BF16)
        out[row, col, 0:128] = jnp.transpose(high)
        out[row, col, 128:256] = jnp.transpose((total - high.astype(F32)).astype(BF16))
        return carry

    lax.fori_loop(0, ROWS * COLS, one, 0)
    core, odd = odd_core(), odd_z()
    down, right = (2 * core - 1) * WIDE, 1 - 2 * odd
    for row in range(ROWS):
        for col in range(COLS):
            base = place(jnp.where(core == row, 3, 2), jnp.where(odd == 1, COLS - 1 - col, col))
            for slot in range(SLOTS):
                side = dirs_s[row, slot, col]
                step = jnp.where(side > 5, 1, jnp.where(side > 2, 0, -1))
                index = base + step * down + (side - 3 * step - 4) * right
                index = jnp.where(side == 4, ZERO, index)
                table[row, slot, col] = jnp.where(masks_s[row, slot, col] == 1, index, ZERO)
            table[row, SLOTS, col] = live_s[row, col]
            table[row, SLOTS + 1, col] = bound_s[row, col]


def fill(room, halo, near, info, far, at, near_at, far_at, corner):
    place_edge(room, near_at, piece(halo[at, near : near + 16].astype(F32), HIGH))
    beyond = halo[at, far : far + 16].astype(F32)
    places = (far_at,) + corner
    for index, spot_at in enumerate(places):
        place_edge(room, spot_at, piece(beyond, index))
    if info is not None:
        lines = halo[at, info : info + 16].astype(F32)
        for spot_at, line in zip((near_at,) + places, (BOUND, BOUND2, BOUND3, BOUND4)):
            room[spot_at, 16:32] = jnp.where(heads(), lines[line : line + 1], 0.0).astype(BF16)


FIRST, SECOND = (NEAR, INFO, FAR), (0, None, 16)


def fill_z(frame, room, rows, halo_a, halo_b):
    for halo, near, far in ((halo_a, COLS, COLS + 1), (halo_b, -1, -2)):
        for u in (2, 3):
            fill(room, halo, *rows, frame.row(u), place(u, near), place(u, far), ())


def fill_x(frame, room, rows, halo, near, far):
    for v in range(-1, COLS + 1):
        beyond = {-1: -2, COLS: COLS + 1}.get(v)
        corner = () if beyond is None else (place(near, beyond), place(far, beyond))
        fill(room, halo, *rows, frame.col(v) + 1, place(near, v), place(far, v), corner)


def half_1(frame, u, weights, signals, table, factor, halos, room, room2, degree, first, ghost_degree, ghost_first):
    for number, (halo, at, gu, gv) in enumerate(ghost_blocks(frame, u, *halos)):
        pack = halo[at, NEAR:INFO].astype(F32)
        value = piece(pack, HIGH) + piece(pack, LOW)
        near = ghost_product(frame, halo, at, place(gu, gv), room, 32)
        sums = near[0:16] + (piece(pack, OWN_HIGH) + piece(pack, OWN_LOW))
        line = jnp.broadcast_to(halo[at, INFO:FAR].astype(F32)[DEGREE : DEGREE + 1], (16, 128))
        around = jnp.broadcast_to(near[16:17], (16, 128)) + (piece(line, 0) + piece(line, 1))
        result = factor * (around * value - sums) - value
        ghost_degree[number] = around
        ghost_first[number] = result
        place_edge(room2, place(gu, gv), jnp.where(lanes() < EDGE, result * bound_row(halo, at), 0.0))
    row = frame.row(u)
    for v in range(COLS):
        col = frame.col(v)
        alive = alive_of(table, row, col)
        value = signals[row, col] * alive
        sums = own_product(weights, table, row, col, room, with_head(value, alive))
        around = jnp.broadcast_to(sums[16:17], (16, 128)) * alive
        result = factor * (around * value - sums[0:16] * alive) - value
        degree[v] = around
        first[v] = result
        place_edge(room2, place(u, v), result * inside_of(table, row, col))


def half_3(frame, u, weights, table, factor, halos, fresh, room, room2, degree, first, second, products, third, ghost_degree, ghost_first):
    values = ghost_blocks(frame, u, *fresh)
    for number, (halo, at, gu, gv) in enumerate(ghost_blocks(frame, u, *halos)):
        pack = values[number][0][at, 0:16].astype(F32)
        value = piece(pack, HIGH) + piece(pack, LOW)
        sums = ghost_product(frame, halo, at, place(gu, gv), room, 16) + (piece(pack, OWN_HIGH) + piece(pack, OWN_LOW))
        result = 2.0 * (factor * (ghost_degree[number] * value - sums) - value) - ghost_first[number]
        place_edge(room2, place(gu, gv), jnp.where(lanes() < EDGE, result * bound_row(halo, at), 0.0))
    row = frame.row(u)
    for v in range(COLS):
        col = frame.col(v)
        near = near_input(table, row, col, room, 16)
        sums = products[u - 2, v] + jnp.dot(near, weights[row, col, 256:384], preferred_element_type=F32)
        value = second[u - 2, v]
        result = 2.0 * (factor * (degree[v] * value - sums * alive_of(table, row, col)) - value) - first[v]
        third[v] = result
        place_edge(room2, place(u, v), result * inside_of(table, row, col))


def carry_rooms(room, room_in, room2, room2_in):
    for v in range(-2, COLS + 2):
        for u in (2, 3):
            room[place(u, v)] = room_in[place(u, v)]
    for v in range(-1, COLS + 1):
        for u in (1, 2):
            room2[place(u, v)] = room2_in[place(u, v)]


def step_1a(
    weights, signals, table, spectral, from_a, from_b, from_s, room, room2, degree, first, ghost_degree, ghost_first
):
    frame = Frame()
    factor = 2.0 / jnp.full((16, 128), spectral[0])
    room[ZERO] = jnp.zeros((32, 128), BF16)
    for u in (2, 3):
        row = frame.row(u)
        for v in range(COLS):
            col, at = frame.col(v), place(u, v)
            inside = inside_of(table, row, col)
            place_edge(room, at, signals[row, col] * inside)
            room[at, 16:32] = jnp.where(heads(), repeat(inside), 0.0).astype(BF16)
    fill_z(frame, room, FIRST, from_a, from_b)
    fill_x(frame, room, FIRST, from_s, 1, 0)
    halos = (from_a, from_b, from_s)
    half_1(frame, 2, weights, signals, table, factor, halos, room, room2, degree, first, ghost_degree, ghost_first)


def step_1b(
    weights, signals, table, spectral, from_a, from_b, from_x, room_in, room2_in, degree_a, first_a,
    degree, first, ghost_degree, ghost_first, second, out_a, out_b, room, room2,
):
    frame = Frame()
    factor = 2.0 / jnp.full((16, 128), spectral[0])
    room[ZERO] = jnp.zeros((32, 128), BF16)
    room2[ZERO] = jnp.zeros((16, 128), BF16)
    carry_rooms(room, room_in, room2, room2_in)
    fill_x(frame, room, FIRST, from_x, 4, 5)
    halos = (from_a, from_b, from_x)
    half_1(frame, 3, weights, signals, table, factor, halos, room, room2, degree, first, ghost_degree, ghost_first)
    for u, degrees, firsts in ((2, degree_a, first_a), (3, degree, first)):
        row = frame.row(u)
        for v in range(COLS):
            col = frame.col(v)
            value = firsts[v]
            sums = own_product(weights, table, row, col, room2, value.astype(BF16))
            alive = alive_of(table, row, col)
            result = 2.0 * (factor * (degrees[v] * value - sums * alive) - value)
            second[u - 2, v] = result - signals[row, col] * alive
    for out, v, v2 in ((out_a, COLS - 1, COLS - 2), (out_b, 0, 1)):
        for u in (2, 3):
            message_2(out, frame.row(u), second, weights, table, u, v, u, v2, frame)


def pack_x2(second, weights, table, out_s, out_x, products):
    frame = Frame()
    for out, u in ((out_s, 2), (out_x, 3)):
        for v in range(COLS):
            products[u - 2, v] = message_2(out, frame.col(v) + 1, second, weights, table, u, v, 5 - u, v, frame)


def step_3a(
    weights, table, spectral, from_a, from_b, from_s, new_a, new_b, new_s,
    degree, first, second, products, ghost_degree, ghost_first, room, room2, third,
):
    frame = Frame()
    factor = 2.0 / jnp.full((16, 128), spectral[0])
    room[ZERO] = jnp.zeros((16, 128), BF16)
    for u in (2, 3):
        for v in range(COLS):
            place_edge(room, place(u, v), second[u - 2, v] * inside_of(table, frame.row(u), frame.col(v)))
    fill_z(frame, room, SECOND, new_a, new_b)
    fill_x(frame, room, SECOND, new_s, 1, 0)
    half_3(
        frame, 2, weights, table, factor, (from_a, from_b, from_s), (new_a, new_b, new_s), room, room2,
        degree, first, second, products, third, ghost_degree, ghost_first,
    )


def step_3b(
    weights, signals, table, spectral, scales, from_a, from_b, from_x, new_a, new_b, new_x, room_in, room2_in,
    degree_a, degree, first_a, first, second, products, ghost_degree, ghost_first, third_a,
    partial, third, fourths, room, room2,
):
    frame = Frame()
    factor = 2.0 / jnp.full((16, 128), spectral[0])
    room[ZERO] = jnp.zeros((16, 128), BF16)
    room2[ZERO] = jnp.zeros((16, 128), BF16)
    carry_rooms(room, room_in, room2, room2_in)
    fill_x(frame, room, SECOND, new_x, 4, 5)
    half_3(
        frame, 3, weights, table, factor, (from_a, from_b, from_x), (new_a, new_b, new_x), room, room2,
        degree, first, second, products, third, ghost_degree, ghost_first,
    )
    count = scales.shape[0]
    squares = [jnp.zeros((16, 128), F32) for _ in range(count)]
    for u, degrees, firsts, thirds in ((2, degree_a, first_a, third_a), (3, degree, first, third)):
        row = frame.row(u)
        for v in range(COLS):
            col = frame.col(v)
            value = thirds[v]
            sums = own_product(weights, table, row, col, room2, value.astype(BF16))
            alive = alive_of(table, row, col)
            fourth = 2.0 * (factor * (degrees[v] * value - sums * alive) - value) - second[u - 2, v]
            fourths[u - 2, v] = fourth
            terms = (signals[row, col] * alive, firsts[v], second[u - 2, v], value, fourth)
            for scale, total in enumerate(weighted(scales, terms)):
                squares[scale] = squares[scale] + total * total
    block = jnp.concatenate(squares + [jnp.zeros((128 - 16 * count, 128), F32)], axis=0)
    line = jnp.sum(jnp.transpose(block), axis=0, keepdims=True)
    partial[...] = jnp.broadcast_to(line[None], partial.shape)


def weighted(scales, terms):
    for scale in range(scales.shape[0]):
        total = (0.5 * scales[scale, 0]) * terms[0]
        for order in range(1, len(terms)):
            total = total + scales[scale, order] * terms[order]
        yield total


def combine(signals, table, scales, first_a, first_b, second, third_a, third_b, fourths, coefficients):
    frame = Frame()
    for u, firsts, thirds in ((2, first_a, third_a), (3, first_b, third_b)):
        row = frame.row(u)
        for v in range(COLS):
            col = frame.col(v)
            terms = (signals[row, col] * alive_of(table, row, col), firsts[v], second[u - 2, v], thirds[v], fourths[u - 2, v])
            for scale, total in enumerate(weighted(scales, terms)):
                coefficients[scale, row, col] = total


def in_hbm(*arrays):
    return tuple(pltpu.with_memory_space_constraint(array, pltpu.MemorySpace.HBM) for array in arrays)


def in_vmem(*arrays):
    return tuple(pltpu.with_memory_space_constraint(array, pltpu.MemorySpace.VMEM) for array in arrays)


def in_smem(*arrays):
    return tuple(pltpu.with_memory_space_constraint(array, pltpu.MemorySpace.SMEM) for array in arrays)


def neighbour_pairs(devices, first):
    pairs = [(i, i + 1) for i in range(first, devices - 1, 2)]
    return pairs + [(j, i) for i, j in pairs]


def shape(dims, kind=BF16):
    return jax.ShapeDtypeStruct(dims, kind)


def shards(signals, tiles, tile_dir, tile_mask, live_rows, bound_rows, scale_coeffs, spectral_bound):
    devices_x, devices_z = lax.axis_size(GX), lax.axis_size("gy")
    devices = devices_x * devices_z
    scales, channels = scale_coeffs.shape[0], signals.shape[2]
    nodes = ROWS * COLS * 128 * devices

    def swap_z(a, b):
        return (
            lax.ppermute(a, "gy", neighbour_pairs(devices_z, 0)),
            lax.ppermute(b, "gy", neighbour_pairs(devices_z, 1)),
        )

    def swap_x(s, x):
        far = lax.ppermute(x, GX, neighbour_pairs(devices_x, 1))
        return lax.ppermute(s, "gx_2", [(0, 1), (1, 0)]), far

    def call(body, outs, in_specs, out_specs, scratch=(), aliases=None, flops=1000, mib=16):
        return pl.pallas_call(
            body,
            out_shape=outs,
            in_specs=in_specs,
            out_specs=out_specs,
            scratch_shapes=list(scratch),
            input_output_aliases=aliases or {},
            compiler_params=params(mib),
            cost_estimate=cost(flops),
        )

    tile_dir, tile_mask = jnp.swapaxes(tile_dir, 1, 2), jnp.swapaxes(tile_mask, 1, 2)
    local = (tiles, signals, tile_dir, tile_mask, live_rows, bound_rows)
    rooms = [
        pltpu.VMEM((2, ROWS, SLOTS, EDGE, 128), BF16),
        pltpu.VMEM(signals.shape, F32),
        pltpu.SMEM(tile_dir.shape, jnp.int32),
        pltpu.SMEM(tile_dir.shape, jnp.int32),
        pltpu.SMEM(live_rows.shape, jnp.int32),
        pltpu.SMEM(live_rows.shape, jnp.int32),
        pltpu.SemaphoreType.DMA((2,)),
        pltpu.SemaphoreType.DMA((5,)),
    ]
    wide_rooms = [pltpu.VMEM((2, COLS, SLOTS, EDGE, 128), BF16)] + rooms[1:]
    message_z, message_x = pltpu.VMEM((ROWS, LONG, 128), BF16), pltpu.VMEM((COLS + 2, LONG, 128), BF16)
    a, b = call(pack_z, [message_z] * 2, [HBM] * 6, [VMEM] * 2, rooms)(*in_hbm(*local))
    s, x = call(pack_x, [message_x] * 2, [HBM] * 6, [VMEM] * 2, wide_rooms, flops=1 << 21)(*in_hbm(*local))
    a, b = swap_z(a, b)
    corner_room = [pltpu.VMEM((2, 2, LONG, 128), BF16), pltpu.SemaphoreType.DMA((2, 2))]
    s, x = call(
        corners_1, [message_x] * 2, [VMEM] * 2 + [ANY] * 2, [ANY] * 2, corner_room, {2: 0, 3: 1}
    )(a, b, *in_vmem(s, x))
    s, x = swap_x(s, x)

    weights, table, scale_table = call(
        turn_tiles,
        [
            shape((ROWS, COLS, 384, 128)),
            pltpu.SMEM((ROWS, SLOTS + 2, COLS), jnp.int32),
            pltpu.SMEM(scale_coeffs.shape, F32),
        ],
        [VMEM] + [HBM] * 5,
        [VMEM, SMEM, SMEM],
        rooms[2:6] + [pltpu.SemaphoreType.DMA((5,))],
        flops=1 << 24,
    )(tiles, *in_hbm(*local[2:], scale_coeffs))
    table, scale_table = in_smem(table, scale_table)
    half = shape((COLS, channels, 128), F32)
    extra = shape((COLS + 4, channels, 128), F32)
    wide_room, room = shape((ZERO + 1, 32, 128)), shape((ZERO + 1, 16, 128))
    wide_scratch, scratch = pltpu.VMEM((ZERO + 1, 32, 128), BF16), pltpu.VMEM((ZERO + 1, 16, 128), BF16)
    short_z, short_x = pltpu.VMEM((ROWS, 32, 128), BF16), pltpu.VMEM((COLS + 2, 32, 128), BF16)
    full = shape((ROWS, COLS, channels, 128), F32)
    room_1, room_2, degree_a, first_a, ghost_degree_a, ghost_first_a = call(
        step_1a, [wide_room, room, half, half, extra, extra], [VMEM] * 2 + [SMEM] * 2 + [VMEM] * 3, [VMEM] * 6, flops=1 << 25
    )(weights, signals, table, spectral_bound, a, b, s)
    degree_b, first_b, ghost_degree_b, ghost_first_b, second, a2, b2 = call(
        step_1b,
        [half, half, extra, extra, full, short_z, short_z],
        [VMEM] * 2 + [SMEM] * 2 + [VMEM] * 7,
        [VMEM] * 7,
        [wide_scratch, scratch],
        flops=1 << 26,
    )(weights, signals, table, spectral_bound, a, b, x, room_1, room_2, degree_a, first_a)
    s2, x2, products = call(
        pack_x2, [short_x] * 2 + [full], [VMEM, VMEM, SMEM], [VMEM] * 3, flops=1 << 20
    )(second, weights, table)
    a2, b2 = swap_z(a2, b2)
    corner_room = [pltpu.VMEM((2, 2, 32, 128), BF16), pltpu.SemaphoreType.DMA((2, 2))]
    s2, x2 = call(
        corners_2, [short_x] * 2, [VMEM] * 2 + [ANY] * 2, [ANY] * 2, corner_room, {2: 0, 3: 1}
    )(a2, b2, *in_vmem(s2, x2))
    s2, x2 = swap_x(s2, x2)
    room_1, room_2, third_a = call(
        step_3a, [room, room, half], [VMEM, SMEM, SMEM] + [VMEM] * 12, [VMEM] * 3, flops=1 << 25
    )(
        weights, table, spectral_bound, a, b, s, a2, b2, s2, degree_a, first_a, second, products,
        ghost_degree_a, ghost_first_a,
    )
    partial, third_b, fourth = call(
        step_3b,
        [pltpu.VMEM((devices, 1, 128), F32), half, full],
        [VMEM] * 2 + [SMEM] * 3 + [VMEM] * 17,
        [VMEM] * 3,
        [scratch, scratch],
        flops=1 << 26,
    )(
        weights, signals, table, spectral_bound, scale_table, a, b, x, a2, b2, x2, room_1, room_2,
        degree_a, degree_b, first_a, first_b, second, products, ghost_degree_b, ghost_first_b, third_a,
    )
    totals = call(
        combine,
        [shape((scales, ROWS, COLS, channels, 128), F32)],
        [VMEM, SMEM, SMEM] + [VMEM] * 6,
        [VMEM],
        flops=1 << 24,
    )(signals, table, scale_table, first_a, first_b, second, third_a, third_b, fourth)[0]
    gathered = lax.all_to_all(partial, GX_GY, 0, 0)
    energy = jnp.sum(gathered, axis=(0, 1))[: scales * channels].reshape(scales, channels) / nodes
    return (totals, energy)


def solution(mesh):
    torus = Mesh(mesh.devices.reshape(4, 4, 2, mesh.shape["gy"]), ("gx_0", "gx_1", "gx_2", "gy"))
    placed = (
        P(GX, "gy", None, None),
        P(GX, "gy", None, None, None),
        P(GX, "gy", None),
        P(GX, "gy", None),
        P(GX, "gy"),
        P(GX, "gy"),
        P(),
        P(),
    )
    return jax.shard_map(
        shards,
        mesh=torus,
        in_specs=placed,
        out_specs=(P(None, GX, "gy", None, None), P()),
        check_vma=False,
    )
```

```python
import functools

import jax
import jax.numpy as jnp
from jax import lax
from jax.experimental import pallas as pl
from jax.experimental.pallas import tpu as pltpu
from jax.sharding import Mesh
from jax.sharding import PartitionSpec as P

GX_GY = ("gx_0", "gx_1", "gx_2", "gy")
GX = ("gx_0", "gx_1", "gx_2")
F32 = jnp.float32
BF16 = jnp.bfloat16
EDGE = 32
ROWS, COLS = 2, 8
WIDE = COLS + 4
SPOTS = (ROWS + 4) * WIDE
ZERO = SPOTS
SLOTS = 4
NEAR, INFO, FAR, LONG = 32, 48, 64, 80
HIGH, LOW, OWN_HIGH, OWN_LOW = 0, 1, 2, 3
DIRS, BOUND, DEGREE, BOUND2, BOUND3, BOUND4 = 0, 1, 2, 3, 4, 5
VMEM = pl.BlockSpec(memory_space=pltpu.VMEM)
SMEM = pl.BlockSpec(memory_space=pltpu.SMEM)
ANY = pl.BlockSpec(memory_space=pl.ANY)
HBM = pl.BlockSpec(memory_space=pltpu.MemorySpace.HBM)


def params(mib):
    return pltpu.CompilerParams(vmem_limit_bytes=mib * 1024 * 1024)


def cost(flops):
    return pl.CostEstimate(flops=flops, bytes_accessed=1 << 20, transcendentals=0)


def lanes():
    return lax.broadcasted_iota(jnp.int32, (16, 128), 1)


def below(count):
    return (lanes() < count).astype(F32)


def split(value):
    high = value.astype(BF16)
    return high, value - high.astype(F32)


def info_of(rows):
    index = lax.broadcasted_iota(jnp.int32, (16, 128), 0)
    info = jnp.zeros((16, 128), F32)
    for row, value in rows.items():
        info = jnp.where(index == row, value, info)
    return info.astype(BF16)


def odd_z():
    return lax.axis_index("gy") % 2


def odd_core():
    return lax.axis_index("gx_2")


def merge(parts):
    lane = lax.broadcasted_iota(jnp.int32, parts[0].shape, 1)
    merged = parts[0]
    for index, part in enumerate(parts[1:], 1):
        merged = jnp.where(lane < EDGE * index, merged, pltpu.roll(part, EDGE * index, 1))
    return merged if len(parts) == 4 else jnp.where(lane < EDGE * len(parts), merged, 0.0)


def piece(pack, index):
    moved = pltpu.roll(pack, 128 - EDGE * index, 1) if index else pack
    return jnp.where(lanes() < EDGE, moved, 0.0)


def repeat(value):
    value = value + pltpu.roll(value, EDGE, 1)
    return value + pltpu.roll(value, 2 * EDGE, 1)


def wide(value):
    return jnp.concatenate([value, jnp.zeros((value.shape[0], 128 - value.shape[1]), value.dtype)], axis=1)


def with_head(value, line):
    return jnp.concatenate([value.astype(BF16), jnp.where(heads(), line, 0.0).astype(BF16)], axis=0)


def heads():
    return lax.broadcasted_iota(jnp.int32, (16, 128), 0) == 0


def block_message(out, at, refs, raw, row, col, row2, col2):
    signals, dirs, masks, live, bound = refs
    alive, inside = below(live[row, col]), below(bound[row, col])
    value = signals[row, col] * alive
    full = with_head(value, alive).astype(F32)
    inputs, sides = [], []
    for slot in range(SLOTS):
        side, used = dirs[row, slot, col], masks[row, slot, col] == 1
        own = jnp.where(side == 4, jnp.where(used, 1.0, 0.0), 0.0)
        inputs.append((full * own).astype(BF16))
        sides.append(jnp.full((16, 128), jnp.where(used, side, 9).astype(F32)))
    product = lax.dot_general(
        jnp.concatenate(inputs, axis=1),
        jnp.concatenate([raw[slot] for slot in range(SLOTS)], axis=1),
        (((1,), (1,)), ((), ())),
        preferred_element_type=F32,
    )
    product = wide(product)
    value = value * inside
    high, low = split(value)
    own_high, own_low = split(product[0:16])
    own_high = own_high.astype(F32)
    degree_high, degree_low = split(product[16:17])
    out[at, 0:NEAR] = merge([raw[slot].astype(F32) for slot in range(SLOTS)]).astype(BF16)
    out[at, NEAR:INFO] = merge([high.astype(F32), low, own_high, own_low]).astype(BF16)
    inside2 = below(bound[row2, col2])
    lane = lanes()
    rows = {
        DIRS: jnp.where(
            lane < EDGE, sides[0], jnp.where(lane < 2 * EDGE, sides[1], jnp.where(lane < 3 * EDGE, sides[2], sides[3]))
        ),
        BOUND: repeat(inside),
        DEGREE: jnp.broadcast_to(degree_high.astype(F32) + pltpu.roll(degree_low, EDGE, 1), (16, 128)),
        BOUND2: repeat(inside2),
    }
    out[at, INFO:FAR] = info_of(rows)
    out[at, FAR:LONG] = (signals[row2, col2] * inside2).astype(BF16)


def fetch(refs, rooms, sems):
    copies = [pltpu.make_async_copy(ref, room, sems.at[i]) for i, (ref, room) in enumerate(zip(refs, rooms))]
    for copy in copies:
        copy.start()
    return copies


def pack_z(
    tiles, signals, dirs, masks, live, bound, out_a, out_b, dirs_s, masks_s, live_s, bound_s, raw, signals_v, sem, sem2
):
    refs = (signals_v, dirs_s, masks_s, live_s, bound_s)
    copies = fetch((signals, dirs, masks, live, bound), refs, sem2)
    odd = odd_z()
    for which in range(2):
        col = jnp.where(odd == which, COLS - 1, 0)
        copies.append(pltpu.make_async_copy(tiles.at[:, col, :, 0:EDGE, :], raw.at[which], sem.at[which]))
        copies[-1].start()
    for copy in copies:
        copy.wait()
    for which, out in enumerate((out_a, out_b)):
        right = odd == which
        col, col2 = jnp.where(right, COLS - 1, 0), jnp.where(right, COLS - 2, 1)
        for row in range(ROWS):
            block_message(out, row, refs, [raw[which, row, slot] for slot in range(SLOTS)], row, col, row, col2)


def pack_x(tiles, signals, dirs, masks, live, bound, out_s, out_b):
    refs = (signals, dirs, masks, live, bound)
    core = odd_core()
    for which, out in enumerate((out_s, out_b)):
        row = jnp.where(core == which, 1, 0)
        for col in range(COLS):
            raw = [tiles[row, col, slot, 0:EDGE] for slot in range(SLOTS)]
            block_message(out, 1 + col, refs, raw, row, col, 1 - row, col)


def place_corners(from_a, from_b, out_s, out_b, room, sem, far, info_at):
    odd, core = odd_z(), odd_core()
    copies = []
    for side, halo in enumerate((from_a, from_b)):
        at = jnp.where(odd == side, COLS + 1, 0)
        for which, out in enumerate((out_s, out_b)):
            row = jnp.where(core == which, 1, 0)
            near = far - 16 if info_at is None else info_at - 16
            first, other = halo[row, far : far + 16].astype(F32), halo[1 - row, far : far + 16].astype(F32)
            pack = merge([halo[1 - row, near : near + 16].astype(F32), first, other])
            room[which, side, 0:far] = halo[row, 0:far]
            room[which, side, far : far + 16] = pack.astype(BF16)
            if info_at is not None:
                info = halo[row, info_at : info_at + 16].astype(F32)
                info2 = halo[1 - row, info_at : info_at + 16].astype(F32)
                index = lax.broadcasted_iota(jnp.int32, (16, 128), 0)
                for place_at, source in (
                    (BOUND2, info2[BOUND : BOUND + 1]),
                    (BOUND3, info[BOUND2 : BOUND2 + 1]),
                    (BOUND4, info2[BOUND2 : BOUND2 + 1]),
                ):
                    info = jnp.where(index == place_at, source, info)
                room[which, side, info_at : info_at + 16] = info.astype(BF16)
            copies.append(pltpu.make_async_copy(room.at[which, side], out.at[at], sem.at[which, side]))
    for copy in copies:
        copy.start()
    for copy in copies:
        copy.wait()


def corners_1(from_a, from_b, in_s, in_b, out_s, out_b, room, sem):
    del in_s, in_b
    place_corners(from_a, from_b, out_s, out_b, room, sem, FAR, INFO)


def corners_2(from_a, from_b, in_s, in_b, out_s, out_b, room, sem):
    del in_s, in_b
    place_corners(from_a, from_b, out_s, out_b, room, sem, 16, None)


def place(u, v):
    return u * WIDE + v + 2


class Frame:
    def __init__(self):
        self.odd, self.core = odd_z(), odd_core()
        self.up = 2 * self.core - 1
        self.right = 1 - 2 * self.odd

    def row(self, u):
        return 1 - self.core if u == 2 else self.core

    def col(self, v):
        return jnp.where(self.odd == 1, COLS - 1 - v, v)


def ghost_blocks(frame, u, halo_a, halo_b, halo_x):
    row = frame.row(u)
    found = [(halo_a, row, u, COLS), (halo_b, row, u, -1)]
    return found + [(halo_x, frame.col(v) + 1, 1 if u == 2 else 4, v) for v in range(-1, COLS + 1)]


def ghost_product(frame, halo, at, spot_at, room, height):
    info = halo[at, INFO:FAR].astype(F32)
    step = jnp.where(info > 5.5, 1.0, jnp.where(info > 2.5, 0.0, -1.0))
    turned = 3.0 * (frame.up.astype(F32) * step) + frame.right.astype(F32) * (info - 3.0 * step - 4.0) + 4.0
    turned = jnp.where(info > 8.5, 9.0, turned)
    turn = jnp.broadcast_to(turned[DIRS : DIRS + 1], (16, 128)).astype(BF16)
    halves = [jnp.zeros((16, 128), BF16) for _ in range(height // 16)]
    for d in (0, 1, 2, 3, 5, 6, 7, 8):
        near = room[spot_at + (d // 3 - 1) * WIDE + d % 3 - 1]
        chosen = turn == d
        halves = [jnp.where(chosen, near[16 * h : 16 * h + 16], half) for h, half in enumerate(halves)]
    inputs = halves[0] if height == 16 else jnp.concatenate(halves, axis=0)
    product = lax.dot_general(inputs, halo[at, 0:NEAR], (((1,), (1,)), ((), ())), preferred_element_type=F32)
    return wide(product)


def slot_lanes():
    return (lanes() // EDGE).astype(F32).astype(BF16)


def near_input(table, row, col, room, height):
    group = slot_lanes()
    blocks = [room[table[row, slot, col]] for slot in range(SLOTS)]
    halves = []
    for half in range(0, height, 16):
        chosen = blocks[0][half : half + 16]
        for slot in range(1, SLOTS):
            chosen = jnp.where(group == slot, blocks[slot][half : half + 16], chosen)
        halves.append(chosen)
    return halves[0] if height == 16 else jnp.concatenate(halves, axis=0)


def own_product(weights, table, row, col, room, own):
    near = near_input(table, row, col, room, own.shape[0])
    product = jnp.dot(jnp.concatenate([own, own], axis=1), weights[0][row, col], preferred_element_type=F32)
    return product + jnp.dot(near, weights[1][row, col], preferred_element_type=F32)


def alive_of(table, row, col):
    return below(table[row, SLOTS, col])


def inside_of(table, row, col):
    return below(table[row, SLOTS + 1, col])


def place_edge(room, at, value):
    room[at, 0:16] = repeat(value).astype(BF16)


def bound_row(halo, at):
    return halo[at, INFO:FAR].astype(F32)[BOUND : BOUND + 1]


def message_2(out, at, second, weights, table, u, v, u2, v2, frame):
    row, col = frame.row(u), frame.col(v)
    value = second[u - 2, v]
    own = value.astype(BF16)
    product = jnp.dot(jnp.concatenate([own, own], axis=1), weights[0][row, col], preferred_element_type=F32)
    high, low = split(value * inside_of(table, row, col))
    own_high, own_low = split(product)
    out[at, 0:16] = merge([high.astype(F32), low, own_high.astype(F32), own_low]).astype(BF16)
    out[at, 16:32] = (second[u2 - 2, v2] * inside_of(table, frame.row(u2), frame.col(v2))).astype(BF16)
    return product


def turn_tiles(tiles, dirs_s, masks_s, live_s, bound_s, scales, corner_out, own_out, table, scales_out, sem):
    copy = pltpu.make_async_copy(scales, scales_out, sem)
    copy.start()
    rows = lax.broadcasted_iota(jnp.int32, (128, 512), 0)
    cols = lax.broadcasted_iota(jnp.int32, (128, 512), 1)
    picked = jnp.where((rows // EDGE == cols // 128) & (rows % EDGE == cols % 128), 1.0, 0.0).astype(BF16)
    same = jnp.where(rows[:, 0:128] == cols[:, 0:128], 1.0, 0.0)
    for row in range(ROWS):
        for col in range(COLS):
            joined = jnp.concatenate([tiles[row, col, slot] for slot in range(SLOTS)], axis=1)
            owned = []
            for slot in range(SLOTS):
                own = jnp.where(dirs_s[row, slot, col] == 4, jnp.where(masks_s[row, slot, col] == 1, 1.0, 0.0), 0.0)
                owned.append((same * own).astype(BF16))
            total = lax.dot_general(
                jnp.concatenate(owned, axis=1), joined, (((1,), (1,)), ((), ())), preferred_element_type=F32
            )
            high, low = split(total)
            own_out[row, col, 0:128] = high
            own_out[row, col, 128:256] = low.astype(BF16)
            if row == 0:
                product = lax.dot_general(picked, joined, (((1,), (1,)), ((), ())), preferred_element_type=F32)
                corner_out[row, col] = product.astype(BF16)
            else:
                for slot in range(SLOTS):
                    corner_out[row, col, EDGE * slot : EDGE * (slot + 1)] = jnp.transpose(tiles[row, col, slot])[0:EDGE]
    core, odd = odd_core(), odd_z()
    down, right = (2 * core - 1) * WIDE, 1 - 2 * odd
    for row in range(ROWS):
        for col in range(COLS):
            base = place(jnp.where(core == row, 3, 2), jnp.where(odd == 1, COLS - 1 - col, col))
            for slot in range(SLOTS):
                side = dirs_s[row, slot, col]
                step = jnp.where(side > 5, 1, jnp.where(side > 2, 0, -1))
                index = base + step * down + (side - 3 * step - 4) * right
                index = jnp.where(side == 4, ZERO, index)
                table[row, slot, col] = jnp.where(masks_s[row, slot, col] == 1, index, ZERO)
            table[row, SLOTS, col] = live_s[row, col]
            table[row, SLOTS + 1, col] = bound_s[row, col]
    copy.wait()


def fill(room, halo, near, info, far, at, near_at, far_at, corner):
    place_edge(room, near_at, piece(halo[at, near : near + 16].astype(F32), HIGH))
    beyond = halo[at, far : far + 16].astype(F32)
    places = (far_at,) + corner
    for index, spot_at in enumerate(places):
        place_edge(room, spot_at, piece(beyond, index))
    if info is not None:
        lines = halo[at, info : info + 16].astype(F32)
        for spot_at, line in zip((near_at,) + places, (BOUND, BOUND2, BOUND3, BOUND4)):
            room[spot_at, 16:32] = jnp.where(heads(), lines[line : line + 1], 0.0).astype(BF16)


FIRST, SECOND = (NEAR, INFO, FAR), (0, None, 16)


def fill_z(frame, room, rows, halo_a, halo_b):
    for halo, near, far in ((halo_a, COLS, COLS + 1), (halo_b, -1, -2)):
        for u in (2, 3):
            fill(room, halo, *rows, frame.row(u), place(u, near), place(u, far), ())


def fill_x(frame, room, rows, halo, near, far):
    for v in range(-1, COLS + 1):
        beyond = {-1: -2, COLS: COLS + 1}.get(v)
        corner = () if beyond is None else (place(near, beyond), place(far, beyond))
        fill(room, halo, *rows, frame.col(v) + 1, place(near, v), place(far, v), corner)


def half_1(frame, u, weights, signals, table, factor, halos, room, room2, degree, first, ghost_degree, ghost_first):
    for number, (halo, at, gu, gv) in enumerate(ghost_blocks(frame, u, *halos)):
        pack = halo[at, NEAR:INFO].astype(F32)
        value = piece(pack, HIGH) + piece(pack, LOW)
        near = ghost_product(frame, halo, at, place(gu, gv), room, 32)
        sums = near[0:16] + (piece(pack, OWN_HIGH) + piece(pack, OWN_LOW))
        line = jnp.broadcast_to(halo[at, INFO:FAR].astype(F32)[DEGREE : DEGREE + 1], (16, 128))
        around = jnp.broadcast_to(near[16:17], (16, 128)) + (piece(line, 0) + piece(line, 1))
        result = factor * (around * value - sums) - value
        ghost_degree[number] = around
        ghost_first[number] = result
        place_edge(room2, place(gu, gv), jnp.where(lanes() < EDGE, result * bound_row(halo, at), 0.0))
    row = frame.row(u)
    for v in range(COLS):
        col = frame.col(v)
        alive = alive_of(table, row, col)
        value = signals[row, col] * alive
        sums = own_product(weights, table, row, col, room, with_head(value, alive))
        around = jnp.broadcast_to(sums[16:17], (16, 128)) * alive
        result = factor * (around * value - sums[0:16] * alive) - value
        degree[v] = around
        first[v] = result
        place_edge(room2, place(u, v), result * inside_of(table, row, col))


def half_3(frame, u, weights, table, factor, halos, fresh, room, room2, degree, first, second, products, third, ghost_degree, ghost_first):
    values = ghost_blocks(frame, u, *fresh)
    for number, (halo, at, gu, gv) in enumerate(ghost_blocks(frame, u, *halos)):
        pack = values[number][0][at, 0:16].astype(F32)
        value = piece(pack, HIGH) + piece(pack, LOW)
        sums = ghost_product(frame, halo, at, place(gu, gv), room, 16) + (piece(pack, OWN_HIGH) + piece(pack, OWN_LOW))
        result = 2.0 * (factor * (ghost_degree[number] * value - sums) - value) - ghost_first[number]
        place_edge(room2, place(gu, gv), jnp.where(lanes() < EDGE, result * bound_row(halo, at), 0.0))
    row = frame.row(u)
    for v in range(COLS):
        col = frame.col(v)
        near = near_input(table, row, col, room, 16)
        sums = products[u - 2, v] + jnp.dot(near, weights[1][row, col], preferred_element_type=F32)
        value = second[u - 2, v]
        result = 2.0 * (factor * (degree[v] * value - sums * alive_of(table, row, col)) - value) - first[v]
        third[v] = result
        place_edge(room2, place(u, v), result * inside_of(table, row, col))


def carry_rooms(room, room_in, room2, room2_in):
    for v in range(-2, COLS + 2):
        for u in (2, 3):
            room[place(u, v)] = room_in[place(u, v)]
    for v in range(-1, COLS + 1):
        for u in (1, 2):
            room2[place(u, v)] = room2_in[place(u, v)]


def step_1a(
    own_tiles, corner_tiles, signals, table, spectral, from_a, from_b, from_s, room, room2, degree, first, ghost_degree, ghost_first
):
    frame, weights = Frame(), (own_tiles, corner_tiles)
    factor = 2.0 / jnp.full((16, 128), spectral[0])
    room[ZERO] = jnp.zeros((32, 128), BF16)
    for u in (2, 3):
        row = frame.row(u)
        for v in range(COLS):
            col, at = frame.col(v), place(u, v)
            inside = inside_of(table, row, col)
            place_edge(room, at, signals[row, col] * inside)
            room[at, 16:32] = jnp.where(heads(), repeat(inside), 0.0).astype(BF16)
    fill_z(frame, room, FIRST, from_a, from_b)
    fill_x(frame, room, FIRST, from_s, 1, 0)
    halos = (from_a, from_b, from_s)
    half_1(frame, 2, weights, signals, table, factor, halos, room, room2, degree, first, ghost_degree, ghost_first)


def step_1b(
    own_tiles, corner_tiles, signals, table, spectral, from_a, from_b, from_x, room_in, room2_in, degree_a, first_a,
    degree, first, ghost_degree, ghost_first, second, out_a, out_b, room, room2,
):
    frame, weights = Frame(), (own_tiles, corner_tiles)
    factor = 2.0 / jnp.full((16, 128), spectral[0])
    room[ZERO] = jnp.zeros((32, 128), BF16)
    room2[ZERO] = jnp.zeros((16, 128), BF16)
    carry_rooms(room, room_in, room2, room2_in)
    fill_x(frame, room, FIRST, from_x, 4, 5)
    halos = (from_a, from_b, from_x)
    half_1(frame, 3, weights, signals, table, factor, halos, room, room2, degree, first, ghost_degree, ghost_first)
    for u, degrees, firsts in ((2, degree_a, first_a), (3, degree, first)):
        row = frame.row(u)
        for v in range(COLS):
            col = frame.col(v)
            value = firsts[v]
            sums = own_product(weights, table, row, col, room2, value.astype(BF16))
            alive = alive_of(table, row, col)
            result = 2.0 * (factor * (degrees[v] * value - sums * alive) - value)
            second[u - 2, v] = result - signals[row, col] * alive
    for out, v, v2 in ((out_a, COLS - 1, COLS - 2), (out_b, 0, 1)):
        for u in (2, 3):
            message_2(out, frame.row(u), second, weights, table, u, v, u, v2, frame)


def pack_x2(second, own_tiles, table, out_s, out_x, products):
    frame, weights = Frame(), (own_tiles,)
    for out, u in ((out_s, 2), (out_x, 3)):
        for v in range(COLS):
            products[u - 2, v] = message_2(out, frame.col(v) + 1, second, weights, table, u, v, 5 - u, v, frame)


def step_3a(
    own_tiles, corner_tiles, table, spectral, from_a, from_b, from_s, new_a, new_b, new_s,
    degree, first, second, products, ghost_degree, ghost_first, room, room2, third,
):
    frame, weights = Frame(), (own_tiles, corner_tiles)
    factor = 2.0 / jnp.full((16, 128), spectral[0])
    room[ZERO] = jnp.zeros((16, 128), BF16)
    for u in (2, 3):
        for v in range(COLS):
            place_edge(room, place(u, v), second[u - 2, v] * inside_of(table, frame.row(u), frame.col(v)))
    fill_z(frame, room, SECOND, new_a, new_b)
    fill_x(frame, room, SECOND, new_s, 1, 0)
    half_3(
        frame, 2, weights, table, factor, (from_a, from_b, from_s), (new_a, new_b, new_s), room, room2,
        degree, first, second, products, third, ghost_degree, ghost_first,
    )


def step_3b(
    own_tiles, corner_tiles, signals, table, spectral, scales, from_a, from_b, from_x, new_a, new_b, new_x, room_in, room2_in,
    degree_a, degree, first_a, first, second, products, ghost_degree, ghost_first, third_a,
    partial, third, fourths, room, room2,
):
    frame, weights = Frame(), (own_tiles, corner_tiles)
    factor = 2.0 / jnp.full((16, 128), spectral[0])
    room[ZERO] = jnp.zeros((16, 128), BF16)
    room2[ZERO] = jnp.zeros((16, 128), BF16)
    carry_rooms(room, room_in, room2, room2_in)
    fill_x(frame, room, SECOND, new_x, 4, 5)
    half_3(
        frame, 3, weights, table, factor, (from_a, from_b, from_x), (new_a, new_b, new_x), room, room2,
        degree, first, second, products, third, ghost_degree, ghost_first,
    )
    count = scales.shape[0]
    squares = [jnp.zeros((16, 128), F32) for _ in range(count)]
    for u, degrees, firsts, thirds in ((2, degree_a, first_a, third_a), (3, degree, first, third)):
        row = frame.row(u)
        for v in range(COLS):
            col = frame.col(v)
            value = thirds[v]
            sums = own_product(weights, table, row, col, room2, value.astype(BF16))
            alive = alive_of(table, row, col)
            fourth = 2.0 * (factor * (degrees[v] * value - sums * alive) - value) - second[u - 2, v]
            fourths[u - 2, v] = fourth
            terms = (signals[row, col] * alive, firsts[v], second[u - 2, v], value, fourth)
            for scale, total in enumerate(weighted(scales, terms)):
                squares[scale] = squares[scale] + total * total
    block = jnp.concatenate(squares + [jnp.zeros((128 - 16 * count, 128), F32)], axis=0)
    line = jnp.sum(jnp.transpose(block), axis=0, keepdims=True)
    partial[...] = jnp.broadcast_to(line[None], partial.shape)


def weighted(scales, terms):
    for scale in range(scales.shape[0]):
        total = (0.5 * scales[scale, 0]) * terms[0]
        for order in range(1, len(terms)):
            total = total + scales[scale, order] * terms[order]
        yield total


def combine(signals, table, scales, first_a, first_b, second, third_a, third_b, fourths, coefficients):
    frame = Frame()
    for u, firsts, thirds in ((2, first_a, third_a), (3, first_b, third_b)):
        row = frame.row(u)
        for v in range(COLS):
            col = frame.col(v)
            terms = (signals[row, col] * alive_of(table, row, col), firsts[v], second[u - 2, v], thirds[v], fourths[u - 2, v])
            for scale, total in enumerate(weighted(scales, terms)):
                coefficients[scale, row, col] = total


def finish(gathered, out, *, nodes):
    total = jnp.sum(gathered[...], axis=0) * (1.0 / nodes)
    scales, channels = out.shape
    for scale in range(scales):
        out[scale : scale + 1] = pltpu.roll(total, 128 - channels * scale, 1)[:, 0:channels] if scale else total[:, 0:channels]


def in_hbm(*arrays):
    return tuple(pltpu.with_memory_space_constraint(array, pltpu.MemorySpace.HBM) for array in arrays)


def in_vmem(*arrays):
    return tuple(pltpu.with_memory_space_constraint(array, pltpu.MemorySpace.VMEM) for array in arrays)


def in_smem(*arrays):
    return tuple(pltpu.with_memory_space_constraint(array, pltpu.MemorySpace.SMEM) for array in arrays)


def neighbour_pairs(devices, first):
    pairs = [(i, i + 1) for i in range(first, devices - 1, 2)]
    return pairs + [(j, i) for i, j in pairs]


def shape(dims, kind=BF16):
    return jax.ShapeDtypeStruct(dims, kind)


def shards(signals, tiles, tile_dir, tile_mask, live_rows, bound_rows, scale_coeffs, spectral_bound):
    devices_x, devices_z = lax.axis_size(GX), lax.axis_size("gy")
    devices = devices_x * devices_z
    scales, channels = scale_coeffs.shape[0], signals.shape[2]
    nodes = ROWS * COLS * 128 * devices

    def swap_z(a, b):
        b = lax.ppermute(b, "gy", neighbour_pairs(devices_z, 1))
        return lax.ppermute(a, "gy", neighbour_pairs(devices_z, 0)), b

    def swap_x(s, x):
        far = lax.ppermute(x, GX, neighbour_pairs(devices_x, 1))
        return lax.ppermute(s, "gx_2", [(0, 1), (1, 0)]), far

    def call(body, outs, in_specs, out_specs, scratch=(), aliases=None, flops=1000, mib=16):
        return pl.pallas_call(
            body,
            out_shape=outs,
            in_specs=in_specs,
            out_specs=out_specs,
            scratch_shapes=list(scratch),
            input_output_aliases=aliases or {},
            compiler_params=params(mib),
            cost_estimate=cost(flops),
        )

    tile_dir, tile_mask = jnp.swapaxes(tile_dir, 1, 2), jnp.swapaxes(tile_mask, 1, 2)
    tables = (tile_dir, tile_mask, live_rows, bound_rows)
    message_z, message_x = pltpu.VMEM((ROWS, LONG, 128), BF16), pltpu.VMEM((COLS + 2, LONG, 128), BF16)
    a, b, *tables = call(
        pack_z,
        [message_z] * 2 + [pltpu.SMEM(table.shape, jnp.int32) for table in tables],
        [HBM] * 6,
        [VMEM] * 2 + [SMEM] * 4,
        [
            pltpu.VMEM((2, ROWS, SLOTS, EDGE, 128), BF16),
            pltpu.VMEM(signals.shape, F32),
            pltpu.SemaphoreType.DMA((2,)),
            pltpu.SemaphoreType.DMA((5,)),
        ],
    )(*in_hbm(tiles, signals, *tables))
    tables = in_smem(*tables)
    s, x = call(pack_x, [message_x] * 2, [VMEM] * 2 + [SMEM] * 4, [VMEM] * 2, flops=1 << 21)(tiles, signals, *tables)
    a, b = swap_z(a, b)
    corner_room = [pltpu.VMEM((2, 2, LONG, 128), BF16), pltpu.SemaphoreType.DMA((2, 2))]
    s, x = call(
        corners_1, [message_x] * 2, [VMEM] * 2 + [ANY] * 2, [ANY] * 2, corner_room, {2: 0, 3: 1}
    )(a, b, *in_vmem(s, x))
    s, x = swap_x(s, x)

    corner_tiles, own_tiles, table, scale_table = call(
        turn_tiles,
        [
            shape((ROWS, COLS, 128, 128)),
            shape((ROWS, COLS, 256, 128)),
            pltpu.SMEM((ROWS, SLOTS + 2, COLS), jnp.int32),
            pltpu.SMEM(scale_coeffs.shape, F32),
        ],
        [VMEM] + [SMEM] * 4 + [HBM],
        [VMEM, VMEM, SMEM, SMEM],
        [pltpu.SemaphoreType.DMA],
        flops=1 << 23,
    )(tiles, *tables, *in_hbm(scale_coeffs))
    table, scale_table = in_smem(table, scale_table)
    half = shape((COLS, channels, 128), F32)
    extra = shape((COLS + 4, channels, 128), F32)
    wide_room, room = shape((ZERO + 1, 32, 128)), shape((ZERO + 1, 16, 128))
    wide_scratch, scratch = pltpu.VMEM((ZERO + 1, 32, 128), BF16), pltpu.VMEM((ZERO + 1, 16, 128), BF16)
    short_z, short_x = pltpu.VMEM((ROWS, 32, 128), BF16), pltpu.VMEM((COLS + 2, 32, 128), BF16)
    full = shape((ROWS, COLS, channels, 128), F32)
    room_1, room_2, degree_a, first_a, ghost_degree_a, ghost_first_a = call(
        step_1a, [wide_room, room, half, half, extra, extra], [VMEM] * 3 + [SMEM] * 2 + [VMEM] * 3, [VMEM] * 6, flops=1 << 25
    )(own_tiles, corner_tiles, signals, table, spectral_bound, a, b, s)
    degree_b, first_b, ghost_degree_b, ghost_first_b, second, a2, b2 = call(
        step_1b,
        [half, half, extra, extra, full, short_z, short_z],
        [VMEM] * 3 + [SMEM] * 2 + [VMEM] * 7,
        [VMEM] * 7,
        [wide_scratch, scratch],
        flops=1 << 26,
    )(own_tiles, corner_tiles, signals, table, spectral_bound, a, b, x, room_1, room_2, degree_a, first_a)
    s2, x2, products = call(
        pack_x2, [short_x] * 2 + [full], [VMEM, VMEM, SMEM], [VMEM] * 3, flops=1 << 20
    )(second, own_tiles, table)
    a2, b2 = swap_z(a2, b2)
    corner_room = [pltpu.VMEM((2, 2, 32, 128), BF16), pltpu.SemaphoreType.DMA((2, 2))]
    s2, x2 = call(
        corners_2, [short_x] * 2, [VMEM] * 2 + [ANY] * 2, [ANY] * 2, corner_room, {2: 0, 3: 1}
    )(a2, b2, *in_vmem(s2, x2))
    s2, x2 = swap_x(s2, x2)
    room_1, room_2, third_a = call(
        step_3a, [room, room, half], [VMEM, VMEM, SMEM, SMEM] + [VMEM] * 12, [VMEM] * 3, flops=1 << 25
    )(
        own_tiles, corner_tiles, table, spectral_bound, a, b, s, a2, b2, s2, degree_a, first_a, second, products,
        ghost_degree_a, ghost_first_a,
    )
    partial, third_b, fourth = call(
        step_3b,
        [pltpu.VMEM((devices, 1, 128), F32), half, full],
        [VMEM] * 3 + [SMEM] * 3 + [VMEM] * 17,
        [VMEM] * 3,
        [scratch, scratch],
        flops=1 << 26,
    )(
        own_tiles, corner_tiles, signals, table, spectral_bound, scale_table, a, b, x, a2, b2, x2, room_1, room_2,
        degree_a, degree_b, first_a, first_b, second, products, ghost_degree_b, ghost_first_b, third_a,
    )
    totals = call(
        combine,
        [shape((scales, ROWS, COLS, channels, 128), F32)],
        [VMEM, SMEM, SMEM] + [VMEM] * 6,
        [VMEM],
        flops=1 << 24,
    )(signals, table, scale_table, first_a, first_b, second, third_a, third_b, fourth)[0]
    gathered = lax.all_to_all(partial, GX_GY, 0, 0)
    energy = pl.pallas_call(
        functools.partial(finish, nodes=nodes),
        out_shape=shape((scales, channels), F32),
        in_specs=[VMEM],
        out_specs=VMEM,
        compiler_params=params(8),
        name="finish",
    )(gathered)
    return (totals, energy)


def solution(mesh):
    torus = Mesh(mesh.devices.reshape(4, 4, 2, mesh.shape["gy"]), ("gx_0", "gx_1", "gx_2", "gy"))
    placed = (
        P(GX, "gy", None, None),
        P(GX, "gy", None, None, None),
        P(GX, "gy", None),
        P(GX, "gy", None),
        P(GX, "gy"),
        P(GX, "gy"),
        P(),
        P(),
    )
    return jax.shard_map(
        shards,
        mesh=torus,
        in_specs=placed,
        out_specs=(P(None, GX, "gy", None, None), P()),
        check_vma=False,
    )
```

```python
import functools

import jax
import jax.numpy as jnp
from jax import lax
from jax.experimental import pallas as pl
from jax.experimental.pallas import tpu as pltpu
from jax.sharding import Mesh
from jax.sharding import PartitionSpec as P

GX_GY = ("gx_0", "gx_1", "gx_2", "gy")
GX = ("gx_0", "gx_1", "gx_2")
F32 = jnp.float32
BF16 = jnp.bfloat16
EDGE = 32
ROWS, COLS = 2, 8
WIDE = COLS + 4
SPOTS = (ROWS + 4) * WIDE
ZERO = SPOTS
SLOTS = 4
NEAR, FAR, LONG = 32, 48, 64
HIGH, LOW, OWN_HIGH, OWN_LOW = 0, 1, 2, 3
INFO = 3
BOUND, BOUND2, BOUND3, BOUND4, DEGREE, DIRS = 0, 1, 2, 3, 4, 6
VMEM = pl.BlockSpec(memory_space=pltpu.VMEM)
SMEM = pl.BlockSpec(memory_space=pltpu.SMEM)
ANY = pl.BlockSpec(memory_space=pl.ANY)
HBM = pl.BlockSpec(memory_space=pltpu.MemorySpace.HBM)


def params(mib):
    return pltpu.CompilerParams(vmem_limit_bytes=mib * 1024 * 1024)


def cost(flops):
    return pl.CostEstimate(flops=flops, bytes_accessed=1 << 20, transcendentals=0)


def lanes():
    return lax.broadcasted_iota(jnp.int32, (16, 128), 1)


def below(count):
    return (lanes() < count).astype(F32)


def split(value):
    high = value.astype(BF16)
    return high, value - high.astype(F32)


def info_of(rows):
    index = lax.broadcasted_iota(jnp.int32, (16, 128), 0)
    info = jnp.zeros((16, 128), F32)
    for row, value in rows.items():
        info = jnp.where(index == row, value, info)
    return info


def odd_z():
    return lax.axis_index("gy") % 2


def odd_core():
    return lax.axis_index("gx_2")


def merge(parts):
    lane = lax.broadcasted_iota(jnp.int32, parts[0].shape, 1)
    merged = parts[0]
    for index, part in enumerate(parts[1:], 1):
        merged = jnp.where(lane < EDGE * index, merged, pltpu.roll(part, EDGE * index, 1))
    return merged if len(parts) == 4 else jnp.where(lane < EDGE * len(parts), merged, 0.0)


def piece(pack, index):
    moved = pltpu.roll(pack, 128 - EDGE * index, 1) if index else pack
    return jnp.where(lanes() < EDGE, moved, 0.0)


def repeat(value):
    value = value + pltpu.roll(value, EDGE, 1)
    return value + pltpu.roll(value, 2 * EDGE, 1)


def wide(value):
    return jnp.concatenate([value, jnp.zeros((value.shape[0], 128 - value.shape[1]), value.dtype)], axis=1)


def with_head(value, line):
    return jnp.concatenate([value.astype(BF16), jnp.where(heads(), line, 0.0).astype(BF16)], axis=0)


def heads():
    return lax.broadcasted_iota(jnp.int32, (16, 128), 0) == 0


def block_message(out, at, refs, raw, row, col, row2, col2):
    signals, dirs, masks, live, bound = refs
    alive, inside = below(live[row, col]), below(bound[row, col])
    value = signals[row, col] * alive
    full = with_head(value, alive).astype(F32)
    inputs, sides = [], []
    for slot in range(SLOTS):
        side, used = dirs[row, slot, col], masks[row, slot, col] == 1
        own = jnp.where(side == 4, jnp.where(used, 1.0, 0.0), 0.0)
        inputs.append((full * own).astype(BF16))
        sides.append(jnp.full((16, 128), jnp.where(used, side, 9).astype(F32)))
    product = lax.dot_general(
        jnp.concatenate(inputs, axis=1),
        jnp.concatenate([raw[slot] for slot in range(SLOTS)], axis=1),
        (((1,), (1,)), ((), ())),
        preferred_element_type=F32,
    )
    product = wide(product)
    value = value * inside
    high, low = split(value)
    own_high, own_low = split(product[0:16])
    own_high = own_high.astype(F32)
    degree_high, degree_low = split(product[16:17])
    out[at, 0:NEAR] = merge([raw[slot].astype(F32) for slot in range(SLOTS)]).astype(BF16)
    out[at, NEAR:FAR] = merge([high.astype(F32), low, own_high, own_low]).astype(BF16)
    inside2 = below(bound[row2, col2])
    rows = {BOUND: inside, BOUND2: inside2, DEGREE: degree_high.astype(F32), DEGREE + 1: degree_low}
    rows.update({DIRS + slot: side for slot, side in enumerate(sides)})
    second = signals[row2, col2] * inside2
    out[at, FAR:LONG] = merge([second, jnp.zeros_like(second), jnp.zeros_like(second), info_of(rows)]).astype(BF16)


def fetch(refs, rooms, sems):
    copies = [pltpu.make_async_copy(ref, room, sems.at[i]) for i, (ref, room) in enumerate(zip(refs, rooms))]
    for copy in copies:
        copy.start()
    return copies


def pack_z(
    tiles, signals, dirs, masks, live, bound, out_a, out_b, dirs_s, masks_s, live_s, bound_s, raw, signals_v, sem, sem2
):
    refs = (signals_v, dirs_s, masks_s, live_s, bound_s)
    copies = fetch((signals, dirs, masks, live, bound), refs, sem2)
    odd = odd_z()
    for which in range(2):
        col = jnp.where(odd == which, COLS - 1, 0)
        copies.append(pltpu.make_async_copy(tiles.at[:, col, :, 0:EDGE, :], raw.at[which], sem.at[which]))
        copies[-1].start()
    for copy in copies:
        copy.wait()
    for which, out in enumerate((out_a, out_b)):
        right = odd == which
        col, col2 = jnp.where(right, COLS - 1, 0), jnp.where(right, COLS - 2, 1)
        for row in range(ROWS):
            block_message(out, row, refs, [raw[which, row, slot] for slot in range(SLOTS)], row, col, row, col2)


def pack_x(tiles, signals, dirs, masks, live, bound, out_s, out_b):
    refs = (signals, dirs, masks, live, bound)
    core = odd_core()
    for which, out in enumerate((out_s, out_b)):
        row = jnp.where(core == which, 1, 0)
        for col in range(COLS):
            raw = [tiles[row, col, slot, 0:EDGE] for slot in range(SLOTS)]
            block_message(out, 1 + col, refs, raw, row, col, 1 - row, col)


def place_corners(from_a, from_b, out_s, out_b, room, sem, near, far, with_info):
    odd, core = odd_z(), odd_core()
    copies = []
    for side, halo in enumerate((from_a, from_b)):
        at = jnp.where(odd == side, COLS + 1, 0)
        for which, out in enumerate((out_s, out_b)):
            row = jnp.where(core == which, 1, 0)
            first, other = halo[row, far : far + 16].astype(F32), halo[1 - row, far : far + 16].astype(F32)
            parts = [halo[1 - row, near : near + 16].astype(F32), first, other]
            if with_info:
                info, info2 = piece(first, INFO), piece(other, INFO)
                index = lax.broadcasted_iota(jnp.int32, (16, 128), 0)
                for line, source in ((BOUND4, info2[BOUND2 : BOUND2 + 1]), (BOUND3, info[BOUND2 : BOUND2 + 1])):
                    info = jnp.where(index == line, source, info)
                parts.append(jnp.where(index == BOUND2, info2[BOUND : BOUND + 1], info))
            room[which, side, 0:far] = halo[row, 0:far]
            room[which, side, far : far + 16] = merge(parts).astype(BF16)
            copies.append(pltpu.make_async_copy(room.at[which, side], out.at[at], sem.at[which, side]))
    for copy in copies:
        copy.start()
    for copy in copies:
        copy.wait()


def corners_1(from_a, from_b, in_s, in_b, out_s, out_b, room, sem):
    del in_s, in_b
    place_corners(from_a, from_b, out_s, out_b, room, sem, NEAR, FAR, True)


def corners_2(from_a, from_b, in_s, in_b, out_s, out_b, room, sem):
    del in_s, in_b
    place_corners(from_a, from_b, out_s, out_b, room, sem, 0, 16, False)


def place(u, v):
    return u * WIDE + v + 2


class Frame:
    def __init__(self):
        self.odd, self.core = odd_z(), odd_core()
        self.up = 2 * self.core - 1
        self.right = 1 - 2 * self.odd

    def row(self, u):
        return 1 - self.core if u == 2 else self.core

    def col(self, v):
        return jnp.where(self.odd == 1, COLS - 1 - v, v)


def ghost_blocks(frame, u, halo_a, halo_b, halo_x):
    row = frame.row(u)
    found = [(halo_a, row, u, COLS), (halo_b, row, u, -1)]
    return found + [(halo_x, frame.col(v) + 1, 1 if u == 2 else 4, v) for v in range(-1, COLS + 1)]


def info_part(halo, at):
    return piece(halo[at, FAR:LONG].astype(F32), INFO)


def ghost_product(frame, halo, at, info, spot_at, room, height):
    side = merge([info[DIRS + slot : DIRS + slot + 1] for slot in range(SLOTS)])
    step = jnp.where(side > 5.5, 1.0, jnp.where(side > 2.5, 0.0, -1.0))
    turned = 3.0 * (frame.up.astype(F32) * step) + frame.right.astype(F32) * (side - 3.0 * step - 4.0) + 4.0
    turned = jnp.where(side > 8.5, 9.0, turned)
    turn = jnp.broadcast_to(turned, (16, 128)).astype(BF16)
    halves = [jnp.zeros((16, 128), BF16) for _ in range(height // 16)]
    for d in (0, 1, 2, 3, 5, 6, 7, 8):
        near = room[spot_at + (d // 3 - 1) * WIDE + d % 3 - 1]
        chosen = turn == d
        halves = [jnp.where(chosen, near[16 * h : 16 * h + 16], half) for h, half in enumerate(halves)]
    inputs = halves[0] if height == 16 else jnp.concatenate(halves, axis=0)
    product = lax.dot_general(inputs, halo[at, 0:NEAR], (((1,), (1,)), ((), ())), preferred_element_type=F32)
    return wide(product)


def slot_lanes():
    return (lanes() // EDGE).astype(F32).astype(BF16)


def near_input(table, row, col, room, height):
    group = slot_lanes()
    blocks = [room[table[row, slot, col]] for slot in range(SLOTS)]
    halves = []
    for half in range(0, height, 16):
        chosen = blocks[0][half : half + 16]
        for slot in range(1, SLOTS):
            chosen = jnp.where(group == slot, blocks[slot][half : half + 16], chosen)
        halves.append(chosen)
    return halves[0] if height == 16 else jnp.concatenate(halves, axis=0)


def own_product(weights, table, row, col, room, own):
    near = near_input(table, row, col, room, own.shape[0])
    product = jnp.dot(jnp.concatenate([own, own], axis=1), weights[0][row, col], preferred_element_type=F32)
    return product + jnp.dot(near, weights[1][row, col], preferred_element_type=F32)


def alive_of(table, row, col):
    return below(table[row, SLOTS, col])


def inside_of(table, row, col):
    return below(table[row, SLOTS + 1, col])


def place_edge(room, at, value):
    room[at, 0:16] = repeat(value).astype(BF16)


def message_2(out, at, second, weights, table, u, v, u2, v2, frame):
    row, col = frame.row(u), frame.col(v)
    value = second[u - 2, v]
    own = value.astype(BF16)
    product = jnp.dot(jnp.concatenate([own, own], axis=1), weights[0][row, col], preferred_element_type=F32)
    high, low = split(value * inside_of(table, row, col))
    own_high, own_low = split(product)
    out[at, 0:16] = merge([high.astype(F32), low, own_high.astype(F32), own_low]).astype(BF16)
    out[at, 16:32] = (second[u2 - 2, v2] * inside_of(table, frame.row(u2), frame.col(v2))).astype(BF16)
    return product


def turn_tiles(tiles, dirs_s, masks_s, live_s, bound_s, scales, corner_out, own_out, table, scales_out, sem):
    copy = pltpu.make_async_copy(scales, scales_out, sem)
    copy.start()
    rows = lax.broadcasted_iota(jnp.int32, (128, 512), 0)
    cols = lax.broadcasted_iota(jnp.int32, (128, 512), 1)
    picked = jnp.where((rows // EDGE == cols // 128) & (rows % EDGE == cols % 128), 1.0, 0.0).astype(BF16)
    same = jnp.where(rows[:, 0:128] == cols[:, 0:128], 1.0, 0.0)
    for row in range(ROWS):
        for col in range(COLS):
            joined = jnp.concatenate([tiles[row, col, slot] for slot in range(SLOTS)], axis=1)
            owned = []
            for slot in range(SLOTS):
                own = jnp.where(dirs_s[row, slot, col] == 4, jnp.where(masks_s[row, slot, col] == 1, 1.0, 0.0), 0.0)
                owned.append((same * own).astype(BF16))
            total = lax.dot_general(
                jnp.concatenate(owned, axis=1), joined, (((1,), (1,)), ((), ())), preferred_element_type=F32
            )
            high, low = split(total)
            own_out[row, col, 0:128] = high
            own_out[row, col, 128:256] = low.astype(BF16)
            if row == 0:
                product = lax.dot_general(picked, joined, (((1,), (1,)), ((), ())), preferred_element_type=F32)
                corner_out[row, col] = product.astype(BF16)
            else:
                for slot in range(SLOTS):
                    corner_out[row, col, EDGE * slot : EDGE * (slot + 1)] = jnp.transpose(tiles[row, col, slot])[0:EDGE]
    core, odd = odd_core(), odd_z()
    down, right = (2 * core - 1) * WIDE, 1 - 2 * odd
    for row in range(ROWS):
        for col in range(COLS):
            base = place(jnp.where(core == row, 3, 2), jnp.where(odd == 1, COLS - 1 - col, col))
            for slot in range(SLOTS):
                side = dirs_s[row, slot, col]
                step = jnp.where(side > 5, 1, jnp.where(side > 2, 0, -1))
                index = base + step * down + (side - 3 * step - 4) * right
                index = jnp.where(side == 4, ZERO, index)
                table[row, slot, col] = jnp.where(masks_s[row, slot, col] == 1, index, ZERO)
            table[row, SLOTS, col] = live_s[row, col]
            table[row, SLOTS + 1, col] = bound_s[row, col]
    copy.wait()


def fill(room, halo, near, far, with_info, at, near_at, far_at, corner):
    place_edge(room, near_at, piece(halo[at, near : near + 16].astype(F32), HIGH))
    beyond = halo[at, far : far + 16].astype(F32)
    places = (far_at,) + corner
    for index, spot_at in enumerate(places):
        place_edge(room, spot_at, piece(beyond, index))
    if with_info:
        lines = repeat(piece(beyond, INFO))
        for spot_at, line in zip((near_at,) + places, (BOUND, BOUND2, BOUND3, BOUND4)):
            room[spot_at, 16:32] = jnp.where(heads(), lines[line : line + 1], 0.0).astype(BF16)


FIRST, SECOND = (NEAR, FAR, True), (0, 16, False)


def fill_z(frame, room, rows, halo_a, halo_b):
    for halo, near, far in ((halo_a, COLS, COLS + 1), (halo_b, -1, -2)):
        for u in (2, 3):
            fill(room, halo, *rows, frame.row(u), place(u, near), place(u, far), ())


def fill_x(frame, room, rows, halo, near, far):
    for v in range(-1, COLS + 1):
        beyond = {-1: -2, COLS: COLS + 1}.get(v)
        corner = () if beyond is None else (place(near, beyond), place(far, beyond))
        fill(room, halo, *rows, frame.col(v) + 1, place(near, v), place(far, v), corner)


def half_1(frame, u, weights, signals, table, factor, halos, room, room2, degree, first, ghost_degree, ghost_first):
    for number, (halo, at, gu, gv) in enumerate(ghost_blocks(frame, u, *halos)):
        pack, info = halo[at, NEAR:FAR].astype(F32), info_part(halo, at)
        value = piece(pack, HIGH) + piece(pack, LOW)
        near = ghost_product(frame, halo, at, info, place(gu, gv), room, 32)
        sums = near[0:16] + (piece(pack, OWN_HIGH) + piece(pack, OWN_LOW))
        around = near[16:17] + (info[DEGREE : DEGREE + 1] + info[DEGREE + 1 : DEGREE + 2])
        around = jnp.broadcast_to(around, (16, 128))
        result = factor * (around * value - sums) - value
        ghost_degree[number] = around
        ghost_first[number] = result
        place_edge(room2, place(gu, gv), jnp.where(lanes() < EDGE, result * info[BOUND : BOUND + 1], 0.0))
    row = frame.row(u)
    for v in range(COLS):
        col = frame.col(v)
        alive = alive_of(table, row, col)
        value = signals[row, col] * alive
        sums = own_product(weights, table, row, col, room, with_head(value, alive))
        around = jnp.broadcast_to(sums[16:17], (16, 128)) * alive
        result = factor * (around * value - sums[0:16] * alive) - value
        degree[v] = around
        first[v] = result
        place_edge(room2, place(u, v), result * inside_of(table, row, col))


def half_3(frame, u, weights, table, factor, halos, fresh, room, room2, degree, first, second, products, third, ghost_degree, ghost_first):
    values = ghost_blocks(frame, u, *fresh)
    for number, (halo, at, gu, gv) in enumerate(ghost_blocks(frame, u, *halos)):
        pack, info = values[number][0][at, 0:16].astype(F32), info_part(halo, at)
        value = piece(pack, HIGH) + piece(pack, LOW)
        sums = ghost_product(frame, halo, at, info, place(gu, gv), room, 16) + (piece(pack, OWN_HIGH) + piece(pack, OWN_LOW))
        result = 2.0 * (factor * (ghost_degree[number] * value - sums) - value) - ghost_first[number]
        place_edge(room2, place(gu, gv), jnp.where(lanes() < EDGE, result * info[BOUND : BOUND + 1], 0.0))
    row = frame.row(u)
    for v in range(COLS):
        col = frame.col(v)
        near = near_input(table, row, col, room, 16)
        sums = products[u - 2, v] + jnp.dot(near, weights[1][row, col], preferred_element_type=F32)
        value = second[u - 2, v]
        result = 2.0 * (factor * (degree[v] * value - sums * alive_of(table, row, col)) - value) - first[v]
        third[v] = result
        place_edge(room2, place(u, v), result * inside_of(table, row, col))


def carry_rooms(room, room_in, room2, room2_in):
    for v in range(-2, COLS + 2):
        for u in (2, 3):
            room[place(u, v)] = room_in[place(u, v)]
    for v in range(-1, COLS + 1):
        for u in (1, 2):
            room2[place(u, v)] = room2_in[place(u, v)]


def step_1a(
    own_tiles, corner_tiles, signals, table, spectral, from_a, from_b, from_s, room, room2, degree, first, ghost_degree, ghost_first
):
    frame, weights = Frame(), (own_tiles, corner_tiles)
    factor = 2.0 / jnp.full((16, 128), spectral[0])
    room[ZERO] = jnp.zeros((32, 128), BF16)
    for u in (2, 3):
        row = frame.row(u)
        for v in range(COLS):
            col, at = frame.col(v), place(u, v)
            inside = inside_of(table, row, col)
            place_edge(room, at, signals[row, col] * inside)
            room[at, 16:32] = jnp.where(heads(), repeat(inside), 0.0).astype(BF16)
    fill_z(frame, room, FIRST, from_a, from_b)
    fill_x(frame, room, FIRST, from_s, 1, 0)
    halos = (from_a, from_b, from_s)
    half_1(frame, 2, weights, signals, table, factor, halos, room, room2, degree, first, ghost_degree, ghost_first)


def step_1b(
    own_tiles, corner_tiles, signals, table, spectral, from_a, from_b, from_x, room_in, room2_in, degree_a, first_a,
    degree, first, ghost_degree, ghost_first, second, out_a, out_b, room, room2,
):
    frame, weights = Frame(), (own_tiles, corner_tiles)
    factor = 2.0 / jnp.full((16, 128), spectral[0])
    room[ZERO] = jnp.zeros((32, 128), BF16)
    room2[ZERO] = jnp.zeros((16, 128), BF16)
    carry_rooms(room, room_in, room2, room2_in)
    fill_x(frame, room, FIRST, from_x, 4, 5)
    halos = (from_a, from_b, from_x)
    half_1(frame, 3, weights, signals, table, factor, halos, room, room2, degree, first, ghost_degree, ghost_first)
    for u, degrees, firsts in ((2, degree_a, first_a), (3, degree, first)):
        row = frame.row(u)
        for v in range(COLS):
            col = frame.col(v)
            value = firsts[v]
            sums = own_product(weights, table, row, col, room2, value.astype(BF16))
            alive = alive_of(table, row, col)
            result = 2.0 * (factor * (degrees[v] * value - sums * alive) - value)
            second[u - 2, v] = result - signals[row, col] * alive
    for out, v, v2 in ((out_a, COLS - 1, COLS - 2), (out_b, 0, 1)):
        for u in (2, 3):
            message_2(out, frame.row(u), second, weights, table, u, v, u, v2, frame)


def pack_x2(second, own_tiles, table, out_s, out_x, products):
    frame, weights = Frame(), (own_tiles,)
    for out, u in ((out_s, 2), (out_x, 3)):
        for v in range(COLS):
            products[u - 2, v] = message_2(out, frame.col(v) + 1, second, weights, table, u, v, 5 - u, v, frame)


def step_3a(
    own_tiles, corner_tiles, table, spectral, from_a, from_b, from_s, new_a, new_b, new_s,
    degree, first, second, products, ghost_degree, ghost_first, room, room2, third,
):
    frame, weights = Frame(), (own_tiles, corner_tiles)
    factor = 2.0 / jnp.full((16, 128), spectral[0])
    room[ZERO] = jnp.zeros((16, 128), BF16)
    for u in (2, 3):
        for v in range(COLS):
            place_edge(room, place(u, v), second[u - 2, v] * inside_of(table, frame.row(u), frame.col(v)))
    fill_z(frame, room, SECOND, new_a, new_b)
    fill_x(frame, room, SECOND, new_s, 1, 0)
    half_3(
        frame, 2, weights, table, factor, (from_a, from_b, from_s), (new_a, new_b, new_s), room, room2,
        degree, first, second, products, third, ghost_degree, ghost_first,
    )


def step_3b(
    own_tiles, corner_tiles, signals, table, spectral, scales, from_a, from_b, from_x, new_a, new_b, new_x, room_in, room2_in,
    degree_a, degree, first_a, first, second, products, ghost_degree, ghost_first, third_a,
    partial, third, fourths, room, room2,
):
    frame, weights = Frame(), (own_tiles, corner_tiles)
    factor = 2.0 / jnp.full((16, 128), spectral[0])
    room[ZERO] = jnp.zeros((16, 128), BF16)
    room2[ZERO] = jnp.zeros((16, 128), BF16)
    carry_rooms(room, room_in, room2, room2_in)
    fill_x(frame, room, SECOND, new_x, 4, 5)
    half_3(
        frame, 3, weights, table, factor, (from_a, from_b, from_x), (new_a, new_b, new_x), room, room2,
        degree, first, second, products, third, ghost_degree, ghost_first,
    )
    count = scales.shape[0]
    squares = [jnp.zeros((16, 128), F32) for _ in range(count)]
    for u, degrees, firsts, thirds in ((2, degree_a, first_a, third_a), (3, degree, first, third)):
        row = frame.row(u)
        for v in range(COLS):
            col = frame.col(v)
            value = thirds[v]
            sums = own_product(weights, table, row, col, room2, value.astype(BF16))
            alive = alive_of(table, row, col)
            fourth = 2.0 * (factor * (degrees[v] * value - sums * alive) - value) - second[u - 2, v]
            fourths[u - 2, v] = fourth
            terms = (signals[row, col] * alive, firsts[v], second[u - 2, v], value, fourth)
            for scale, total in enumerate(weighted(scales, terms)):
                squares[scale] = squares[scale] + total * total
    block = jnp.concatenate(squares + [jnp.zeros((128 - 16 * count, 128), F32)], axis=0)
    line = jnp.sum(jnp.transpose(block), axis=0, keepdims=True)
    partial[...] = jnp.broadcast_to(line[None], partial.shape)


def weighted(scales, terms):
    for scale in range(scales.shape[0]):
        total = (0.5 * scales[scale, 0]) * terms[0]
        for order in range(1, len(terms)):
            total = total + scales[scale, order] * terms[order]
        yield total


def combine(signals, table, scales, first_a, first_b, second, third_a, third_b, fourths, coefficients):
    frame = Frame()
    for u, firsts, thirds in ((2, first_a, third_a), (3, first_b, third_b)):
        row = frame.row(u)
        for v in range(COLS):
            col = frame.col(v)
            terms = (signals[row, col] * alive_of(table, row, col), firsts[v], second[u - 2, v], thirds[v], fourths[u - 2, v])
            for scale, total in enumerate(weighted(scales, terms)):
                coefficients[scale, row, col] = total


def finish(gathered, out, *, nodes):
    total = jnp.sum(gathered[...], axis=0) * (1.0 / nodes)
    scales, channels = out.shape
    for scale in range(scales):
        out[scale : scale + 1] = pltpu.roll(total, 128 - channels * scale, 1)[:, 0:channels] if scale else total[:, 0:channels]


def in_hbm(*arrays):
    return tuple(pltpu.with_memory_space_constraint(array, pltpu.MemorySpace.HBM) for array in arrays)


def in_vmem(*arrays):
    return tuple(pltpu.with_memory_space_constraint(array, pltpu.MemorySpace.VMEM) for array in arrays)


def in_smem(*arrays):
    return tuple(pltpu.with_memory_space_constraint(array, pltpu.MemorySpace.SMEM) for array in arrays)


def neighbour_pairs(devices, first):
    pairs = [(i, i + 1) for i in range(first, devices - 1, 2)]
    return pairs + [(j, i) for i, j in pairs]


def shape(dims, kind=BF16):
    return jax.ShapeDtypeStruct(dims, kind)


def shards(signals, tiles, tile_dir, tile_mask, live_rows, bound_rows, scale_coeffs, spectral_bound):
    devices_x, devices_z = lax.axis_size(GX), lax.axis_size("gy")
    devices = devices_x * devices_z
    scales, channels = scale_coeffs.shape[0], signals.shape[2]
    nodes = ROWS * COLS * 128 * devices

    def swap_z(a, b):
        b = lax.ppermute(b, "gy", neighbour_pairs(devices_z, 1))
        return lax.ppermute(a, "gy", neighbour_pairs(devices_z, 0)), b

    def swap_x(s, x):
        far = lax.ppermute(x, GX, neighbour_pairs(devices_x, 1))
        return lax.ppermute(s, "gx_2", [(0, 1), (1, 0)]), far

    def call(body, outs, in_specs, out_specs, scratch=(), aliases=None, flops=1000, mib=16):
        return pl.pallas_call(
            body,
            out_shape=outs,
            in_specs=in_specs,
            out_specs=out_specs,
            scratch_shapes=list(scratch),
            input_output_aliases=aliases or {},
            compiler_params=params(mib),
            cost_estimate=cost(flops),
        )

    tile_dir, tile_mask = jnp.swapaxes(tile_dir, 1, 2), jnp.swapaxes(tile_mask, 1, 2)
    tables = (tile_dir, tile_mask, live_rows, bound_rows)
    message_z, message_x = pltpu.VMEM((ROWS, LONG, 128), BF16), pltpu.VMEM((COLS + 2, LONG, 128), BF16)
    a, b, *tables = call(
        pack_z,
        [message_z] * 2 + [pltpu.SMEM(table.shape, jnp.int32) for table in tables],
        [HBM] * 6,
        [VMEM] * 2 + [SMEM] * 4,
        [
            pltpu.VMEM((2, ROWS, SLOTS, EDGE, 128), BF16),
            pltpu.VMEM(signals.shape, F32),
            pltpu.SemaphoreType.DMA((2,)),
            pltpu.SemaphoreType.DMA((5,)),
        ],
    )(*in_hbm(tiles, signals, *tables))
    tables = in_smem(*tables)
    s, x = call(pack_x, [message_x] * 2, [VMEM] * 2 + [SMEM] * 4, [VMEM] * 2, flops=1 << 21)(tiles, signals, *tables)
    a, b = swap_z(a, b)
    corner_room = [pltpu.VMEM((2, 2, LONG, 128), BF16), pltpu.SemaphoreType.DMA((2, 2))]
    s, x = call(
        corners_1, [message_x] * 2, [VMEM] * 2 + [ANY] * 2, [ANY] * 2, corner_room, {2: 0, 3: 1}
    )(a, b, *in_vmem(s, x))
    s, x = swap_x(s, x)

    corner_tiles, own_tiles, table, scale_table = call(
        turn_tiles,
        [
            shape((ROWS, COLS, 128, 128)),
            shape((ROWS, COLS, 256, 128)),
            pltpu.SMEM((ROWS, SLOTS + 2, COLS), jnp.int32),
            pltpu.SMEM(scale_coeffs.shape, F32),
        ],
        [VMEM] + [SMEM] * 4 + [HBM],
        [VMEM, VMEM, SMEM, SMEM],
        [pltpu.SemaphoreType.DMA],
        flops=1 << 23,
    )(tiles, *tables, *in_hbm(scale_coeffs))
    table, scale_table = in_smem(table, scale_table)
    half = shape((COLS, channels, 128), F32)
    extra = shape((COLS + 4, channels, 128), F32)
    wide_room, room = shape((ZERO + 1, 32, 128)), shape((ZERO + 1, 16, 128))
    wide_scratch, scratch = pltpu.VMEM((ZERO + 1, 32, 128), BF16), pltpu.VMEM((ZERO + 1, 16, 128), BF16)
    short_z, short_x = pltpu.VMEM((ROWS, 32, 128), BF16), pltpu.VMEM((COLS + 2, 32, 128), BF16)
    full = shape((ROWS, COLS, channels, 128), F32)
    room_1, room_2, degree_a, first_a, ghost_degree_a, ghost_first_a = call(
        step_1a, [wide_room, room, half, half, extra, extra], [VMEM] * 3 + [SMEM] * 2 + [VMEM] * 3, [VMEM] * 6, flops=1 << 25
    )(own_tiles, corner_tiles, signals, table, spectral_bound, a, b, s)
    degree_b, first_b, ghost_degree_b, ghost_first_b, second, a2, b2 = call(
        step_1b,
        [half, half, extra, extra, full, short_z, short_z],
        [VMEM] * 3 + [SMEM] * 2 + [VMEM] * 7,
        [VMEM] * 7,
        [wide_scratch, scratch],
        flops=1 << 26,
    )(own_tiles, corner_tiles, signals, table, spectral_bound, a, b, x, room_1, room_2, degree_a, first_a)
    s2, x2, products = call(
        pack_x2, [short_x] * 2 + [full], [VMEM, VMEM, SMEM], [VMEM] * 3, flops=1 << 20
    )(second, own_tiles, table)
    a2, b2 = swap_z(a2, b2)
    corner_room = [pltpu.VMEM((2, 2, 32, 128), BF16), pltpu.SemaphoreType.DMA((2, 2))]
    s2, x2 = call(
        corners_2, [short_x] * 2, [VMEM] * 2 + [ANY] * 2, [ANY] * 2, corner_room, {2: 0, 3: 1}
    )(a2, b2, *in_vmem(s2, x2))
    s2, x2 = swap_x(s2, x2)
    room_1, room_2, third_a = call(
        step_3a, [room, room, half], [VMEM, VMEM, SMEM, SMEM] + [VMEM] * 12, [VMEM] * 3, flops=1 << 25
    )(
        own_tiles, corner_tiles, table, spectral_bound, a, b, s, a2, b2, s2, degree_a, first_a, second, products,
        ghost_degree_a, ghost_first_a,
    )
    partial, third_b, fourth = call(
        step_3b,
        [pltpu.VMEM((devices, 1, 128), F32), half, full],
        [VMEM] * 3 + [SMEM] * 3 + [VMEM] * 17,
        [VMEM] * 3,
        [scratch, scratch],
        flops=1 << 26,
    )(
        own_tiles, corner_tiles, signals, table, spectral_bound, scale_table, a, b, x, a2, b2, x2, room_1, room_2,
        degree_a, degree_b, first_a, first_b, second, products, ghost_degree_b, ghost_first_b, third_a,
    )
    totals = call(
        combine,
        [shape((scales, ROWS, COLS, channels, 128), F32)],
        [VMEM, SMEM, SMEM] + [VMEM] * 6,
        [VMEM],
        flops=1 << 24,
    )(signals, table, scale_table, first_a, first_b, second, third_a, third_b, fourth)[0]
    gathered = lax.all_to_all(partial, GX_GY, 0, 0)
    energy = pl.pallas_call(
        functools.partial(finish, nodes=nodes),
        out_shape=shape((scales, channels), F32),
        in_specs=[VMEM],
        out_specs=VMEM,
        compiler_params=params(8),
        name="finish",
    )(gathered)
    return (totals, energy)


def solution(mesh):
    torus = Mesh(mesh.devices.reshape(4, 4, 2, mesh.shape["gy"]), ("gx_0", "gx_1", "gx_2", "gy"))
    placed = (
        P(GX, "gy", None, None),
        P(GX, "gy", None, None, None),
        P(GX, "gy", None),
        P(GX, "gy", None),
        P(GX, "gy"),
        P(GX, "gy"),
        P(),
        P(),
    )
    return jax.shard_map(
        shards,
        mesh=torus,
        in_specs=placed,
        out_specs=(P(None, GX, "gy", None, None), P()),
        check_vma=False,
    )
```

```python
import functools

import jax
import jax.numpy as jnp
from jax import lax
from jax.experimental import pallas as pl
from jax.experimental.pallas import tpu as pltpu
from jax.sharding import Mesh
from jax.sharding import PartitionSpec as P

GX_GY = ("gx_0", "gx_1", "gx_2", "gy")
GX = ("gx_0", "gx_1", "gx_2")
F32 = jnp.float32
BF16 = jnp.bfloat16
EDGE = 32
ROWS, COLS = 2, 8
WIDE = COLS + 4
SPOTS = (ROWS + 4) * WIDE
ZERO = SPOTS
SLOTS = 4
NEAR, FAR, LONG = 32, 48, 64
HIGH, LOW, OWN_HIGH, OWN_LOW = 0, 1, 2, 3
INFO = 3
BOUND, BOUND2, BOUND3, BOUND4, DEGREE, DIRS = 0, 1, 2, 3, 4, 6
VMEM = pl.BlockSpec(memory_space=pltpu.VMEM)
SMEM = pl.BlockSpec(memory_space=pltpu.SMEM)
ANY = pl.BlockSpec(memory_space=pl.ANY)
HBM = pl.BlockSpec(memory_space=pltpu.MemorySpace.HBM)


def params(mib):
    return pltpu.CompilerParams(vmem_limit_bytes=mib * 1024 * 1024)


def cost(flops):
    return pl.CostEstimate(flops=flops, bytes_accessed=1 << 20, transcendentals=0)


def lanes():
    return lax.broadcasted_iota(jnp.int32, (16, 128), 1)


def below(count):
    return (lanes() < count).astype(F32)


def split(value):
    high = value.astype(BF16)
    return high, value - high.astype(F32)


def info_of(rows):
    index = lax.broadcasted_iota(jnp.int32, (16, 128), 0)
    info = jnp.zeros((16, 128), F32)
    for row, value in rows.items():
        info = jnp.where(index == row, value, info)
    return info


def odd_z():
    return lax.axis_index("gy") % 2


def odd_core():
    return lax.axis_index("gx_2")


def merge(parts):
    lane = lax.broadcasted_iota(jnp.int32, parts[0].shape, 1)
    merged = parts[0]
    for index, part in enumerate(parts[1:], 1):
        merged = jnp.where(lane < EDGE * index, merged, pltpu.roll(part, EDGE * index, 1))
    return merged if len(parts) == 4 else jnp.where(lane < EDGE * len(parts), merged, 0.0)


def piece(pack, index):
    moved = pltpu.roll(pack, 128 - EDGE * index, 1) if index else pack
    return jnp.where(lanes() < EDGE, moved, 0.0)


def repeat(value):
    value = value + pltpu.roll(value, EDGE, 1)
    return value + pltpu.roll(value, 2 * EDGE, 1)


def wide(value):
    return jnp.concatenate([value, jnp.zeros((value.shape[0], 128 - value.shape[1]), value.dtype)], axis=1)


def with_head(value, line):
    return jnp.concatenate([value.astype(BF16), jnp.where(heads(), line, 0.0).astype(BF16)], axis=0)


def heads():
    return lax.broadcasted_iota(jnp.int32, (16, 128), 0) == 0


def block_message(out, at, refs, raw, row, col, row2, col2):
    signals, dirs, masks, live, bound = refs
    alive, inside = below(live[row, col]), below(bound[row, col])
    value = signals[row, col] * alive
    full = with_head(value, alive).astype(F32)
    inputs, sides = [], []
    for slot in range(SLOTS):
        side, used = dirs[row, slot, col], masks[row, slot, col] == 1
        own = jnp.where(side == 4, jnp.where(used, 1.0, 0.0), 0.0)
        inputs.append((full * own).astype(BF16))
        sides.append(jnp.full((16, 128), jnp.where(used, side, 9).astype(F32)))
    product = lax.dot_general(
        jnp.concatenate(inputs, axis=1),
        jnp.concatenate([raw[slot] for slot in range(SLOTS)], axis=1),
        (((1,), (1,)), ((), ())),
        preferred_element_type=F32,
    )
    product = wide(product)
    value = value * inside
    high, low = split(value)
    own_high, own_low = split(product[0:16])
    own_high = own_high.astype(F32)
    degree_high, degree_low = split(product[16:17])
    out[at, 0:NEAR] = merge([raw[slot].astype(F32) for slot in range(SLOTS)]).astype(BF16)
    out[at, NEAR:FAR] = merge([high.astype(F32), low, own_high, own_low]).astype(BF16)
    inside2 = below(bound[row2, col2])
    rows = {BOUND: inside, BOUND2: inside2, DEGREE: degree_high.astype(F32), DEGREE + 1: degree_low}
    rows.update({DIRS + slot: side for slot, side in enumerate(sides)})
    second = signals[row2, col2] * inside2
    out[at, FAR:LONG] = merge([second, jnp.zeros_like(second), jnp.zeros_like(second), info_of(rows)]).astype(BF16)


def fetch(refs, rooms, sems):
    copies = [pltpu.make_async_copy(ref, room, sems.at[i]) for i, (ref, room) in enumerate(zip(refs, rooms))]
    for copy in copies:
        copy.start()
    return copies


def pack_z(
    tiles, signals, dirs, masks, live, bound, out_a, out_b, dirs_s, masks_s, live_s, bound_s, raw, signals_v, sem, sem2
):
    refs = (signals_v, dirs_s, masks_s, live_s, bound_s)
    copies = fetch((signals, dirs, masks, live, bound), refs, sem2)
    odd = odd_z()
    for which in range(2):
        col = jnp.where(odd == which, COLS - 1, 0)
        copies.append(pltpu.make_async_copy(tiles.at[:, col, :, 0:EDGE, :], raw.at[which], sem.at[which]))
        copies[-1].start()
    for copy in copies:
        copy.wait()
    for which, out in enumerate((out_a, out_b)):
        right = odd == which
        col, col2 = jnp.where(right, COLS - 1, 0), jnp.where(right, COLS - 2, 1)
        for row in range(ROWS):
            block_message(out, row, refs, [raw[which, row, slot] for slot in range(SLOTS)], row, col, row, col2)


def pack_x(tiles, signals, dirs, masks, live, bound, out_s, out_b):
    refs = (signals, dirs, masks, live, bound)
    core = odd_core()
    for which, out in enumerate((out_s, out_b)):
        row = jnp.where(core == which, 1, 0)
        for col in range(COLS):
            raw = [tiles[row, col, slot, 0:EDGE] for slot in range(SLOTS)]
            block_message(out, 1 + col, refs, raw, row, col, 1 - row, col)


def place_corners(from_a, from_b, out_s, out_b, room, sem, near, far, with_info):
    odd, core = odd_z(), odd_core()
    copies = []
    for side, halo in enumerate((from_a, from_b)):
        at = jnp.where(odd == side, COLS + 1, 0)
        for which, out in enumerate((out_s, out_b)):
            row = jnp.where(core == which, 1, 0)
            first, other = halo[row, far : far + 16].astype(F32), halo[1 - row, far : far + 16].astype(F32)
            parts = [halo[1 - row, near : near + 16].astype(F32), first, other]
            if with_info:
                info, info2 = piece(first, INFO), piece(other, INFO)
                index = lax.broadcasted_iota(jnp.int32, (16, 128), 0)
                for line, source in ((BOUND4, info2[BOUND2 : BOUND2 + 1]), (BOUND3, info[BOUND2 : BOUND2 + 1])):
                    info = jnp.where(index == line, source, info)
                parts.append(jnp.where(index == BOUND2, info2[BOUND : BOUND + 1], info))
            room[which, side, 0:far] = halo[row, 0:far]
            room[which, side, far : far + 16] = merge(parts).astype(BF16)
            copies.append(pltpu.make_async_copy(room.at[which, side], out.at[at], sem.at[which, side]))
    for copy in copies:
        copy.start()
    for copy in copies:
        copy.wait()


def corners_1(from_a, from_b, in_s, in_b, out_s, out_b, room, sem):
    del in_s, in_b
    place_corners(from_a, from_b, out_s, out_b, room, sem, NEAR, FAR, True)


def corners_2(from_a, from_b, in_s, in_b, out_s, out_b, room, sem):
    del in_s, in_b
    place_corners(from_a, from_b, out_s, out_b, room, sem, 0, 16, False)


def place(u, v):
    return u * WIDE + v + 2


class Frame:
    def __init__(self):
        self.odd, self.core = odd_z(), odd_core()
        self.up = 2 * self.core - 1
        self.right = 1 - 2 * self.odd

    def row(self, u):
        return 1 - self.core if u == 2 else self.core

    def col(self, v):
        return jnp.where(self.odd == 1, COLS - 1 - v, v)


def ghost_blocks(frame, u, halo_a, halo_b, halo_x):
    row = frame.row(u)
    found = [(halo_a, row, u, COLS), (halo_b, row, u, -1)]
    return found + [(halo_x, frame.col(v) + 1, 1 if u == 2 else 4, v) for v in range(-1, COLS + 1)]


def info_part(halo, at):
    return piece(halo[at, FAR:LONG].astype(F32), INFO)


def ghost_product(frame, halo, at, info, spot_at, room, height):
    side = merge([info[DIRS + slot : DIRS + slot + 1] for slot in range(SLOTS)])
    step = jnp.where(side > 5.5, 1.0, jnp.where(side > 2.5, 0.0, -1.0))
    turned = 3.0 * (frame.up.astype(F32) * step) + frame.right.astype(F32) * (side - 3.0 * step - 4.0) + 4.0
    turned = jnp.where(side > 8.5, 9.0, turned)
    turn = jnp.broadcast_to(turned, (16, 128)).astype(BF16)
    halves = [jnp.zeros((16, 128), BF16) for _ in range(height // 16)]
    for d in (0, 1, 2, 3, 5, 6, 7, 8):
        near = room[spot_at + (d // 3 - 1) * WIDE + d % 3 - 1]
        chosen = turn == d
        halves = [jnp.where(chosen, near[16 * h : 16 * h + 16], half) for h, half in enumerate(halves)]
    inputs = halves[0] if height == 16 else jnp.concatenate(halves, axis=0)
    product = lax.dot_general(inputs, halo[at, 0:NEAR], (((1,), (1,)), ((), ())), preferred_element_type=F32)
    return wide(product)


def slot_lanes():
    return (lanes() // EDGE).astype(F32).astype(BF16)


def near_input(table, row, col, room, height):
    group = slot_lanes()
    blocks = [room[table[row, slot, col]] for slot in range(SLOTS)]
    halves = []
    for half in range(0, height, 16):
        chosen = blocks[0][half : half + 16]
        for slot in range(1, SLOTS):
            chosen = jnp.where(group == slot, blocks[slot][half : half + 16], chosen)
        halves.append(chosen)
    return halves[0] if height == 16 else jnp.concatenate(halves, axis=0)


def own_product(weights, table, row, col, room, own):
    near = near_input(table, row, col, room, own.shape[0])
    product = jnp.dot(jnp.concatenate([own, own], axis=1), weights[0][row, col], preferred_element_type=F32)
    return product + jnp.dot(near, weights[1][row, col], preferred_element_type=F32)


def alive_of(table, row, col):
    return below(table[row, SLOTS, col])


def inside_of(table, row, col):
    return below(table[row, SLOTS + 1, col])


def place_edge(room, at, value):
    room[at, 0:16] = repeat(value).astype(BF16)


def message_2(out, at, second, weights, table, u, v, u2, v2, frame):
    row, col = frame.row(u), frame.col(v)
    value = second[u - 2, v]
    own = value.astype(BF16)
    product = jnp.dot(jnp.concatenate([own, own], axis=1), weights[0][row, col], preferred_element_type=F32)
    high, low = split(value * inside_of(table, row, col))
    own_high, own_low = split(product)
    out[at, 0:16] = merge([high.astype(F32), low, own_high.astype(F32), own_low]).astype(BF16)
    out[at, 16:32] = (second[u2 - 2, v2] * inside_of(table, frame.row(u2), frame.col(v2))).astype(BF16)
    return product


def turn_tiles(tiles, dirs_s, masks_s, live_s, bound_s, scales, corner_out, own_out, table, scales_out, sem):
    copy = pltpu.make_async_copy(scales, scales_out, sem)
    copy.start()
    rows = lax.broadcasted_iota(jnp.int32, (128, 512), 0)
    cols = lax.broadcasted_iota(jnp.int32, (128, 512), 1)
    picked = jnp.where((rows // EDGE == cols // 128) & (rows % EDGE == cols % 128), 1.0, 0.0).astype(BF16)
    same = jnp.where(rows[:, 0:128] == cols[:, 0:128], 1.0, 0.0)
    for row in range(ROWS):
        for col in range(COLS):
            joined = jnp.concatenate([tiles[row, col, slot] for slot in range(SLOTS)], axis=1)
            owned = []
            for slot in range(SLOTS):
                own = jnp.where(dirs_s[row, slot, col] == 4, jnp.where(masks_s[row, slot, col] == 1, 1.0, 0.0), 0.0)
                owned.append((same * own).astype(BF16))
            total = lax.dot_general(
                jnp.concatenate(owned, axis=1), joined, (((1,), (1,)), ((), ())), preferred_element_type=F32
            )
            high, low = split(total)
            own_out[row, col, 0:128] = high
            own_out[row, col, 128:256] = low.astype(BF16)
            if row == 0:
                product = lax.dot_general(picked, joined, (((1,), (1,)), ((), ())), preferred_element_type=F32)
                corner_out[row, col] = product.astype(BF16)
            else:
                for slot in range(SLOTS):
                    corner_out[row, col, EDGE * slot : EDGE * (slot + 1)] = jnp.transpose(tiles[row, col, slot])[0:EDGE]
    core, odd = odd_core(), odd_z()
    down, right = (2 * core - 1) * WIDE, 1 - 2 * odd
    for row in range(ROWS):
        for col in range(COLS):
            base = place(jnp.where(core == row, 3, 2), jnp.where(odd == 1, COLS - 1 - col, col))
            for slot in range(SLOTS):
                side = dirs_s[row, slot, col]
                step = jnp.where(side > 5, 1, jnp.where(side > 2, 0, -1))
                index = base + step * down + (side - 3 * step - 4) * right
                index = jnp.where(side == 4, ZERO, index)
                table[row, slot, col] = jnp.where(masks_s[row, slot, col] == 1, index, ZERO)
            table[row, SLOTS, col] = live_s[row, col]
            table[row, SLOTS + 1, col] = bound_s[row, col]
    copy.wait()


def fill(room, halo, near, far, with_info, at, near_at, far_at, corner):
    place_edge(room, near_at, piece(halo[at, near : near + 16].astype(F32), HIGH))
    beyond = halo[at, far : far + 16].astype(F32)
    places = (far_at,) + corner
    for index, spot_at in enumerate(places):
        place_edge(room, spot_at, piece(beyond, index))
    if with_info:
        lines = repeat(piece(beyond, INFO))
        for spot_at, line in zip((near_at,) + places, (BOUND, BOUND2, BOUND3, BOUND4)):
            room[spot_at, 16:32] = jnp.where(heads(), lines[line : line + 1], 0.0).astype(BF16)


FIRST, SECOND = (NEAR, FAR, True), (0, 16, False)


def fill_z(frame, room, rows, halo_a, halo_b):
    for halo, near, far in ((halo_a, COLS, COLS + 1), (halo_b, -1, -2)):
        for u in (2, 3):
            fill(room, halo, *rows, frame.row(u), place(u, near), place(u, far), ())


def fill_x(frame, room, rows, halo, near, far):
    for v in range(-1, COLS + 1):
        beyond = {-1: -2, COLS: COLS + 1}.get(v)
        corner = () if beyond is None else (place(near, beyond), place(far, beyond))
        fill(room, halo, *rows, frame.col(v) + 1, place(near, v), place(far, v), corner)


def half_1(frame, u, weights, signals, table, factor, halos, room, room2, degree, first, ghost_degree, ghost_first):
    for number, (halo, at, gu, gv) in enumerate(ghost_blocks(frame, u, *halos)):
        pack, info = halo[at, NEAR:FAR].astype(F32), info_part(halo, at)
        value = piece(pack, HIGH) + piece(pack, LOW)
        near = ghost_product(frame, halo, at, info, place(gu, gv), room, 32)
        sums = near[0:16] + (piece(pack, OWN_HIGH) + piece(pack, OWN_LOW))
        around = near[16:17] + (info[DEGREE : DEGREE + 1] + info[DEGREE + 1 : DEGREE + 2])
        around = jnp.broadcast_to(around, (16, 128))
        result = factor * (around * value - sums) - value
        ghost_degree[number] = around
        ghost_first[number] = result
        place_edge(room2, place(gu, gv), jnp.where(lanes() < EDGE, result * info[BOUND : BOUND + 1], 0.0))
    row = frame.row(u)
    for v in range(COLS):
        col = frame.col(v)
        alive = alive_of(table, row, col)
        value = signals[row, col] * alive
        sums = own_product(weights, table, row, col, room, with_head(value, alive))
        around = jnp.broadcast_to(sums[16:17], (16, 128)) * alive
        result = factor * (around * value - sums[0:16] * alive) - value
        degree[v] = around
        first[v] = result
        place_edge(room2, place(u, v), result * inside_of(table, row, col))


def half_3(frame, u, weights, table, factor, halos, fresh, room, room2, degree, first, second, products, third, ghost_degree, ghost_first):
    values = ghost_blocks(frame, u, *fresh)
    for number, (halo, at, gu, gv) in enumerate(ghost_blocks(frame, u, *halos)):
        pack, info = values[number][0][at, 0:16].astype(F32), info_part(halo, at)
        value = piece(pack, HIGH) + piece(pack, LOW)
        sums = ghost_product(frame, halo, at, info, place(gu, gv), room, 16) + (piece(pack, OWN_HIGH) + piece(pack, OWN_LOW))
        result = 2.0 * (factor * (ghost_degree[number] * value - sums) - value) - ghost_first[number]
        place_edge(room2, place(gu, gv), jnp.where(lanes() < EDGE, result * info[BOUND : BOUND + 1], 0.0))
    row = frame.row(u)
    for v in range(COLS):
        col = frame.col(v)
        near = near_input(table, row, col, room, 16)
        sums = products[u - 2, v] + jnp.dot(near, weights[1][row, col], preferred_element_type=F32)
        value = second[u - 2, v]
        result = 2.0 * (factor * (degree[v] * value - sums * alive_of(table, row, col)) - value) - first[v]
        third[v] = result
        place_edge(room2, place(u, v), result * inside_of(table, row, col))


def carry_rooms(room, room_in, room2, room2_in):
    for v in range(-2, COLS + 2):
        for u in (2, 3):
            room[place(u, v)] = room_in[place(u, v)]
    for v in range(-1, COLS + 1):
        for u in (1, 2):
            room2[place(u, v)] = room2_in[place(u, v)]


def step_1a(
    own_tiles, corner_tiles, signals, table, spectral, from_a, from_b, from_s, room, room2, degree, first, ghost_degree, ghost_first
):
    frame, weights = Frame(), (own_tiles, corner_tiles)
    factor = 2.0 / jnp.full((16, 128), spectral[0])
    room[ZERO] = jnp.zeros((32, 128), BF16)
    for u in (2, 3):
        row = frame.row(u)
        for v in range(COLS):
            col, at = frame.col(v), place(u, v)
            inside = inside_of(table, row, col)
            place_edge(room, at, signals[row, col] * inside)
            room[at, 16:32] = jnp.where(heads(), repeat(inside), 0.0).astype(BF16)
    fill_z(frame, room, FIRST, from_a, from_b)
    fill_x(frame, room, FIRST, from_s, 1, 0)
    halos = (from_a, from_b, from_s)
    half_1(frame, 2, weights, signals, table, factor, halos, room, room2, degree, first, ghost_degree, ghost_first)


def step_1b(
    own_tiles, corner_tiles, signals, table, spectral, from_a, from_b, from_x, room_in, room2_in, degree_a, first_a,
    degree, first, ghost_degree, ghost_first, second, out_a, out_b, room2, room,
):
    frame, weights = Frame(), (own_tiles, corner_tiles)
    factor = 2.0 / jnp.full((16, 128), spectral[0])
    room[ZERO] = jnp.zeros((32, 128), BF16)
    room2[ZERO] = jnp.zeros((16, 128), BF16)
    carry_rooms(room, room_in, room2, room2_in)
    fill_x(frame, room, FIRST, from_x, 4, 5)
    halos = (from_a, from_b, from_x)
    half_1(frame, 3, weights, signals, table, factor, halos, room, room2, degree, first, ghost_degree, ghost_first)
    rows = ((2, degree_a, first_a), (3, degree, first))
    second_step(frame, (0, 1, COLS - 2, COLS - 1), weights, signals, table, factor, room2, rows, second)
    for out, v, v2 in ((out_a, COLS - 1, COLS - 2), (out_b, 0, 1)):
        for u in (2, 3):
            message_2(out, frame.row(u), second, weights, table, u, v, u, v2, frame)


def second_step(frame, cols, weights, signals, table, factor, room2, rows, second):
    for u, degrees, firsts in rows:
        row = frame.row(u)
        for v in cols:
            col = frame.col(v)
            value = firsts[v]
            sums = own_product(weights, table, row, col, room2, value.astype(BF16))
            alive = alive_of(table, row, col)
            result = 2.0 * (factor * (degrees[v] * value - sums * alive) - value)
            second[u - 2, v] = result - signals[row, col] * alive


def pack_x2(
    edges, own_tiles, corner_tiles, signals, table, spectral, room2, degree_a, degree, first_a, first,
    out_s, out_x, products, second,
):
    frame, weights = Frame(), (own_tiles, corner_tiles)
    factor = 2.0 / jnp.full((16, 128), spectral[0])
    for u in (2, 3):
        for v in (0, 1, COLS - 2, COLS - 1):
            second[u - 2, v] = edges[u - 2, v]
    rows = ((2, degree_a, first_a), (3, degree, first))
    second_step(frame, range(2, COLS - 2), weights, signals, table, factor, room2, rows, second)
    for out, u in ((out_s, 2), (out_x, 3)):
        for v in range(COLS):
            products[u - 2, v] = message_2(out, frame.col(v) + 1, second, weights, table, u, v, 5 - u, v, frame)


def step_3a(
    own_tiles, corner_tiles, table, spectral, from_a, from_b, from_s, new_a, new_b, new_s,
    degree, first, second, products, ghost_degree, ghost_first, room, room2, third,
):
    frame, weights = Frame(), (own_tiles, corner_tiles)
    factor = 2.0 / jnp.full((16, 128), spectral[0])
    room[ZERO] = jnp.zeros((16, 128), BF16)
    for u in (2, 3):
        for v in range(COLS):
            place_edge(room, place(u, v), second[u - 2, v] * inside_of(table, frame.row(u), frame.col(v)))
    fill_z(frame, room, SECOND, new_a, new_b)
    fill_x(frame, room, SECOND, new_s, 1, 0)
    half_3(
        frame, 2, weights, table, factor, (from_a, from_b, from_s), (new_a, new_b, new_s), room, room2,
        degree, first, second, products, third, ghost_degree, ghost_first,
    )


def step_3b(
    own_tiles, corner_tiles, signals, table, spectral, scales, from_a, from_b, from_x, new_a, new_b, new_x, room_in, room2_in,
    degree_a, degree, first_a, first, second, products, ghost_degree, ghost_first, third_a,
    partial, third, fourths, room, room2,
):
    frame, weights = Frame(), (own_tiles, corner_tiles)
    factor = 2.0 / jnp.full((16, 128), spectral[0])
    room[ZERO] = jnp.zeros((16, 128), BF16)
    room2[ZERO] = jnp.zeros((16, 128), BF16)
    carry_rooms(room, room_in, room2, room2_in)
    fill_x(frame, room, SECOND, new_x, 4, 5)
    half_3(
        frame, 3, weights, table, factor, (from_a, from_b, from_x), (new_a, new_b, new_x), room, room2,
        degree, first, second, products, third, ghost_degree, ghost_first,
    )
    count = scales.shape[0]
    squares = [jnp.zeros((16, 128), F32) for _ in range(count)]
    for u, degrees, firsts, thirds in ((2, degree_a, first_a, third_a), (3, degree, first, third)):
        row = frame.row(u)
        for v in range(COLS):
            col = frame.col(v)
            value = thirds[v]
            sums = own_product(weights, table, row, col, room2, value.astype(BF16))
            alive = alive_of(table, row, col)
            fourth = 2.0 * (factor * (degrees[v] * value - sums * alive) - value) - second[u - 2, v]
            fourths[u - 2, v] = fourth
            terms = (signals[row, col] * alive, firsts[v], second[u - 2, v], value, fourth)
            for scale, total in enumerate(weighted(scales, terms)):
                squares[scale] = squares[scale] + total * total
    block = jnp.concatenate(squares + [jnp.zeros((128 - 16 * count, 128), F32)], axis=0)
    line = jnp.sum(jnp.transpose(block), axis=0, keepdims=True)
    partial[...] = jnp.broadcast_to(line[None], partial.shape)


def weighted(scales, terms):
    for scale in range(scales.shape[0]):
        total = (0.5 * scales[scale, 0]) * terms[0]
        for order in range(1, len(terms)):
            total = total + scales[scale, order] * terms[order]
        yield total


def combine(signals, table, scales, first_a, first_b, second, third_a, third_b, fourths, coefficients):
    frame = Frame()
    for u, firsts, thirds in ((2, first_a, third_a), (3, first_b, third_b)):
        row = frame.row(u)
        for v in range(COLS):
            col = frame.col(v)
            terms = (signals[row, col] * alive_of(table, row, col), firsts[v], second[u - 2, v], thirds[v], fourths[u - 2, v])
            for scale, total in enumerate(weighted(scales, terms)):
                coefficients[scale, row, col] = total


def finish(gathered, out, *, nodes):
    total = jnp.sum(gathered[...], axis=0) * (1.0 / nodes)
    scales, channels = out.shape
    for scale in range(scales):
        out[scale : scale + 1] = pltpu.roll(total, 128 - channels * scale, 1)[:, 0:channels] if scale else total[:, 0:channels]


def in_hbm(*arrays):
    return tuple(pltpu.with_memory_space_constraint(array, pltpu.MemorySpace.HBM) for array in arrays)


def in_vmem(*arrays):
    return tuple(pltpu.with_memory_space_constraint(array, pltpu.MemorySpace.VMEM) for array in arrays)


def in_smem(*arrays):
    return tuple(pltpu.with_memory_space_constraint(array, pltpu.MemorySpace.SMEM) for array in arrays)


def neighbour_pairs(devices, first):
    pairs = [(i, i + 1) for i in range(first, devices - 1, 2)]
    return pairs + [(j, i) for i, j in pairs]


def shape(dims, kind=BF16):
    return jax.ShapeDtypeStruct(dims, kind)


def shards(signals, tiles, tile_dir, tile_mask, live_rows, bound_rows, scale_coeffs, spectral_bound):
    devices_x, devices_z = lax.axis_size(GX), lax.axis_size("gy")
    devices = devices_x * devices_z
    scales, channels = scale_coeffs.shape[0], signals.shape[2]
    nodes = ROWS * COLS * 128 * devices

    def swap_z(a, b):
        b = lax.ppermute(b, "gy", neighbour_pairs(devices_z, 1))
        return lax.ppermute(a, "gy", neighbour_pairs(devices_z, 0)), b

    def swap_x(s, x):
        far = lax.ppermute(x, GX, neighbour_pairs(devices_x, 1))
        return lax.ppermute(s, "gx_2", [(0, 1), (1, 0)]), far

    def call(body, outs, in_specs, out_specs, scratch=(), aliases=None, flops=1000, mib=16):
        return pl.pallas_call(
            body,
            out_shape=outs,
            in_specs=in_specs,
            out_specs=out_specs,
            scratch_shapes=list(scratch),
            input_output_aliases=aliases or {},
            compiler_params=params(mib),
            cost_estimate=cost(flops),
        )

    tile_dir, tile_mask = jnp.swapaxes(tile_dir, 1, 2), jnp.swapaxes(tile_mask, 1, 2)
    tables = (tile_dir, tile_mask, live_rows, bound_rows)
    message_z, message_x = pltpu.VMEM((ROWS, LONG, 128), BF16), pltpu.VMEM((COLS + 2, LONG, 128), BF16)
    a, b, *tables = call(
        pack_z,
        [message_z] * 2 + [pltpu.SMEM(table.shape, jnp.int32) for table in tables],
        [HBM] * 6,
        [VMEM] * 2 + [SMEM] * 4,
        [
            pltpu.VMEM((2, ROWS, SLOTS, EDGE, 128), BF16),
            pltpu.VMEM(signals.shape, F32),
            pltpu.SemaphoreType.DMA((2,)),
            pltpu.SemaphoreType.DMA((5,)),
        ],
    )(*in_hbm(tiles, signals, *tables))
    tables = in_smem(*tables)
    s, x = call(pack_x, [message_x] * 2, [VMEM] * 2 + [SMEM] * 4, [VMEM] * 2, flops=1 << 21)(tiles, signals, *tables)
    a, b = swap_z(a, b)
    corner_room = [pltpu.VMEM((2, 2, LONG, 128), BF16), pltpu.SemaphoreType.DMA((2, 2))]
    s, x = call(
        corners_1, [message_x] * 2, [VMEM] * 2 + [ANY] * 2, [ANY] * 2, corner_room, {2: 0, 3: 1}
    )(a, b, *in_vmem(s, x))
    s, x = swap_x(s, x)

    corner_tiles, own_tiles, table, scale_table = call(
        turn_tiles,
        [
            shape((ROWS, COLS, 128, 128)),
            shape((ROWS, COLS, 256, 128)),
            pltpu.SMEM((ROWS, SLOTS + 2, COLS), jnp.int32),
            pltpu.SMEM(scale_coeffs.shape, F32),
        ],
        [VMEM] + [SMEM] * 4 + [HBM],
        [VMEM, VMEM, SMEM, SMEM],
        [pltpu.SemaphoreType.DMA],
        flops=1 << 23,
    )(tiles, *tables, *in_hbm(scale_coeffs))
    table, scale_table = in_smem(table, scale_table)
    half = shape((COLS, channels, 128), F32)
    extra = shape((COLS + 4, channels, 128), F32)
    wide_room, room = shape((ZERO + 1, 32, 128)), shape((ZERO + 1, 16, 128))
    wide_scratch, scratch = pltpu.VMEM((ZERO + 1, 32, 128), BF16), pltpu.VMEM((ZERO + 1, 16, 128), BF16)
    short_z, short_x = pltpu.VMEM((ROWS, 32, 128), BF16), pltpu.VMEM((COLS + 2, 32, 128), BF16)
    full = shape((ROWS, COLS, channels, 128), F32)
    room_1, room_2, degree_a, first_a, ghost_degree_a, ghost_first_a = call(
        step_1a, [wide_room, room, half, half, extra, extra], [VMEM] * 3 + [SMEM] * 2 + [VMEM] * 3, [VMEM] * 6, flops=1 << 25
    )(own_tiles, corner_tiles, signals, table, spectral_bound, a, b, s)
    degree_b, first_b, ghost_degree_b, ghost_first_b, edges, a2, b2, room_3 = call(
        step_1b,
        [half, half, extra, extra, full, short_z, short_z, room],
        [VMEM] * 3 + [SMEM] * 2 + [VMEM] * 7,
        [VMEM] * 8,
        [wide_scratch],
        flops=1 << 26,
    )(own_tiles, corner_tiles, signals, table, spectral_bound, a, b, x, room_1, room_2, degree_a, first_a)
    s2, x2, products, second = call(
        pack_x2, [short_x] * 2 + [full] * 2, [VMEM] * 4 + [SMEM] * 2 + [VMEM] * 5, [VMEM] * 4, flops=1 << 20
    )(edges, own_tiles, corner_tiles, signals, table, spectral_bound, room_3, degree_a, degree_b, first_a, first_b)
    a2, b2 = swap_z(a2, b2)
    corner_room = [pltpu.VMEM((2, 2, 32, 128), BF16), pltpu.SemaphoreType.DMA((2, 2))]
    s2, x2 = call(
        corners_2, [short_x] * 2, [VMEM] * 2 + [ANY] * 2, [ANY] * 2, corner_room, {2: 0, 3: 1}
    )(a2, b2, *in_vmem(s2, x2))
    s2, x2 = swap_x(s2, x2)
    room_1, room_2, third_a = call(
        step_3a, [room, room, half], [VMEM, VMEM, SMEM, SMEM] + [VMEM] * 12, [VMEM] * 3, flops=1 << 25
    )(
        own_tiles, corner_tiles, table, spectral_bound, a, b, s, a2, b2, s2, degree_a, first_a, second, products,
        ghost_degree_a, ghost_first_a,
    )
    partial, third_b, fourth = call(
        step_3b,
        [pltpu.VMEM((devices, 1, 128), F32), half, full],
        [VMEM] * 3 + [SMEM] * 3 + [VMEM] * 17,
        [VMEM] * 3,
        [scratch, scratch],
        flops=1 << 26,
    )(
        own_tiles, corner_tiles, signals, table, spectral_bound, scale_table, a, b, x, a2, b2, x2, room_1, room_2,
        degree_a, degree_b, first_a, first_b, second, products, ghost_degree_b, ghost_first_b, third_a,
    )
    totals = call(
        combine,
        [shape((scales, ROWS, COLS, channels, 128), F32)],
        [VMEM, SMEM, SMEM] + [VMEM] * 6,
        [VMEM],
        flops=1 << 24,
    )(signals, table, scale_table, first_a, first_b, second, third_a, third_b, fourth)[0]
    gathered = lax.all_to_all(partial, GX_GY, 0, 0)
    energy = pl.pallas_call(
        functools.partial(finish, nodes=nodes),
        out_shape=shape((scales, channels), F32),
        in_specs=[VMEM],
        out_specs=VMEM,
        compiler_params=params(8),
        name="finish",
    )(gathered)
    return (totals, energy)


def solution(mesh):
    torus = Mesh(mesh.devices.reshape(4, 4, 2, mesh.shape["gy"]), ("gx_0", "gx_1", "gx_2", "gy"))
    placed = (
        P(GX, "gy", None, None),
        P(GX, "gy", None, None, None),
        P(GX, "gy", None),
        P(GX, "gy", None),
        P(GX, "gy"),
        P(GX, "gy"),
        P(),
        P(),
    )
    return jax.shard_map(
        shards,
        mesh=torus,
        in_specs=placed,
        out_specs=(P(None, GX, "gy", None, None), P()),
        check_vma=False,
    )
```

```python
import functools

import jax
import jax.numpy as jnp
from jax import lax
from jax.experimental import pallas as pl
from jax.experimental.pallas import tpu as pltpu
from jax.sharding import Mesh
from jax.sharding import PartitionSpec as P

GX_GY = ("gx_0", "gx_1", "gx_2", "gy")
GX = ("gx_0", "gx_1", "gx_2")
F32 = jnp.float32
BF16 = jnp.bfloat16
EDGE = 32
ROWS, COLS = 2, 8
WIDE = COLS + 4
SPOTS = (ROWS + 4) * WIDE
ZERO = SPOTS
SLOTS = 4
NEAR, FAR, LONG = 32, 48, 64
HIGH, LOW, OWN_HIGH, OWN_LOW = 0, 1, 2, 3
INFO = 3
BOUND, BOUND2, BOUND3, BOUND4, DEGREE, DIRS = 0, 1, 2, 3, 4, 6
VMEM = pl.BlockSpec(memory_space=pltpu.VMEM)
SMEM = pl.BlockSpec(memory_space=pltpu.SMEM)
ANY = pl.BlockSpec(memory_space=pl.ANY)
HBM = pl.BlockSpec(memory_space=pltpu.MemorySpace.HBM)


def params(mib):
    return pltpu.CompilerParams(vmem_limit_bytes=mib * 1024 * 1024)


def cost(flops):
    return pl.CostEstimate(flops=flops, bytes_accessed=1 << 20, transcendentals=0)


def lanes():
    return lax.broadcasted_iota(jnp.int32, (16, 128), 1)


def below(count):
    return (lanes() < count).astype(F32)


def split(value):
    high = value.astype(BF16)
    return high, value - high.astype(F32)


def info_of(rows):
    index = lax.broadcasted_iota(jnp.int32, (16, 128), 0)
    info = jnp.zeros((16, 128), F32)
    for row, value in rows.items():
        info = jnp.where(index == row, value, info)
    return info


def odd_z():
    return lax.axis_index("gy") % 2


def odd_core():
    return lax.axis_index("gx_2")


def merge(parts):
    lane = lax.broadcasted_iota(jnp.int32, parts[0].shape, 1)
    merged = parts[0]
    for index, part in enumerate(parts[1:], 1):
        merged = jnp.where(lane < EDGE * index, merged, pltpu.roll(part, EDGE * index, 1))
    return merged if len(parts) == 4 else jnp.where(lane < EDGE * len(parts), merged, 0.0)


def piece(pack, index):
    moved = pltpu.roll(pack, 128 - EDGE * index, 1) if index else pack
    return jnp.where(lanes() < EDGE, moved, 0.0)


def repeat(value):
    value = value + pltpu.roll(value, EDGE, 1)
    return value + pltpu.roll(value, 2 * EDGE, 1)


def wide(value):
    return jnp.concatenate([value, jnp.zeros((value.shape[0], 128 - value.shape[1]), value.dtype)], axis=1)


def with_head(value, line):
    return jnp.concatenate([value.astype(BF16), jnp.where(heads(), line, 0.0).astype(BF16)], axis=0)


def heads():
    return lax.broadcasted_iota(jnp.int32, (16, 128), 0) == 0


def block_message(out, at, refs, raw, row, col, row2, col2):
    signals, dirs, masks, live, bound = refs
    alive, inside = below(live[row, col]), below(bound[row, col])
    value = signals[row, col] * alive
    full = with_head(value, alive).astype(F32)
    inputs, sides = [], []
    for slot in range(SLOTS):
        side, used = dirs[row, slot, col], masks[row, slot, col] == 1
        own = jnp.where(side == 4, jnp.where(used, 1.0, 0.0), 0.0)
        inputs.append((full * own).astype(BF16))
        sides.append(jnp.full((16, 128), jnp.where(used, side, 9).astype(F32)))
    product = lax.dot_general(
        jnp.concatenate(inputs, axis=1),
        jnp.concatenate([raw[slot] for slot in range(SLOTS)], axis=1),
        (((1,), (1,)), ((), ())),
        preferred_element_type=F32,
    )
    product = wide(product)
    value = value * inside
    high, low = split(value)
    own_high, own_low = split(product[0:16])
    own_high = own_high.astype(F32)
    degree_high, degree_low = split(product[16:17])
    out[at, 0:NEAR] = merge([raw[slot].astype(F32) for slot in range(SLOTS)]).astype(BF16)
    out[at, NEAR:FAR] = merge([high.astype(F32), low, own_high, own_low]).astype(BF16)
    inside2 = below(bound[row2, col2])
    rows = {BOUND: inside, BOUND2: inside2, DEGREE: degree_high.astype(F32), DEGREE + 1: degree_low}
    rows.update({DIRS + slot: side for slot, side in enumerate(sides)})
    second = signals[row2, col2] * inside2
    out[at, FAR:LONG] = merge([second, jnp.zeros_like(second), jnp.zeros_like(second), info_of(rows)]).astype(BF16)


def fetch(refs, rooms, sems):
    copies = [pltpu.make_async_copy(ref, room, sems.at[i]) for i, (ref, room) in enumerate(zip(refs, rooms))]
    for copy in copies:
        copy.start()
    return copies


def no_message_outside(out):
    z = lax.axis_index("gy")

    @pl.when((z == 0) | (z == lax.axis_size("gy") - 1))
    def _():
        out[...] = jnp.zeros_like(out)


def pack_z(
    tiles, signals, dirs, masks, live, bound, out_a, out_b, dirs_s, masks_s, live_s, bound_s, raw, signals_v, sem, sem2
):
    refs = (signals_v, dirs_s, masks_s, live_s, bound_s)
    copies = fetch((signals, dirs, masks, live, bound), refs, sem2)
    odd = odd_z()
    for which in range(2):
        col = jnp.where(odd == which, COLS - 1, 0)
        copies.append(pltpu.make_async_copy(tiles.at[:, col, :, 0:EDGE, :], raw.at[which], sem.at[which]))
        copies[-1].start()
    for copy in copies:
        copy.wait()
    for which, out in enumerate((out_a, out_b)):
        right = odd == which
        col, col2 = jnp.where(right, COLS - 1, 0), jnp.where(right, COLS - 2, 1)
        for row in range(ROWS):
            block_message(out, row, refs, [raw[which, row, slot] for slot in range(SLOTS)], row, col, row, col2)
    no_message_outside(out_b)


def pack_x(tiles, signals, dirs, masks, live, bound, out_s, out_b):
    refs = (signals, dirs, masks, live, bound)
    core = odd_core()
    for which, out in enumerate((out_s, out_b)):
        row = jnp.where(core == which, 1, 0)
        for col in range(COLS):
            raw = [tiles[row, col, slot, 0:EDGE] for slot in range(SLOTS)]
            block_message(out, 1 + col, refs, raw, row, col, 1 - row, col)


def place_corners(from_a, from_b, out_s, out_b, room, sem, near, far, with_info):
    odd, core = odd_z(), odd_core()
    copies = []
    for side, halo in enumerate((from_a, from_b)):
        at = jnp.where(odd == side, COLS + 1, 0)
        for which, out in enumerate((out_s, out_b)):
            row = jnp.where(core == which, 1, 0)
            first, other = halo[row, far : far + 16].astype(F32), halo[1 - row, far : far + 16].astype(F32)
            parts = [halo[1 - row, near : near + 16].astype(F32), first, other]
            if with_info:
                info, info2 = piece(first, INFO), piece(other, INFO)
                index = lax.broadcasted_iota(jnp.int32, (16, 128), 0)
                for line, source in ((BOUND4, info2[BOUND2 : BOUND2 + 1]), (BOUND3, info[BOUND2 : BOUND2 + 1])):
                    info = jnp.where(index == line, source, info)
                parts.append(jnp.where(index == BOUND2, info2[BOUND : BOUND + 1], info))
            room[which, side, 0:far] = halo[row, 0:far]
            room[which, side, far : far + 16] = merge(parts).astype(BF16)
            copies.append(pltpu.make_async_copy(room.at[which, side], out.at[at], sem.at[which, side]))
    for copy in copies:
        copy.start()
    for copy in copies:
        copy.wait()


def corners_1(from_a, from_b, in_s, in_b, out_s, out_b, room, sem):
    del in_s, in_b
    place_corners(from_a, from_b, out_s, out_b, room, sem, NEAR, FAR, True)


def corners_2(from_a, from_b, in_s, in_b, out_s, out_b, room, sem):
    del in_s, in_b
    place_corners(from_a, from_b, out_s, out_b, room, sem, 0, 16, False)


def place(u, v):
    return u * WIDE + v + 2


class Frame:
    def __init__(self):
        self.odd, self.core = odd_z(), odd_core()
        self.up = 2 * self.core - 1
        self.right = 1 - 2 * self.odd

    def row(self, u):
        return 1 - self.core if u == 2 else self.core

    def col(self, v):
        return jnp.where(self.odd == 1, COLS - 1 - v, v)


def ghost_blocks(frame, u, halo_a, halo_b, halo_x):
    row = frame.row(u)
    found = [(halo_a, row, u, COLS), (halo_b, row, u, -1)]
    return found + [(halo_x, frame.col(v) + 1, 1 if u == 2 else 4, v) for v in range(-1, COLS + 1)]


def info_part(halo, at):
    return piece(halo[at, FAR:LONG].astype(F32), INFO)


def ghost_product(frame, halo, at, info, spot_at, room, height):
    side = merge([info[DIRS + slot : DIRS + slot + 1] for slot in range(SLOTS)])
    step = jnp.where(side > 5.5, 1.0, jnp.where(side > 2.5, 0.0, -1.0))
    turned = 3.0 * (frame.up.astype(F32) * step) + frame.right.astype(F32) * (side - 3.0 * step - 4.0) + 4.0
    turned = jnp.where(side > 8.5, 9.0, turned)
    turn = jnp.broadcast_to(turned, (16, 128)).astype(BF16)
    halves = [jnp.zeros((16, 128), BF16) for _ in range(height // 16)]
    for d in (0, 1, 2, 3, 5, 6, 7, 8):
        near = room[spot_at + (d // 3 - 1) * WIDE + d % 3 - 1]
        chosen = turn == d
        halves = [jnp.where(chosen, near[16 * h : 16 * h + 16], half) for h, half in enumerate(halves)]
    inputs = halves[0] if height == 16 else jnp.concatenate(halves, axis=0)
    product = lax.dot_general(inputs, halo[at, 0:NEAR], (((1,), (1,)), ((), ())), preferred_element_type=F32)
    return wide(product)


def slot_lanes():
    return (lanes() // EDGE).astype(F32).astype(BF16)


def near_input(table, row, col, room, height):
    group = slot_lanes()
    blocks = [room[table[row, slot, col]] for slot in range(SLOTS)]
    halves = []
    for half in range(0, height, 16):
        chosen = blocks[0][half : half + 16]
        for slot in range(1, SLOTS):
            chosen = jnp.where(group == slot, blocks[slot][half : half + 16], chosen)
        halves.append(chosen)
    return halves[0] if height == 16 else jnp.concatenate(halves, axis=0)


def own_product(weights, table, row, col, room, own):
    near = near_input(table, row, col, room, own.shape[0])
    product = jnp.dot(jnp.concatenate([own, own], axis=1), weights[0][row, col], preferred_element_type=F32)
    return product + jnp.dot(near, weights[1][row, col], preferred_element_type=F32)


def alive_of(table, row, col):
    return below(table[row, SLOTS, col])


def inside_of(table, row, col):
    return below(table[row, SLOTS + 1, col])


def place_edge(room, at, value):
    room[at, 0:16] = repeat(value).astype(BF16)


def message_2(out, at, second, weights, table, u, v, u2, v2, frame):
    row, col = frame.row(u), frame.col(v)
    value = second[u - 2, v]
    own = value.astype(BF16)
    product = jnp.dot(jnp.concatenate([own, own], axis=1), weights[0][row, col], preferred_element_type=F32)
    high, low = split(value * inside_of(table, row, col))
    own_high, own_low = split(product)
    out[at, 0:16] = merge([high.astype(F32), low, own_high.astype(F32), own_low]).astype(BF16)
    out[at, 16:32] = (second[u2 - 2, v2] * inside_of(table, frame.row(u2), frame.col(v2))).astype(BF16)
    return product


def turn_tiles(tiles, dirs_s, masks_s, live_s, bound_s, scales, corner_out, own_out, table, scales_out, sem):
    copy = pltpu.make_async_copy(scales, scales_out, sem)
    copy.start()
    rows = lax.broadcasted_iota(jnp.int32, (128, 512), 0)
    cols = lax.broadcasted_iota(jnp.int32, (128, 512), 1)
    picked = jnp.where((rows // EDGE == cols // 128) & (rows % EDGE == cols % 128), 1.0, 0.0).astype(BF16)
    same = jnp.where(rows[:, 0:128] == cols[:, 0:128], 1.0, 0.0)
    for row in range(ROWS):
        for col in range(COLS):
            joined = jnp.concatenate([tiles[row, col, slot] for slot in range(SLOTS)], axis=1)
            owned = []
            for slot in range(SLOTS):
                own = jnp.where(dirs_s[row, slot, col] == 4, jnp.where(masks_s[row, slot, col] == 1, 1.0, 0.0), 0.0)
                owned.append((same * own).astype(BF16))
            total = lax.dot_general(
                jnp.concatenate(owned, axis=1), joined, (((1,), (1,)), ((), ())), preferred_element_type=F32
            )
            high, low = split(total)
            own_out[row, col, 0:128] = high
            own_out[row, col, 128:256] = low.astype(BF16)
            if row == 0:
                product = lax.dot_general(picked, joined, (((1,), (1,)), ((), ())), preferred_element_type=F32)
                corner_out[row, col] = product.astype(BF16)
            else:
                for slot in range(SLOTS):
                    corner_out[row, col, EDGE * slot : EDGE * (slot + 1)] = jnp.transpose(tiles[row, col, slot])[0:EDGE]
    core, odd = odd_core(), odd_z()
    down, right = (2 * core - 1) * WIDE, 1 - 2 * odd
    for row in range(ROWS):
        for col in range(COLS):
            base = place(jnp.where(core == row, 3, 2), jnp.where(odd == 1, COLS - 1 - col, col))
            for slot in range(SLOTS):
                side = dirs_s[row, slot, col]
                step = jnp.where(side > 5, 1, jnp.where(side > 2, 0, -1))
                index = base + step * down + (side - 3 * step - 4) * right
                index = jnp.where(side == 4, ZERO, index)
                table[row, slot, col] = jnp.where(masks_s[row, slot, col] == 1, index, ZERO)
            table[row, SLOTS, col] = live_s[row, col]
            table[row, SLOTS + 1, col] = bound_s[row, col]
    copy.wait()


def fill(room, halo, near, far, with_info, at, near_at, far_at, corner):
    place_edge(room, near_at, piece(halo[at, near : near + 16].astype(F32), HIGH))
    beyond = halo[at, far : far + 16].astype(F32)
    places = (far_at,) + corner
    for index, spot_at in enumerate(places):
        place_edge(room, spot_at, piece(beyond, index))
    if with_info:
        lines = repeat(piece(beyond, INFO))
        for spot_at, line in zip((near_at,) + places, (BOUND, BOUND2, BOUND3, BOUND4)):
            room[spot_at, 16:32] = jnp.where(heads(), lines[line : line + 1], 0.0).astype(BF16)


FIRST, SECOND = (NEAR, FAR, True), (0, 16, False)


def fill_z(frame, room, rows, halo_a, halo_b):
    for halo, near, far in ((halo_a, COLS, COLS + 1), (halo_b, -1, -2)):
        for u in (2, 3):
            fill(room, halo, *rows, frame.row(u), place(u, near), place(u, far), ())


def fill_x(frame, room, rows, halo, near, far):
    for v in range(-1, COLS + 1):
        beyond = {-1: -2, COLS: COLS + 1}.get(v)
        corner = () if beyond is None else (place(near, beyond), place(far, beyond))
        fill(room, halo, *rows, frame.col(v) + 1, place(near, v), place(far, v), corner)


def half_1(frame, u, weights, signals, table, factor, halos, room, room2, degree, first, ghost_degree, ghost_first):
    for number, (halo, at, gu, gv) in enumerate(ghost_blocks(frame, u, *halos)):
        pack, info = halo[at, NEAR:FAR].astype(F32), info_part(halo, at)
        value = piece(pack, HIGH) + piece(pack, LOW)
        near = ghost_product(frame, halo, at, info, place(gu, gv), room, 32)
        sums = near[0:16] + (piece(pack, OWN_HIGH) + piece(pack, OWN_LOW))
        around = near[16:17] + (info[DEGREE : DEGREE + 1] + info[DEGREE + 1 : DEGREE + 2])
        around = jnp.broadcast_to(around, (16, 128))
        result = factor * (around * value - sums) - value
        ghost_degree[number] = around
        ghost_first[number] = result
        place_edge(room2, place(gu, gv), jnp.where(lanes() < EDGE, result * info[BOUND : BOUND + 1], 0.0))
    row = frame.row(u)
    for v in range(COLS):
        col = frame.col(v)
        alive = alive_of(table, row, col)
        value = signals[row, col] * alive
        sums = own_product(weights, table, row, col, room, with_head(value, alive))
        around = jnp.broadcast_to(sums[16:17], (16, 128)) * alive
        result = factor * (around * value - sums[0:16] * alive) - value
        degree[v] = around
        first[v] = result
        place_edge(room2, place(u, v), result * inside_of(table, row, col))


def half_3(frame, u, weights, table, factor, halos, fresh, room, room2, degree, first, second, products, third, ghost_degree, ghost_first):
    values = ghost_blocks(frame, u, *fresh)
    for number, (halo, at, gu, gv) in enumerate(ghost_blocks(frame, u, *halos)):
        pack, info = values[number][0][at, 0:16].astype(F32), info_part(halo, at)
        value = piece(pack, HIGH) + piece(pack, LOW)
        sums = ghost_product(frame, halo, at, info, place(gu, gv), room, 16) + (piece(pack, OWN_HIGH) + piece(pack, OWN_LOW))
        result = 2.0 * (factor * (ghost_degree[number] * value - sums) - value) - ghost_first[number]
        place_edge(room2, place(gu, gv), jnp.where(lanes() < EDGE, result * info[BOUND : BOUND + 1], 0.0))
    row = frame.row(u)
    for v in range(COLS):
        col = frame.col(v)
        near = near_input(table, row, col, room, 16)
        sums = products[u - 2, v] + jnp.dot(near, weights[1][row, col], preferred_element_type=F32)
        value = second[u - 2, v]
        result = 2.0 * (factor * (degree[v] * value - sums * alive_of(table, row, col)) - value) - first[v]
        third[v] = result
        place_edge(room2, place(u, v), result * inside_of(table, row, col))


def carry_rooms(room, room_in, room2, room2_in):
    for v in range(-2, COLS + 2):
        for u in (2, 3):
            room[place(u, v)] = room_in[place(u, v)]
    for v in range(-1, COLS + 1):
        for u in (1, 2):
            room2[place(u, v)] = room2_in[place(u, v)]


def step_1a(
    own_tiles, corner_tiles, signals, table, spectral, from_a, from_b, from_s, room, room2, degree, first, ghost_degree, ghost_first
):
    frame, weights = Frame(), (own_tiles, corner_tiles)
    factor = 2.0 / jnp.full((16, 128), spectral[0])
    room[ZERO] = jnp.zeros((32, 128), BF16)
    for u in (2, 3):
        row = frame.row(u)
        for v in range(COLS):
            col, at = frame.col(v), place(u, v)
            inside = inside_of(table, row, col)
            place_edge(room, at, signals[row, col] * inside)
            room[at, 16:32] = jnp.where(heads(), repeat(inside), 0.0).astype(BF16)
    fill_z(frame, room, FIRST, from_a, from_b)
    fill_x(frame, room, FIRST, from_s, 1, 0)
    halos = (from_a, from_b, from_s)
    half_1(frame, 2, weights, signals, table, factor, halos, room, room2, degree, first, ghost_degree, ghost_first)


def step_1b(
    own_tiles, corner_tiles, signals, table, spectral, from_a, from_b, from_x, room_in, room2_in, degree_a, first_a,
    degree, first, ghost_degree, ghost_first, second, out_a, out_b, room2, room,
):
    frame, weights = Frame(), (own_tiles, corner_tiles)
    factor = 2.0 / jnp.full((16, 128), spectral[0])
    room[ZERO] = jnp.zeros((32, 128), BF16)
    room2[ZERO] = jnp.zeros((16, 128), BF16)
    carry_rooms(room, room_in, room2, room2_in)
    fill_x(frame, room, FIRST, from_x, 4, 5)
    halos = (from_a, from_b, from_x)
    half_1(frame, 3, weights, signals, table, factor, halos, room, room2, degree, first, ghost_degree, ghost_first)
    rows = ((2, degree_a, first_a), (3, degree, first))
    second_step(frame, (0, 1, COLS - 2, COLS - 1), weights, signals, table, factor, room2, rows, second)
    for out, v, v2 in ((out_a, COLS - 1, COLS - 2), (out_b, 0, 1)):
        for u in (2, 3):
            message_2(out, frame.row(u), second, weights, table, u, v, u, v2, frame)
    no_message_outside(out_b)


def second_step(frame, cols, weights, signals, table, factor, room2, rows, second):
    for u, degrees, firsts in rows:
        row = frame.row(u)
        for v in cols:
            col = frame.col(v)
            value = firsts[v]
            sums = own_product(weights, table, row, col, room2, value.astype(BF16))
            alive = alive_of(table, row, col)
            result = 2.0 * (factor * (degrees[v] * value - sums * alive) - value)
            second[u - 2, v] = result - signals[row, col] * alive


def pack_x2(
    edges, own_tiles, corner_tiles, signals, table, spectral, room2, degree_a, degree, first_a, first,
    out_s, out_x, products, second,
):
    frame, weights = Frame(), (own_tiles, corner_tiles)
    factor = 2.0 / jnp.full((16, 128), spectral[0])
    for u in (2, 3):
        for v in (0, 1, COLS - 2, COLS - 1):
            second[u - 2, v] = edges[u - 2, v]
    rows = ((2, degree_a, first_a), (3, degree, first))
    second_step(frame, range(2, COLS - 2), weights, signals, table, factor, room2, rows, second)
    for out, u in ((out_s, 2), (out_x, 3)):
        for v in range(COLS):
            products[u - 2, v] = message_2(out, frame.col(v) + 1, second, weights, table, u, v, 5 - u, v, frame)


def step_3a(
    own_tiles, corner_tiles, table, spectral, from_a, from_b, from_s, new_a, new_b, new_s,
    degree, first, second, products, ghost_degree, ghost_first, room, room2, third,
):
    frame, weights = Frame(), (own_tiles, corner_tiles)
    factor = 2.0 / jnp.full((16, 128), spectral[0])
    room[ZERO] = jnp.zeros((16, 128), BF16)
    for u in (2, 3):
        for v in range(COLS):
            place_edge(room, place(u, v), second[u - 2, v] * inside_of(table, frame.row(u), frame.col(v)))
    fill_z(frame, room, SECOND, new_a, new_b)
    fill_x(frame, room, SECOND, new_s, 1, 0)
    half_3(
        frame, 2, weights, table, factor, (from_a, from_b, from_s), (new_a, new_b, new_s), room, room2,
        degree, first, second, products, third, ghost_degree, ghost_first,
    )


def step_3b(
    own_tiles, corner_tiles, signals, table, spectral, scales, from_a, from_b, from_x, new_a, new_b, new_x, room_in, room2_in,
    degree_a, degree, first_a, first, second, products, ghost_degree, ghost_first, third_a,
    partial, third, fourths, room, room2,
):
    frame, weights = Frame(), (own_tiles, corner_tiles)
    factor = 2.0 / jnp.full((16, 128), spectral[0])
    room[ZERO] = jnp.zeros((16, 128), BF16)
    room2[ZERO] = jnp.zeros((16, 128), BF16)
    carry_rooms(room, room_in, room2, room2_in)
    fill_x(frame, room, SECOND, new_x, 4, 5)
    half_3(
        frame, 3, weights, table, factor, (from_a, from_b, from_x), (new_a, new_b, new_x), room, room2,
        degree, first, second, products, third, ghost_degree, ghost_first,
    )
    count = scales.shape[0]
    squares = [jnp.zeros((16, 128), F32) for _ in range(count)]
    for u, degrees, firsts, thirds in ((2, degree_a, first_a, third_a), (3, degree, first, third)):
        row = frame.row(u)
        for v in range(COLS):
            col = frame.col(v)
            value = thirds[v]
            sums = own_product(weights, table, row, col, room2, value.astype(BF16))
            alive = alive_of(table, row, col)
            fourth = 2.0 * (factor * (degrees[v] * value - sums * alive) - value) - second[u - 2, v]
            fourths[u - 2, v] = fourth
            terms = (signals[row, col] * alive, firsts[v], second[u - 2, v], value, fourth)
            for scale, total in enumerate(weighted(scales, terms)):
                squares[scale] = squares[scale] + total * total
    block = jnp.concatenate(squares + [jnp.zeros((128 - 16 * count, 128), F32)], axis=0)
    line = jnp.sum(jnp.transpose(block), axis=0, keepdims=True)
    partial[...] = jnp.broadcast_to(line[None], partial.shape)


def weighted(scales, terms):
    for scale in range(scales.shape[0]):
        total = (0.5 * scales[scale, 0]) * terms[0]
        for order in range(1, len(terms)):
            total = total + scales[scale, order] * terms[order]
        yield total


def combine(signals, table, scales, first_a, first_b, second, third_a, third_b, fourths, coefficients):
    frame = Frame()
    for u, firsts, thirds in ((2, first_a, third_a), (3, first_b, third_b)):
        row = frame.row(u)
        for v in range(COLS):
            col = frame.col(v)
            terms = (signals[row, col] * alive_of(table, row, col), firsts[v], second[u - 2, v], thirds[v], fourths[u - 2, v])
            for scale, total in enumerate(weighted(scales, terms)):
                coefficients[scale, row, col] = total


def finish(gathered, out, *, nodes):
    total = jnp.sum(gathered[...], axis=0) * (1.0 / nodes)
    scales, channels = out.shape
    for scale in range(scales):
        out[scale : scale + 1] = pltpu.roll(total, 128 - channels * scale, 1)[:, 0:channels] if scale else total[:, 0:channels]


def in_hbm(*arrays):
    return tuple(pltpu.with_memory_space_constraint(array, pltpu.MemorySpace.HBM) for array in arrays)


def in_vmem(*arrays):
    return tuple(pltpu.with_memory_space_constraint(array, pltpu.MemorySpace.VMEM) for array in arrays)


def in_smem(*arrays):
    return tuple(pltpu.with_memory_space_constraint(array, pltpu.MemorySpace.SMEM) for array in arrays)


def neighbour_pairs(devices, first):
    pairs = [(i, i + 1) for i in range(first, devices - 1, 2)]
    return pairs + [(j, i) for i, j in pairs]


def shape(dims, kind=BF16):
    return jax.ShapeDtypeStruct(dims, kind)


def shards(signals, tiles, tile_dir, tile_mask, live_rows, bound_rows, scale_coeffs, spectral_bound):
    devices_x, devices_z = lax.axis_size(GX), lax.axis_size("gy")
    devices = devices_x * devices_z
    scales, channels = scale_coeffs.shape[0], signals.shape[2]
    nodes = ROWS * COLS * 128 * devices

    def swap_z(a, b):
        ends = [(0, 0), (devices_z - 1, devices_z - 1)]
        b = lax.ppermute(b, "gy", neighbour_pairs(devices_z, 1) + ends)
        return lax.ppermute(a, "gy", neighbour_pairs(devices_z, 0)), b

    def swap_x(s, x):
        far = lax.ppermute(x, GX, neighbour_pairs(devices_x, 1))
        return lax.ppermute(s, "gx_2", [(0, 1), (1, 0)]), far

    def call(body, outs, in_specs, out_specs, scratch=(), aliases=None, flops=1000, mib=16):
        return pl.pallas_call(
            body,
            out_shape=outs,
            in_specs=in_specs,
            out_specs=out_specs,
            scratch_shapes=list(scratch),
            input_output_aliases=aliases or {},
            compiler_params=params(mib),
            cost_estimate=cost(flops),
        )

    tile_dir, tile_mask = jnp.swapaxes(tile_dir, 1, 2), jnp.swapaxes(tile_mask, 1, 2)
    tables = (tile_dir, tile_mask, live_rows, bound_rows)
    message_z, message_x = pltpu.VMEM((ROWS, LONG, 128), BF16), pltpu.VMEM((COLS + 2, LONG, 128), BF16)
    a, b, *tables = call(
        pack_z,
        [message_z] * 2 + [pltpu.SMEM(table.shape, jnp.int32) for table in tables],
        [HBM] * 6,
        [VMEM] * 2 + [SMEM] * 4,
        [
            pltpu.VMEM((2, ROWS, SLOTS, EDGE, 128), BF16),
            pltpu.VMEM(signals.shape, F32),
            pltpu.SemaphoreType.DMA((2,)),
            pltpu.SemaphoreType.DMA((5,)),
        ],
    )(*in_hbm(tiles, signals, *tables))
    tables = in_smem(*tables)
    s, x = call(pack_x, [message_x] * 2, [VMEM] * 2 + [SMEM] * 4, [VMEM] * 2, flops=1 << 21)(tiles, signals, *tables)
    a, b = swap_z(a, b)
    corner_room = [pltpu.VMEM((2, 2, LONG, 128), BF16), pltpu.SemaphoreType.DMA((2, 2))]
    s, x = call(
        corners_1, [message_x] * 2, [VMEM] * 2 + [ANY] * 2, [ANY] * 2, corner_room, {2: 0, 3: 1}
    )(a, b, *in_vmem(s, x))
    s, x = swap_x(s, x)

    corner_tiles, own_tiles, table, scale_table = call(
        turn_tiles,
        [
            shape((ROWS, COLS, 128, 128)),
            shape((ROWS, COLS, 256, 128)),
            pltpu.SMEM((ROWS, SLOTS + 2, COLS), jnp.int32),
            pltpu.SMEM(scale_coeffs.shape, F32),
        ],
        [VMEM] + [SMEM] * 4 + [HBM],
        [VMEM, VMEM, SMEM, SMEM],
        [pltpu.SemaphoreType.DMA],
        flops=1 << 23,
    )(tiles, *tables, *in_hbm(scale_coeffs))
    table, scale_table = in_smem(table, scale_table)
    half = shape((COLS, channels, 128), F32)
    extra = shape((COLS + 4, channels, 128), F32)
    wide_room, room = shape((ZERO + 1, 32, 128)), shape((ZERO + 1, 16, 128))
    wide_scratch, scratch = pltpu.VMEM((ZERO + 1, 32, 128), BF16), pltpu.VMEM((ZERO + 1, 16, 128), BF16)
    short_z, short_x = pltpu.VMEM((ROWS, 32, 128), BF16), pltpu.VMEM((COLS + 2, 32, 128), BF16)
    full = shape((ROWS, COLS, channels, 128), F32)
    room_1, room_2, degree_a, first_a, ghost_degree_a, ghost_first_a = call(
        step_1a, [wide_room, room, half, half, extra, extra], [VMEM] * 3 + [SMEM] * 2 + [VMEM] * 3, [VMEM] * 6, flops=1 << 25
    )(own_tiles, corner_tiles, signals, table, spectral_bound, a, b, s)
    degree_b, first_b, ghost_degree_b, ghost_first_b, edges, a2, b2, room_3 = call(
        step_1b,
        [half, half, extra, extra, full, short_z, short_z, room],
        [VMEM] * 3 + [SMEM] * 2 + [VMEM] * 7,
        [VMEM] * 8,
        [wide_scratch],
        flops=1 << 26,
    )(own_tiles, corner_tiles, signals, table, spectral_bound, a, b, x, room_1, room_2, degree_a, first_a)
    s2, x2, products, second = call(
        pack_x2, [short_x] * 2 + [full] * 2, [VMEM] * 4 + [SMEM] * 2 + [VMEM] * 5, [VMEM] * 4, flops=1 << 20
    )(edges, own_tiles, corner_tiles, signals, table, spectral_bound, room_3, degree_a, degree_b, first_a, first_b)
    a2, b2 = swap_z(a2, b2)
    corner_room = [pltpu.VMEM((2, 2, 32, 128), BF16), pltpu.SemaphoreType.DMA((2, 2))]
    s2, x2 = call(
        corners_2, [short_x] * 2, [VMEM] * 2 + [ANY] * 2, [ANY] * 2, corner_room, {2: 0, 3: 1}
    )(a2, b2, *in_vmem(s2, x2))
    s2, x2 = swap_x(s2, x2)
    room_1, room_2, third_a = call(
        step_3a, [room, room, half], [VMEM, VMEM, SMEM, SMEM] + [VMEM] * 12, [VMEM] * 3, flops=1 << 25
    )(
        own_tiles, corner_tiles, table, spectral_bound, a, b, s, a2, b2, s2, degree_a, first_a, second, products,
        ghost_degree_a, ghost_first_a,
    )
    partial, third_b, fourth = call(
        step_3b,
        [pltpu.VMEM((devices, 1, 128), F32), half, full],
        [VMEM] * 3 + [SMEM] * 3 + [VMEM] * 17,
        [VMEM] * 3,
        [scratch, scratch],
        flops=1 << 26,
    )(
        own_tiles, corner_tiles, signals, table, spectral_bound, scale_table, a, b, x, a2, b2, x2, room_1, room_2,
        degree_a, degree_b, first_a, first_b, second, products, ghost_degree_b, ghost_first_b, third_a,
    )
    totals = call(
        combine,
        [shape((scales, ROWS, COLS, channels, 128), F32)],
        [VMEM, SMEM, SMEM] + [VMEM] * 6,
        [VMEM],
        flops=1 << 24,
    )(signals, table, scale_table, first_a, first_b, second, third_a, third_b, fourth)[0]
    gathered = lax.all_to_all(partial, GX_GY, 0, 0)
    energy = pl.pallas_call(
        functools.partial(finish, nodes=nodes),
        out_shape=shape((scales, channels), F32),
        in_specs=[VMEM],
        out_specs=VMEM,
        compiler_params=params(8),
        name="finish",
    )(gathered)
    return (totals, energy)


def solution(mesh):
    torus = Mesh(mesh.devices.reshape(4, 4, 2, mesh.shape["gy"]), ("gx_0", "gx_1", "gx_2", "gy"))
    placed = (
        P(GX, "gy", None, None),
        P(GX, "gy", None, None, None),
        P(GX, "gy", None),
        P(GX, "gy", None),
        P(GX, "gy"),
        P(GX, "gy"),
        P(),
        P(),
    )
    return jax.shard_map(
        shards,
        mesh=torus,
        in_specs=placed,
        out_specs=(P(None, GX, "gy", None, None), P()),
        check_vma=False,
    )
```
